32 devices in a mesh: dp: 8 (over z, x), tensor: 4 (over y, core).
Axes of the slice: x: 2, y: 2, z: 4, core: 2. Of those that a mesh axis runs over, the one named last changes fastest.
Arguments:
- caption_tokens: bfloat16 [32768, 768], P(('dp', 'tensor')), may hold values from -6 to 6
- caption_lengths: int32 [512], P('dp'), may hold values from 8 to 64, as said below
- output_grad: bfloat16 [32768, 768], P(('dp', 'tensor')), may hold values from -6 to 6
- norm_gain: bfloat16 [768], replicated, may hold values from 0.5 to 1.5
- norm_bias: bfloat16 [768], replicated, may hold values from -1 to 1
- query_weight: bfloat16 [768, 768], P(None, 'tensor'), may hold values from -0.21875 to 0.21875
- query_bias: bfloat16 [768], P('tensor'), may hold values from -1 to 1
- key_weight: bfloat16 [768, 768], P(None, 'tensor'), may hold values from -0.21875 to 0.21875
- value_weight: bfloat16 [768, 768], P(None, 'tensor'), may hold values from -0.21875 to 0.21875
- value_bias: bfloat16 [768], P('tensor'), may hold values from -1 to 1
- output_weight: bfloat16 [768, 768], P('tensor'), may hold values from -0.875 to 0.875
- output_bias: bfloat16 [768], replicated, may hold values from -1 to 1
- second_gain: bfloat16 [768], replicated, may hold values from 0.5 to 1.5
- second_bias: bfloat16 [768], replicated, may hold values from -1 to 1
- hidden_weight: bfloat16 [768, 3072], P(None, 'tensor'), may hold values from -0.21875 to 0.21875
- hidden_bias: bfloat16 [3072], P('tensor'), may hold values from -1 to 1
- down_weight: bfloat16 [3072, 768], P('tensor'), may hold values from -0.109375 to 0.109375
- down_bias: bfloat16 [768], replicated, may hold values from -1 to 1
Outputs:
- layer_out: bfloat16 [32768, 768], P(('dp', 'tensor'))
- input_grad: bfloat16 [32768, 768], P(('dp', 'tensor'))
- norm_gain_grad: float32 [768], replicated
- norm_bias_grad: float32 [768], replicated
- query_weight_grad: float32 [768, 768], P(None, 'tensor')
- query_bias_grad: float32 [768], P('tensor')
- key_weight_grad: float32 [768, 768], P(None, 'tensor')
- value_weight_grad: float32 [768, 768], P(None, 'tensor')
- value_bias_grad: float32 [768], P('tensor')
- output_weight_grad: float32 [768, 768], P('tensor')
- output_bias_grad: float32 [768], replicated
- second_gain_grad: float32 [768], replicated
- second_bias_grad: float32 [768], replicated
- hidden_weight_grad: float32 [768, 3072], P(None, 'tensor')
- hidden_bias_grad: float32 [3072], P('tensor')
- down_weight_grad: float32 [3072, 768], P('tensor')
- down_bias_grad: float32 [768], replicated
The draws below stay inside these ranges and needn't reach their ends.
Inputs may be any that keep to these rules, and one draw needn't show every extreme that they name: `caption_lengths`: one caption has all 64 slots live, and one only 8.
All inputs are finite; a program needn't handle non-finite values.
Results may differ from the reference program's by a relative error of at most 0.013.
Values may be sent and summed in bfloat16 or wider, within the bound.
A program may use at most 192 MiB of HBM per device.

```python
import math
import jax
import jax.numpy as jnp
from jax import lax

D = 768
HDIM = 64
FF = 3072
LMAX = 64
CAPTIONS = 512
ROWS = 32768
N_DP = 8


def draw_caption_lengths(key, part):
    first, second, third = jax.random.split(jax.random.fold_in(key, 11), 3)
    count = CAPTIONS
    lengths = jax.random.randint(first, (count,), LMAX // 8, LMAX + 1)
    longest = jax.random.randint(second, (), 0, count)
    shortest = (longest + 1 + jax.random.randint(third, (), 0, count - 1)) % count
    places = jnp.arange(count)
    lengths = jnp.where(places == longest, LMAX, lengths)
    lengths = jnp.where(places == shortest, LMAX // 8, lengths)
    return lengths.astype(jnp.int32)


def levels(rng, dims, cuts, low, largest):
    def one(dim, parts):
        steps = jax.random.uniform(jax.random.fold_in(jax.random.fold_in(rng, 6), dim), (parts,), jnp.float32, low / len(cuts), largest / len(cuts))
        return jnp.repeat(jnp.exp(steps), dims[dim] // parts).reshape((-1,) + (1,) * (len(dims) - dim - 1))

    factor_of = one(*cuts[0])
    for cut in cuts[1:]:
        factor_of = factor_of * one(*cut)
    return factor_of


def gaussian(own_key, dims, width, reach, cuts=(), dtype=jnp.bfloat16):
    level = levels(own_key, dims, cuts, -0.22, 0.18) if cuts else 1.0
    entries = jax.random.normal(own_key, dims, jnp.float32) * width * level
    return jnp.minimum(jnp.maximum(entries, -reach), reach).astype(dtype)


def setup_inputs(seed: int = 0) -> dict:
    seeds = jax.random.split(jax.random.key(seed), 19)
    return {
        "caption_tokens": gaussian(seeds[0], (ROWS, D), 1.0, 6.0, ((0, 32),)),
        "caption_lengths": draw_caption_lengths(jax.random.fold_in(seeds[18], 71), 0),
        "output_grad": gaussian(seeds[2], (ROWS, D), 1.0, 6.0, ((0, 32),)),
        "norm_gain": jnp.clip(1.0 + 0.1 * jax.random.normal(seeds[3], (D,), jnp.float32), 0.5, 1.5).astype(jnp.bfloat16),
        "norm_bias": gaussian(seeds[4], (D,), 0.2, 1.0),
        "query_weight": gaussian(seeds[5], (D, D), D ** -0.5, 0.21875, ((1, 4),)),
        "query_bias": gaussian(seeds[6], (D,), 0.2, 1.0, ((0, 4),)),
        "key_weight": gaussian(seeds[7], (D, D), D ** -0.5, 0.21875, ((1, 4),)),
        "value_weight": gaussian(seeds[8], (D, D), D ** -0.5, 0.21875, ((1, 4),)),
        "value_bias": gaussian(seeds[9], (D,), 0.2, 1.0, ((0, 4),)),
        "output_weight": gaussian(seeds[10], (D, D), (D // 16) ** -0.5, 0.875, ((0, 4),)),
        "output_bias": gaussian(seeds[11], (D,), 0.2, 1.0),
        "second_gain": jnp.clip(1.0 + 0.1 * jax.random.normal(seeds[12], (D,), jnp.float32), 0.5, 1.5).astype(jnp.bfloat16),
        "second_bias": gaussian(seeds[13], (D,), 0.2, 1.0),
        "hidden_weight": gaussian(seeds[14], (D, FF), D ** -0.5, 0.21875, ((1, 4),)),
        "hidden_bias": gaussian(seeds[15], (FF,), 0.2, 1.0, ((0, 4),)),
        "down_weight": gaussian(seeds[16], (FF, D), FF ** -0.5, 0.109375, ((0, 4),)),
        "down_bias": gaussian(seeds[17], (D,), 0.2, 1.0),
    }


EPS = 1e-05
NEG = -1e+30

@jax.custom_vjp
def low(v):
    return lax.optimization_barrier(v.astype(jnp.bfloat16)).astype(jnp.float32)

@jax.custom_vjp
def low_back(v):
    return v

def low_keep(v):
    return (low(v), None)

def low_pass(kept, grad):
    return (grad,)

def back_keep(v):
    return (v, None)

def back_low(kept, grad):
    return (low(grad),)
low.defvjp(low_keep, low_pass)
low_back.defvjp(back_keep, back_low)

def product(left, right):
    return jnp.dot(left, right, precision=lax.Precision.HIGHEST)

def layer_norm(values, gain, shift):
    center = lax.optimization_barrier(jnp.mean(values, -1, keepdims=True))
    spread = values - center
    power = lax.optimization_barrier(jnp.mean(spread * spread, -1, keepdims=True))
    return spread * lax.rsqrt(power + EPS) * gain + shift

def layer(params, tokens, lengths):
    norm_gain, norm_bias, query_weight, query_bias, key_weight, value_weight, value_bias, output_weight, output_bias, second_gain, second_bias, hidden_weight, hidden_bias, down_weight, down_bias = params
    normed = low(layer_norm(tokens, norm_gain, norm_bias))
    queries = low(low_back(product(normed, query_weight) + query_bias))
    keys_all = low(low_back(product(normed, key_weight)))
    values = low(low_back(product(normed, value_weight) + value_bias))
    count = tokens.shape[0] // LMAX
    shaped = (count, LMAX, D // HDIM, HDIM)
    scores = jnp.einsum('cqhd,ckhd->chqk', queries.reshape(shaped), keys_all.reshape(shaped), precision=lax.Precision.HIGHEST) * (1.0 / math.sqrt(HDIM))
    scores = low_back(scores)
    valid = lax.broadcasted_iota(jnp.int32, (count, LMAX), 1) < lengths[:, None]
    scores = jnp.where(valid[:, None, None, :], scores, NEG)
    peak = lax.optimization_barrier(jnp.max(scores, -1, keepdims=True))
    exponent = jnp.exp(scores - peak)
    probs = exponent / lax.optimization_barrier(jnp.sum(exponent, -1, keepdims=True))
    mixed = jnp.einsum('chqk,ckhd->cqhd', low(probs), values.reshape(shaped), precision=lax.Precision.HIGHEST).reshape(tokens.shape[0], D)
    mixed = low(low_back(mixed))
    middle = tokens + low_back(product(mixed, output_weight)) + output_bias
    second = low(layer_norm(middle, second_gain, second_bias))
    hidden = low_back(product(second, hidden_weight) + hidden_bias)
    active = low(jax.nn.gelu(hidden, approximate=False))
    return middle + low_back(product(active, down_weight)) + down_bias

def reference(caption_tokens, caption_lengths, output_grad, norm_gain, norm_bias, query_weight, query_bias, key_weight, value_weight, value_bias, output_weight, output_bias, second_gain, second_bias, hidden_weight, hidden_bias, down_weight, down_bias):
    params = (norm_gain.astype(jnp.float32), norm_bias.astype(jnp.float32), query_weight.astype(jnp.float32), query_bias.astype(jnp.float32), key_weight.astype(jnp.float32), value_weight.astype(jnp.float32), value_bias.astype(jnp.float32), output_weight.astype(jnp.float32), output_bias.astype(jnp.float32), second_gain.astype(jnp.float32), second_bias.astype(jnp.float32), hidden_weight.astype(jnp.float32), hidden_bias.astype(jnp.float32), down_weight.astype(jnp.float32), down_bias.astype(jnp.float32))
    groups = N_DP
    per_group = CAPTIONS // groups
    group_rows = per_group * LMAX
    tokens = caption_tokens.astype(jnp.float32).reshape(groups, group_rows, D)
    cotangent = output_grad.astype(jnp.float32).reshape(groups, group_rows, D)
    lengths = caption_lengths.astype(jnp.int32).reshape(groups, per_group)

    def step(totals, item):
        group_tokens, group_lengths, group_grad = item

        def apply(weights, inputs):
            return layer(weights, inputs, group_lengths)
        result, pullback = jax.vjp(apply, params, group_tokens)
        weight_grads, token_grad = pullback(group_grad)
        totals = jax.tree.map(lambda first, later: first + later, totals, weight_grads)
        return (totals, (result.astype(jnp.bfloat16), token_grad.astype(jnp.bfloat16)))
    zeros = tuple((jnp.zeros(entry.shape, jnp.float32) for entry in params))
    totals, (outputs, token_grads) = lax.scan(step, zeros, (tokens, lengths, cotangent))
    return (outputs.reshape(ROWS, D), token_grads.reshape(ROWS, D), totals[0], totals[1], totals[2], totals[3], totals[4], totals[5], totals[6], totals[7], totals[8], totals[9], totals[10], totals[11], totals[12], totals[13], totals[14])
```

```python
import math

import jax
import jax.numpy as jnp
from jax import lax
from jax.sharding import PartitionSpec as P


HDIM = 64
LMAX = 64
EPS = 1e-05
NEG = -1e30
AXES = ("dp", "tensor")
BF = jnp.bfloat16
F32 = jnp.float32


def layer_norm(values, gain, shift):
    center = jnp.mean(values, -1, keepdims=True)
    spread = values - center
    power = jnp.mean(spread * spread, -1, keepdims=True)
    return spread * lax.rsqrt(power + EPS) * gain + shift


def widen(values):
    return values.astype(F32)


def dot_nn(left, right):
    return jnp.dot(left, right, preferred_element_type=F32)


def dot_nt(left, right):
    return lax.dot_general(left, right, (((1,), (1,)), ((), ())), preferred_element_type=F32)


def dot_tn(left, right):
    return lax.dot_general(left, right, (((0,), (0,)), ((), ())), preferred_element_type=F32)


class Comm:
    def __init__(self, ndp, nt):
        self.ndp, self.nt = ndp, nt
        self.dp = lax.axis_index("dp")
        self.t = lax.axis_index("tensor")

    def swap(self, value, dp_mask=0, t_mask=0):
        count = self.ndp * self.nt
        mask = dp_mask * self.nt + t_mask
        return lax.ppermute(value, AXES, [(i, i ^ mask) for i in range(count)])

    def gather_weight(self, shard):
        half = shard.shape[0] // 2
        bit = self.dp & 1
        mine = lax.dynamic_slice_in_dim(shard, bit * half, half, 0)
        far = self.swap(mine, t_mask=2)
        other = self.swap(far, dp_mask=1)
        first = jnp.where(bit == 0, far, other)
        second = jnp.where(bit == 0, other, far)
        cross = jnp.concatenate([first, second], 0)
        near = self.swap(shard, t_mask=1)
        cross_near = self.swap(cross, t_mask=1)
        pieces = jnp.stack([shard, near, cross, cross_near])
        return jnp.take(pieces, jnp.arange(4) ^ self.t, axis=0)

    def reduce_weight(self, grad):
        t = self.t

        def pick(i):
            return lax.dynamic_index_in_dim(grad, i, 0, keepdims=False)

        near = self.swap(jnp.stack([pick(t ^ 1), pick(t ^ 3)]), t_mask=1)
        own = (widen(pick(t)) + widen(near[0])).astype(BF)
        cross = (widen(pick(t ^ 2)) + widen(near[1])).astype(BF)
        own = (widen(own) + widen(self.swap(cross, t_mask=2))).astype(BF)
        masks = []
        mask = 1
        while mask < self.ndp:
            masks.append(mask)
            mask *= 2
        for mask in masks:
            half = own.shape[0] // 2
            bit = ((self.dp & mask) != 0).astype(jnp.int32)
            keep = lax.dynamic_slice_in_dim(own, bit * half, half, 0)
            send = lax.dynamic_slice_in_dim(own, (1 - bit) * half, half, 0)
            own = (widen(keep) + widen(self.swap(send, dp_mask=mask))).astype(BF)
        for mask in reversed(masks):
            bit = (self.dp & mask) != 0
            other = self.swap(own, dp_mask=mask)
            own = jnp.concatenate([jnp.where(bit, other, own), jnp.where(bit, own, other)], 0)
        return own

    def reduce_small(self, value):
        for t_mask in (1, 2):
            value = value + self.swap(value, t_mask=t_mask)
        mask = 1
        while mask < self.ndp:
            value = value + self.swap(value, dp_mask=mask)
            mask *= 2
        return value


def per_device(
    ndp,
    nt,
    caption_tokens,
    caption_lengths,
    output_grad,
    norm_gain,
    norm_bias,
    query_weight,
    query_bias,
    key_weight,
    value_weight,
    value_bias,
    output_weight,
    output_bias,
    second_gain,
    second_bias,
    hidden_weight,
    hidden_bias,
    down_weight,
    down_bias,
):
    comm = Comm(ndp, nt)
    t = comm.t
    dim = caption_tokens.shape[1]
    rows = caption_tokens.shape[0]
    part = query_weight.shape[1]
    shard_q = query_weight.T
    shard_k = key_weight.T
    shard_v = value_weight.T
    shard_h = hidden_weight.T
    weight_qkv = comm.gather_weight(jnp.concatenate([shard_q, shard_k, shard_v], 0))
    weight_o = comm.gather_weight(output_weight).reshape(dim, dim)
    weight_h = comm.gather_weight(shard_h).reshape(-1, dim)
    weight_d = comm.gather_weight(down_weight).reshape(-1, dim)
    weight_q = weight_qkv[:, :part].reshape(dim, dim)
    weight_k = weight_qkv[:, part : 2 * part].reshape(dim, dim)
    weight_v = weight_qkv[:, 2 * part :].reshape(dim, dim)
    full_qb = lax.all_gather(query_bias, "tensor", axis=0, tiled=True)
    full_vb = lax.all_gather(value_bias, "tensor", axis=0, tiled=True)
    full_hb = lax.all_gather(hidden_bias, "tensor", axis=0, tiled=True)
    count = rows // LMAX
    lengths = lax.dynamic_slice_in_dim(caption_lengths, t * count, count, 0)

    tokens = widen(caption_tokens)
    normed, first_back = jax.vjp(layer_norm, tokens, widen(norm_gain), widen(norm_bias))
    rows_in = normed.astype(BF)
    queries = (dot_nt(rows_in, weight_q) + widen(full_qb)).astype(BF)
    keys_all = dot_nt(rows_in, weight_k).astype(BF)
    values = (dot_nt(rows_in, weight_v) + widen(full_vb)).astype(BF)
    shaped = (count, LMAX, dim // HDIM, HDIM)
    query_four = queries.reshape(shaped)
    key_four = keys_all.reshape(shaped)
    value_four = values.reshape(shaped)
    factor = 1.0 / math.sqrt(HDIM)
    valid = lax.broadcasted_iota(jnp.int32, (count, LMAX), 1) < lengths[:, None]
    scores = jnp.einsum("cqhd,ckhd->chqk", query_four, key_four, preferred_element_type=F32) * factor
    scores = jnp.where(valid[:, None, None, :], scores, NEG)
    peak = jnp.max(scores, -1, keepdims=True)
    exponent = jnp.exp(scores - peak)
    probs = exponent / jnp.sum(exponent, -1, keepdims=True)
    probs_low = probs.astype(BF)
    mixed = (
        jnp.einsum("chqk,ckhd->cqhd", probs_low, value_four, preferred_element_type=F32)
        .reshape(rows, dim)
        .astype(BF)
    )
    middle = tokens + dot_nn(mixed, weight_o) + widen(output_bias)
    second, second_back = jax.vjp(layer_norm, middle, widen(second_gain), widen(second_bias))
    second_low = second.astype(BF)
    hidden = dot_nt(second_low, weight_h) + widen(full_hb)
    active, active_back = jax.vjp(lambda v: jax.nn.gelu(v, approximate=False), hidden)
    active_low = active.astype(BF)
    upstream = widen(output_grad)
    down_bias_grad = jnp.sum(upstream, 0)
    grad_d = comm.reduce_weight(dot_tn(active_low, output_grad).astype(BF).reshape(nt, -1, dim))
    (hidden_grad,) = active_back(dot_nt(output_grad, weight_d))
    hidden_low = hidden_grad.astype(BF)
    hidden_bias_grad = jnp.sum(hidden_low, 0, dtype=F32)
    grad_h = comm.reduce_weight(dot_tn(hidden_low, second_low).astype(BF).reshape(nt, -1, dim))
    middle_part, second_gain_grad, second_bias_grad = second_back(dot_nn(hidden_low, weight_h))
    middle_grad = upstream + middle_part
    output_bias_grad = jnp.sum(middle_grad, 0)
    middle_low = middle_grad.astype(BF)
    grad_o = comm.reduce_weight(dot_tn(mixed, middle_low).astype(BF).reshape(nt, -1, dim))
    mixed_grad = dot_nt(middle_low, weight_o).astype(BF).reshape(shaped)
    value_grad = (
        jnp.einsum("chqk,cqhd->ckhd", probs_low, mixed_grad, preferred_element_type=F32)
        .reshape(rows, dim)
        .astype(BF)
    )
    prob_grad = jnp.einsum("cqhd,ckhd->chqk", mixed_grad, value_four, preferred_element_type=F32)
    score_grad = (probs * (prob_grad - jnp.sum(probs * prob_grad, -1, keepdims=True))).astype(BF)
    query_grad = (
        (jnp.einsum("chqk,ckhd->cqhd", score_grad, key_four, preferred_element_type=F32) * factor)
        .reshape(rows, dim)
        .astype(BF)
    )
    key_grad = (
        (jnp.einsum("chqk,cqhd->ckhd", score_grad, query_four, preferred_element_type=F32) * factor)
        .reshape(rows, dim)
        .astype(BF)
    )
    query_bias_grad = jnp.sum(query_grad, 0, dtype=F32)
    value_bias_grad = jnp.sum(value_grad, 0, dtype=F32)
    grad_qkv = comm.reduce_weight(
        jnp.concatenate(
            [
                dot_tn(query_grad, rows_in).reshape(nt, part, dim),
                dot_tn(key_grad, rows_in).reshape(nt, part, dim),
                dot_tn(value_grad, rows_in).reshape(nt, part, dim),
            ],
            1,
        ).astype(BF)
    )
    normed_in = dot_nn(query_grad, weight_q) + dot_nn(key_grad, weight_k) + dot_nn(value_grad, weight_v)
    token_part, norm_gain_grad, norm_bias_grad = first_back(normed_in)
    token_grad = middle_grad + token_part
    result = middle + dot_nn(active_low, weight_d) + widen(down_bias)
    small = jnp.concatenate(
        [
            jnp.stack(
                [
                    norm_gain_grad,
                    norm_bias_grad,
                    output_bias_grad,
                    second_gain_grad,
                    second_bias_grad,
                    down_bias_grad,
                    query_bias_grad,
                    value_bias_grad,
                ]
            ),
            hidden_bias_grad.reshape(-1, dim),
        ],
        0,
    )
    small = comm.reduce_small(small)
    grad_qkv = widen(grad_qkv)
    return (
        result.astype(BF),
        token_grad.astype(BF),
        small[0],
        small[1],
        grad_qkv[:part].T,
        lax.dynamic_slice_in_dim(small[6], t * part, part, 0),
        grad_qkv[part : 2 * part].T,
        grad_qkv[2 * part :].T,
        lax.dynamic_slice_in_dim(small[7], t * part, part, 0),
        widen(grad_o),
        small[2],
        small[3],
        small[4],
        widen(grad_h).T,
        lax.dynamic_slice_in_dim(
            small[8:].reshape(-1), t * hidden_bias.shape[0], hidden_bias.shape[0], 0
        ),
        widen(grad_d),
        small[5],
    )


def solution(mesh):
    ndp, nt = mesh.shape["dp"], mesh.shape["tensor"]
    both = P(("dp", "tensor"), None)
    col, row, vec = P(None, "tensor"), P("tensor", None), P("tensor")

    def body(*args):
        return per_device(ndp, nt, *args)

    return jax.shard_map(
        body,
        mesh=mesh,
        in_specs=(both, P("dp"), both, P(), P(), col, vec, col, col, vec, row, P(), P(), P(), col, vec, row, P()),
        out_specs=(both, both, P(), P(), col, vec, col, col, vec, row, P(), P(), P(), col, vec, row, P()),
        check_vma=False,
    )
```

```python
import functools
import math

import jax
import jax.numpy as jnp
from jax import lax
from jax.experimental import pallas as pl
from jax.experimental.pallas import tpu as pltpu
from jax.sharding import PartitionSpec as P


HDIM = 64
LMAX = 64
EPS = 1e-05
NEG = -1e30
GROUP = 4
BLOCK = 256
PAD = 32
AXES = ("dp", "tensor")
BF = jnp.bfloat16
F32 = jnp.float32
VMEM_LIMIT = 60 * 1024 * 1024


def widen(values):
    return values.astype(F32)


def dot_nn(left, right):
    return jnp.dot(left, right, preferred_element_type=F32)


def dot_nt(left, right):
    return lax.dot_general(left, right, (((1,), (1,)), ((), ())), preferred_element_type=F32)


def dot_tn(left, right):
    return lax.dot_general(left, right, (((0,), (0,)), ((), ())), preferred_element_type=F32)


def normalize(values):
    center = jnp.mean(values, -1, keepdims=True)
    spread = values - center
    scale = lax.rsqrt(jnp.mean(spread * spread, -1, keepdims=True) + EPS)
    return spread * scale, scale


def normalize_back(grad, unit, scale):
    return scale * (
        grad - jnp.mean(grad, -1, keepdims=True) - unit * jnp.mean(grad * unit, -1, keepdims=True)
    )


def erf(values):
    values = jnp.clip(values, -4.0, 4.0)
    square = values * values
    top = -2.72614225801306e-10
    for coef in (
        2.77068142495902e-08,
        -2.10102402082508e-06,
        -5.69250639462346e-05,
        -7.34990630326855e-04,
        -2.95459980854025e-03,
        -1.60960333262415e-02,
    ):
        top = top * square + coef
    low = -1.45660718464996e-05
    for coef in (
        -2.13374055278905e-04,
        -1.68282697438203e-03,
        -7.37332916720468e-03,
        -1.42647390514189e-02,
    ):
        low = low * square + coef
    return values * top / low


def diagonal_mask(size):
    rows = lax.shift_right_logical(lax.broadcasted_iota(jnp.int32, (size, size), 0), 6)
    cols = lax.shift_right_logical(lax.broadcasted_iota(jnp.int32, (size, size), 1), 6)
    return jnp.where(rows == cols, 1.0, 0.0).astype(BF)


def spread_heads(values, mask):
    return jnp.concatenate([values] * GROUP, 0) * mask


def pick_heads(values):
    lane = lax.shift_right_logical(
        lax.broadcasted_iota(jnp.int32, (LMAX, values.shape[1]), 1), 6
    )
    out = values[:LMAX]
    for head in range(1, GROUP):
        out = jnp.where(lane == head, values[head * LMAX : (head + 1) * LMAX], out)
    return out


def full(shape):
    return pl.BlockSpec(shape, lambda i, *_: (0,) * len(shape))


def rowed(width):
    return pl.BlockSpec((BLOCK, width), lambda i, *_: (i, 0))


def params():
    return pltpu.CompilerParams(
        dimension_semantics=("arbitrary",), vmem_limit_bytes=VMEM_LIMIT
    )


def forward_kernel(
    length_ref,
    tokens_ref,
    p0,
    p1,
    p2,
    p3,
    bias_ref,
    vec_ref,
    normed_ref,
    q_ref,
    k_ref,
    v_ref,
    probs_ref,
    mixed_ref,
    middle_ref,
    second_ref,
    weights_ref,
    mask_ref,
):
    step = pl.program_id(0)
    dim = tokens_ref.shape[1]
    part = dim // 4

    @pl.when(step == 0)
    def _():
        for j, piece in enumerate((p0, p1, p2, p3)):
            for kind in range(4):
                weights_ref[kind, j * part : (j + 1) * part, :] = piece[
                    kind * part : (kind + 1) * part, :
                ]
        mask_ref[...] = diagonal_mask(GROUP * HDIM)

    tokens = widen(tokens_ref[...])
    vec = vec_ref[...]
    unit, _ = normalize(tokens)
    normed = (unit * vec[0:1] + vec[1:2]).astype(BF)
    normed_ref[...] = normed
    q_ref[...] = (dot_nt(normed, weights_ref[0]) + bias_ref[0:1, :]).astype(BF)
    k_ref[...] = dot_nt(normed, weights_ref[1]).astype(BF)
    v_ref[...] = (dot_nt(normed, weights_ref[2]) + bias_ref[1:2, :]).astype(BF)
    width = GROUP * HDIM
    factor = 1.0 / math.sqrt(HDIM)
    mask = mask_ref[...]
    for c in range(BLOCK // LMAX):
        rows = pl.ds(c * LMAX, LMAX)
        length = length_ref[step * (BLOCK // LMAX) + c]
        live = lax.broadcasted_iota(jnp.int32, (LMAX, width), 0) < length
        for g in range(dim // width):
            cols = pl.ds(g * width, width)
            wide = spread_heads(q_ref[rows, cols], mask)
            scores = dot_nt(k_ref[rows, cols], wide) * factor
            scores = jnp.where(live, scores, NEG)
            exponent = jnp.exp(scores - jnp.max(scores, 0, keepdims=True))
            probs = exponent * (1.0 / jnp.sum(exponent, 0, keepdims=True))
            probs_ref[rows, cols] = probs
            crossed = dot_tn(probs.astype(BF), v_ref[rows, cols])
            mixed_ref[rows, cols] = pick_heads(crossed).astype(BF)
    middle = tokens + dot_nn(mixed_ref[...], weights_ref[3]) + vec[2:3]
    middle_ref[...] = middle
    unit, _ = normalize(middle)
    second_ref[...] = (unit * vec[3:4] + vec[4:5]).astype(BF)


def forward(lengths, tokens, pieces, bias, vec):
    rows, dim = tokens.shape
    steps = rows // BLOCK
    shapes = [
        (dim, BF),
        (dim, BF),
        (dim, BF),
        (dim, BF),
        (dim, F32),
        (dim, BF),
        (dim, F32),
        (dim, BF),
    ]
    return pl.pallas_call(
        forward_kernel,
        grid_spec=pltpu.PrefetchScalarGridSpec(
            num_scalar_prefetch=1,
            grid=(steps,),
            in_specs=[rowed(dim)]
            + [full(piece.shape) for piece in pieces]
            + [full(bias.shape), full(vec.shape)],
            out_specs=[rowed(width) for width, _ in shapes] + [full((4, dim, dim))],
            scratch_shapes=[pltpu.VMEM((GROUP * HDIM, GROUP * HDIM), BF)],
        ),
        out_shape=[jax.ShapeDtypeStruct((rows, width), kind) for width, kind in shapes]
        + [jax.ShapeDtypeStruct((4, dim, dim), BF)],
        compiler_params=params(),
        cost_estimate=pl.CostEstimate(
            flops=12 * rows * dim * dim, bytes_accessed=24 * rows * dim, transcendentals=rows * dim
        ),
        name="attend",
    )(lengths, tokens, *pieces, bias, vec)


def expert_kernel(first, *refs):
    if first:
        second_ref, grad_ref, up_ref, down_ref, bias_ref = refs[:5]
        refs = refs[5:]
    else:
        second_ref, grad_ref, up_ref, down_ref, bias_ref, prior_ref = refs[:6]
        refs = refs[6:]
    active_ref, total_ref, up_grad_ref, down_grad_ref, bias_grad_ref, hidden_s = refs
    step = pl.program_id(0)
    rows = pl.ds(pl.multiple_of(step * BLOCK, BLOCK), BLOCK)
    hidden = dot_nn(second_ref[rows, :], up_ref[...]) + bias_ref[0:1, :]
    lean = 0.5 + 0.5 * erf(hidden * (1.0 / math.sqrt(2.0)))
    slope = lean + hidden * (jnp.exp(-0.5 * hidden * hidden) * (1.0 / math.sqrt(2.0 * math.pi)))
    active_ref[rows, :] = (hidden * lean).astype(BF)
    back = (dot_nt(grad_ref[rows, :], down_ref[...]) * slope).astype(BF)
    hidden_s[rows, :] = back
    total = dot_nt(back, up_ref[...])
    total_ref[...] = total if first else total + prior_ref[...]

    @pl.when(step == pl.num_programs(0) - 1)
    def _():
        down_grad_ref[...] = dot_tn(active_ref[...], grad_ref[...]).astype(BF)
        up_grad_ref[...] = dot_tn(second_ref[...], hidden_s[...]).astype(BF)
        bias_grad_ref[...] = jnp.broadcast_to(
            jnp.sum(widen(hidden_s[...]), 0, keepdims=True), bias_grad_ref.shape
        )


def expert(second, grad, up, down, bias, prior):
    rows, dim = second.shape
    units = up.shape[1]
    first = prior is None
    args = [second, grad, up, down, bias] + ([] if first else [prior])
    return pl.pallas_call(
        functools.partial(expert_kernel, first),
        grid=(rows // BLOCK,),
        in_specs=[full(a.shape) for a in args[:5]] + ([] if first else [rowed(dim)]),
        out_specs=[
            full((rows, units)),
            rowed(dim),
            full((dim, units)),
            full((units, dim)),
            full((8, units)),
        ],
        out_shape=[
            jax.ShapeDtypeStruct((rows, units), BF),
            jax.ShapeDtypeStruct((rows, dim), F32),
            jax.ShapeDtypeStruct((dim, units), BF),
            jax.ShapeDtypeStruct((units, dim), BF),
            jax.ShapeDtypeStruct((8, units), F32),
        ],
        scratch_shapes=[pltpu.VMEM((rows, units), BF)],
        compiler_params=params(),
        cost_estimate=pl.CostEstimate(
            flops=10 * rows * dim * units,
            bytes_accessed=14 * rows * dim,
            transcendentals=2 * rows * units,
        ),
        name="expert",
    )(*args)


def backward_kernel(
    grad_ref,
    middle_ref,
    inner_ref,
    mixed_ref,
    q_ref,
    k_ref,
    v_ref,
    probs_ref,
    normed_ref,
    out_weight_ref,
    vec_ref,
    middle_grad_ref,
    dq_ref,
    dk_ref,
    dv_ref,
    pieces_ref,
    small_ref,
    mask_ref,
    low_s,
    mixed_grad_s,
):
    step = pl.program_id(0)
    dim = grad_ref.shape[1]
    part = dim // 4

    @pl.when(step == 0)
    def _():
        mask_ref[...] = diagonal_mask(GROUP * HDIM)
        small_ref[...] = jnp.zeros_like(small_ref)

    all_rows = pl.ds(pl.multiple_of(step * BLOCK, BLOCK), BLOCK)
    vec = vec_ref[...]
    upstream = widen(grad_ref[...])
    unit, scale = normalize(middle_ref[...])
    inner = inner_ref[...]
    middle_grad = upstream + normalize_back(inner * vec[3:4], unit, scale)
    middle_grad_ref[...] = middle_grad
    middle_low = middle_grad.astype(BF)
    low_s[all_rows, :] = middle_low
    small_ref[0:1, :] += jnp.sum(middle_grad, 0, keepdims=True)
    small_ref[1:2, :] += jnp.sum(inner * unit, 0, keepdims=True)
    small_ref[2:3, :] += jnp.sum(inner, 0, keepdims=True)
    small_ref[3:4, :] += jnp.sum(upstream, 0, keepdims=True)
    mixed_grad_s[...] = dot_nt(middle_low, out_weight_ref[0]).astype(BF)
    width = GROUP * HDIM
    factor = 1.0 / math.sqrt(HDIM)
    mask = mask_ref[...]
    for c in range(BLOCK // LMAX):
        rows = pl.ds(c * LMAX, LMAX)
        into = pl.ds(pl.multiple_of(step * BLOCK + c * LMAX, LMAX), LMAX)
        for g in range(dim // width):
            cols = pl.ds(g * width, width)
            wide = spread_heads(mixed_grad_s[rows, cols], mask)
            probs = probs_ref[rows, cols]
            prob_grad = dot_nt(v_ref[rows, cols], wide)
            dv_ref[into, cols] = dot_nn(probs.astype(BF), wide).astype(BF)
            weighted = jnp.sum(probs * prob_grad, 0, keepdims=True)
            score_grad = (probs * (prob_grad - weighted)).astype(BF)
            queries = spread_heads(q_ref[rows, cols], mask)
            dk_ref[into, cols] = (dot_nn(score_grad, queries) * factor).astype(BF)
            crossed = dot_tn(score_grad, k_ref[rows, cols])
            dq_ref[into, cols] = (pick_heads(crossed) * factor).astype(BF)

    @pl.when(step == pl.num_programs(0) - 1)
    def _():
        small_ref[4:5, :] = jnp.sum(widen(dq_ref[...]), 0, keepdims=True)
        small_ref[5:6, :] = jnp.sum(widen(dv_ref[...]), 0, keepdims=True)
        for kind, (left, right) in enumerate(
            ((dq_ref, normed_ref), (dk_ref, normed_ref), (dv_ref, normed_ref), (mixed_ref, low_s))
        ):
            result = dot_tn(left[...], right[...]).astype(BF)
            for j in range(4):
                pieces_ref[j, kind * part : (kind + 1) * part, :] = result[
                    j * part : (j + 1) * part
                ]


def backward(grad, middle, inner, mixed, q, k, v, probs, normed, weights, vec):
    rows, dim = grad.shape
    whole = full((rows, dim))
    return pl.pallas_call(
        backward_kernel,
        grid=(rows // BLOCK,),
        in_specs=[rowed(dim), rowed(dim), rowed(dim), whole]
        + [rowed(dim)] * 4
        + [whole, pl.BlockSpec((1, dim, dim), lambda i: (3, 0, 0)), full(vec.shape)],
        out_specs=[rowed(dim), whole, whole, whole, full((4, dim, dim)), full((8, dim))],
        out_shape=[
            jax.ShapeDtypeStruct((rows, dim), F32),
            jax.ShapeDtypeStruct((rows, dim), BF),
            jax.ShapeDtypeStruct((rows, dim), BF),
            jax.ShapeDtypeStruct((rows, dim), BF),
            jax.ShapeDtypeStruct((4, dim, dim), BF),
            jax.ShapeDtypeStruct((8, dim), F32),
        ],
        scratch_shapes=[
            pltpu.VMEM((GROUP * HDIM, GROUP * HDIM), BF),
            pltpu.VMEM((rows, dim), BF),
            pltpu.VMEM((BLOCK, dim), BF),
        ],
        compiler_params=params(),
        cost_estimate=pl.CostEstimate(
            flops=14 * rows * dim * dim, bytes_accessed=40 * rows * dim, transcendentals=0
        ),
        name="attend_back",
    )(grad, middle, inner, mixed, q, k, v, probs, normed, weights, vec)


def input_kernel(
    tokens_ref, middle_grad_ref, dq_ref, dk_ref, dv_ref, weights_ref, vec_ref, out_ref, small_ref
):
    @pl.when(pl.program_id(0) == 0)
    def _():
        small_ref[...] = jnp.zeros_like(small_ref)

    unit, scale = normalize(widen(tokens_ref[...]))
    grad = (
        dot_nn(dq_ref[...], weights_ref[0])
        + dot_nn(dk_ref[...], weights_ref[1])
        + dot_nn(dv_ref[...], weights_ref[2])
    )
    small_ref[0:1, :] += jnp.sum(grad * unit, 0, keepdims=True)
    small_ref[1:2, :] += jnp.sum(grad, 0, keepdims=True)
    back = normalize_back(grad * vec_ref[0:1, :], unit, scale)
    out_ref[...] = (middle_grad_ref[...] + back).astype(BF)


def input_back(tokens, middle_grad, dq, dk, dv, weights, vec):
    rows, dim = tokens.shape
    return pl.pallas_call(
        input_kernel,
        grid=(rows // BLOCK,),
        in_specs=[rowed(dim)] * 5 + [full((3, dim, dim)), full(vec.shape)],
        out_specs=[rowed(dim), full((8, dim))],
        out_shape=[
            jax.ShapeDtypeStruct((rows, dim), BF),
            jax.ShapeDtypeStruct((8, dim), F32),
        ],
        compiler_params=params(),
        cost_estimate=pl.CostEstimate(
            flops=6 * rows * dim * dim, bytes_accessed=14 * rows * dim, transcendentals=0
        ),
        name="input_back",
    )(tokens, middle_grad, dq, dk, dv, weights, vec)


def result_kernel(middle_ref, a0, a1, a2, a3, d0, d1, d2, d3, vec_ref, out_ref):
    total = middle_ref[...] + vec_ref[5:6, :]
    for active, down in ((a0, d0), (a1, d1), (a2, d2), (a3, d3)):
        total += dot_nn(active[...], down[...])
    out_ref[...] = total.astype(BF)


def layer_result(middle, actives, downs, vec):
    rows, dim = middle.shape
    units = actives[0].shape[1]
    return pl.pallas_call(
        result_kernel,
        grid=(rows // BLOCK,),
        in_specs=[rowed(dim)]
        + [rowed(units)] * 4
        + [full(d.shape) for d in downs]
        + [full(vec.shape)],
        out_specs=rowed(dim),
        out_shape=jax.ShapeDtypeStruct((rows, dim), BF),
        compiler_params=params(),
        cost_estimate=pl.CostEstimate(
            flops=8 * rows * dim * units, bytes_accessed=22 * rows * dim, transcendentals=0
        ),
        name="layer_result",
    )(middle, *actives, *downs, vec)


class Comm:
    def __init__(self, ndp, nt):
        self.ndp, self.nt = ndp, nt
        self.dp = lax.axis_index("dp")
        self.t = lax.axis_index("tensor")
        self.masks = []
        mask = 1
        while mask < ndp:
            self.masks.append(mask)
            mask *= 2

    def swap(self, value, dp_mask=0, t_mask=0):
        count = self.ndp * self.nt
        mask = dp_mask * self.nt + t_mask
        return lax.ppermute(value, AXES, [(i, i ^ mask) for i in range(count)])

    def gather_weight(self, shard):
        half = shard.shape[0] // 2
        bit = self.dp & 1
        mine = lax.dynamic_slice_in_dim(shard, bit * half, half, 0)
        far = self.swap(mine, t_mask=2)
        near = self.swap(shard, t_mask=1)
        other = self.swap(far, dp_mask=1)
        cross = jnp.concatenate([jnp.where(bit == 0, far, other), jnp.where(bit == 0, other, far)], 0)
        return [shard, near, cross, self.swap(cross, t_mask=1)]

    def reduce_rest(self, own):
        for mask in self.masks:
            half = own.shape[0] // 2
            bit = ((self.dp & mask) != 0).astype(jnp.int32)
            keep = lax.dynamic_slice_in_dim(own, bit * half, half, 0)
            send = lax.dynamic_slice_in_dim(own, (1 - bit) * half, half, 0)
            own = (widen(keep) + widen(self.swap(send, dp_mask=mask))).astype(BF)
        for mask in reversed(self.masks):
            bit = (self.dp & mask) != 0
            other = self.swap(own, dp_mask=mask)
            own = jnp.concatenate([jnp.where(bit, other, own), jnp.where(bit, own, other)], 0)
        return own

    def reduce_small(self, value):
        for t_mask in (1, 2):
            value = value + self.swap(value, t_mask=t_mask)
        for mask in self.masks:
            value = value + self.swap(value, dp_mask=mask)
        return value


def add_low(left, right):
    return (widen(left) + widen(right)).astype(BF)


def per_device(
    ndp,
    nt,
    caption_tokens,
    caption_lengths,
    output_grad,
    norm_gain,
    norm_bias,
    query_weight,
    query_bias,
    key_weight,
    value_weight,
    value_bias,
    output_weight,
    output_bias,
    second_gain,
    second_bias,
    hidden_weight,
    hidden_bias,
    down_weight,
    down_bias,
):
    comm = Comm(ndp, nt)
    t = comm.t
    rows, dim = caption_tokens.shape
    part = query_weight.shape[1]
    count = rows // LMAX
    lengths = lax.dynamic_slice_in_dim(caption_lengths, t * count, count, 0)
    biases = jnp.pad(
        jnp.stack([jnp.pad(jnp.concatenate([query_bias, value_bias]), (0, dim - 2 * part)), hidden_bias]),
        ((0, PAD - 2), (0, 0)),
    )
    shard = jnp.concatenate([query_weight.T, key_weight.T, value_weight.T, output_weight, biases], 0)
    pieces = comm.gather_weight(shard)
    ups = comm.gather_weight(hidden_weight)
    downs = comm.gather_weight(down_weight)
    rows_of = [widen(piece[4 * part : 4 * part + 2]) for piece in pieces]
    bias = jnp.stack(
        [
            jnp.concatenate([r[0, :part] for r in rows_of]),
            jnp.concatenate([r[0, part : 2 * part] for r in rows_of]),
        ]
    )
    vec = jnp.stack(
        [widen(v) for v in (norm_gain, norm_bias, output_bias, second_gain, second_bias, down_bias)]
    )
    vec = jnp.pad(vec, ((0, 2), (0, 0)))
    normed, q, k, v, probs, mixed, middle, second, weights = forward(
        lengths, caption_tokens, pieces, bias, vec
    )
    actives, up_grads, down_grads, hidden_sums = [None] * 4, [None] * 4, [None] * 4, [None] * 4
    inner = None
    for j in (3, 2, 1, 0):
        actives[j], inner, up_grads[j], down_grads[j], hidden_sums[j] = expert(
            second, output_grad, ups[j], downs[j], rows_of[j][1:2], inner
        )
    stack = [jnp.stack([u, d]) for u, d in zip(up_grads, down_grads)]
    cross = add_low(stack[2], comm.swap(stack[3], t_mask=1))
    own = add_low(stack[0], comm.swap(stack[1], t_mask=1))
    own = add_low(own, comm.swap(cross, t_mask=2))
    grad_ffn = comm.reduce_rest(own.reshape(-1, dim))

    middle_grad, dq, dk, dv, grads, small = backward(
        output_grad, middle, inner, mixed, q, k, v, probs, normed, weights, vec
    )
    near = comm.swap(jnp.stack([grads[1], grads[3]]), t_mask=1)
    own = add_low(grads[0], near[0])
    cross = add_low(grads[2], near[1])
    grad_att = comm.reduce_rest(add_low(own, comm.swap(cross, t_mask=2)))

    token_grad, last_small = input_back(caption_tokens, middle_grad, dq, dk, dv, weights, vec)
    result = layer_result(middle, actives, downs, vec)
    order = jnp.arange(4) ^ t

    def restore(values):
        return jnp.take(values.reshape(4, -1), order, axis=0).reshape(-1, dim)

    hidden_sum = jnp.concatenate([s[0] for s in hidden_sums])
    sums = comm.reduce_small(
        jnp.concatenate(
            [
                last_small[:2],
                small[:4],
                restore(small[4]),
                restore(small[5]),
                restore(hidden_sum),
            ],
            0,
        )
    )
    grad_att = widen(grad_att)
    grad_ffn = widen(grad_ffn)
    return (
        result,
        token_grad,
        sums[0],
        sums[1],
        grad_att[:part].T,
        lax.dynamic_slice_in_dim(sums[6], t * part, part, 0),
        grad_att[part : 2 * part].T,
        grad_att[2 * part : 3 * part].T,
        lax.dynamic_slice_in_dim(sums[7], t * part, part, 0),
        grad_att[3 * part :],
        sums[2],
        sums[3],
        sums[4],
        grad_ffn[:dim],
        lax.dynamic_slice_in_dim(sums[8:].reshape(-1), t * hidden_bias.shape[0], hidden_bias.shape[0], 0),
        grad_ffn[dim:],
        sums[5],
    )


def solution(mesh):
    ndp, nt = mesh.shape["dp"], mesh.shape["tensor"]
    both = P(("dp", "tensor"), None)
    col, row, vec = P(None, "tensor"), P("tensor", None), P("tensor")

    def body(*args):
        return per_device(ndp, nt, *args)

    return jax.shard_map(
        body,
        mesh=mesh,
        in_specs=(both, P("dp"), both, P(), P(), col, vec, col, col, vec, row, P(), P(), P(), col, vec, row, P()),
        out_specs=(both, both, P(), P(), col, vec, col, col, vec, row, P(), P(), P(), col, vec, row, P()),
        check_vma=False,
    )
```

```python
import functools
import math

import jax
import jax.numpy as jnp
from jax import lax
from jax.experimental import pallas as pl
from jax.experimental.pallas import tpu as pltpu
from jax.sharding import PartitionSpec as P


HDIM = 64
LMAX = 64
EPS = 1e-05
NEG = -1e30
GROUP = 4
BLOCK = 256
PAD = 32
CHUNK = 256
TILE = 64
AXES = ("dp", "tensor")
BF = jnp.bfloat16
F32 = jnp.float32
VMEM_LIMIT = 60 * 1024 * 1024


def widen(values):
    return values.astype(F32)


def dot_nn(left, right):
    return jnp.dot(left, right, preferred_element_type=F32)


def dot_nt(left, right):
    return lax.dot_general(left, right, (((1,), (1,)), ((), ())), preferred_element_type=F32)


def dot_tn(left, right):
    return lax.dot_general(left, right, (((0,), (0,)), ((), ())), preferred_element_type=F32)


def normalize(values):
    center = jnp.mean(values, -1, keepdims=True)
    spread = values - center
    scale = lax.rsqrt(jnp.mean(spread * spread, -1, keepdims=True) + EPS)
    return spread * scale, scale


def normalize_back(grad, unit, scale):
    return scale * (
        grad - jnp.mean(grad, -1, keepdims=True) - unit * jnp.mean(grad * unit, -1, keepdims=True)
    )


def erf(values):
    values = jnp.clip(values, -4.0, 4.0)
    square = values * values
    top = -2.72614225801306e-10
    for coef in (
        2.77068142495902e-08,
        -2.10102402082508e-06,
        -5.69250639462346e-05,
        -7.34990630326855e-04,
        -2.95459980854025e-03,
        -1.60960333262415e-02,
    ):
        top = top * square + coef
    low = -1.45660718464996e-05
    for coef in (
        -2.13374055278905e-04,
        -1.68282697438203e-03,
        -7.37332916720468e-03,
        -1.42647390514189e-02,
    ):
        low = low * square + coef
    return values * top / low


def diagonal_mask(size):
    rows = lax.shift_right_logical(lax.broadcasted_iota(jnp.int32, (size, size), 0), 6)
    cols = lax.shift_right_logical(lax.broadcasted_iota(jnp.int32, (size, size), 1), 6)
    return jnp.where(rows == cols, 1.0, 0.0).astype(BF)


def spread_heads(values, mask):
    return jnp.concatenate([values] * GROUP, 0) * mask


def pick_heads(values):
    lane = lax.shift_right_logical(
        lax.broadcasted_iota(jnp.int32, (LMAX, values.shape[1]), 1), 6
    )
    out = values[:LMAX]
    for head in range(1, GROUP):
        out = jnp.where(lane == head, values[head * LMAX : (head + 1) * LMAX], out)
    return out


def full(shape):
    return pl.BlockSpec(shape, lambda i, *_: (0,) * len(shape))


def rowed(width):
    return pl.BlockSpec((BLOCK, width), lambda i, *_: (i, 0))


def params():
    return pltpu.CompilerParams(
        dimension_semantics=("arbitrary",), vmem_limit_bytes=VMEM_LIMIT
    )


def forward_kernel(
    length_ref,
    tokens_ref,
    p0,
    p1,
    p2,
    p3,
    bias_ref,
    vec_ref,
    normed_ref,
    q_ref,
    k_ref,
    v_ref,
    probs_ref,
    mixed_ref,
    middle_ref,
    second_ref,
    weights_ref,
    mask_ref,
):
    step = pl.program_id(0)
    dim = tokens_ref.shape[1]
    part = dim // 4

    @pl.when(step == 0)
    def _():
        for j, piece in enumerate((p0, p1, p2, p3)):
            for kind in range(4):
                weights_ref[kind, j * part : (j + 1) * part, :] = piece[
                    kind * part : (kind + 1) * part, :
                ]
        mask_ref[...] = diagonal_mask(GROUP * HDIM)

    tokens = widen(tokens_ref[...])
    vec = vec_ref[...]
    unit, _ = normalize(tokens)
    normed = (unit * vec[0:1] + vec[1:2]).astype(BF)
    normed_ref[...] = normed
    q_ref[...] = (dot_nt(normed, weights_ref[0]) + bias_ref[0:1, :]).astype(BF)
    k_ref[...] = dot_nt(normed, weights_ref[1]).astype(BF)
    v_ref[...] = (dot_nt(normed, weights_ref[2]) + bias_ref[1:2, :]).astype(BF)
    width = GROUP * HDIM
    factor = 1.0 / math.sqrt(HDIM)
    mask = mask_ref[...]
    for c in range(BLOCK // LMAX):
        rows = pl.ds(c * LMAX, LMAX)
        length = length_ref[step * (BLOCK // LMAX) + c]
        live = lax.broadcasted_iota(jnp.int32, (LMAX, width), 0) < length
        for g in range(dim // width):
            cols = pl.ds(g * width, width)
            wide = spread_heads(q_ref[rows, cols], mask)
            scores = dot_nt(k_ref[rows, cols], wide) * factor
            scores = jnp.where(live, scores, NEG)
            exponent = jnp.exp(scores - jnp.max(scores, 0, keepdims=True))
            probs = exponent * (1.0 / jnp.sum(exponent, 0, keepdims=True))
            probs_ref[rows, cols] = probs
            crossed = dot_tn(probs.astype(BF), v_ref[rows, cols])
            mixed_ref[rows, cols] = pick_heads(crossed).astype(BF)
    middle = tokens + dot_nn(mixed_ref[...], weights_ref[3]) + vec[2:3]
    middle_ref[...] = middle
    unit, _ = normalize(middle)
    second_ref[...] = (unit * vec[3:4] + vec[4:5]).astype(BF)


def forward(lengths, tokens, pieces, bias, vec):
    rows, dim = tokens.shape
    steps = rows // BLOCK
    shapes = [
        (dim, BF),
        (dim, BF),
        (dim, BF),
        (dim, BF),
        (dim, F32),
        (dim, BF),
        (dim, F32),
        (dim, BF),
    ]
    return pl.pallas_call(
        forward_kernel,
        grid_spec=pltpu.PrefetchScalarGridSpec(
            num_scalar_prefetch=1,
            grid=(steps,),
            in_specs=[rowed(dim)]
            + [full(piece.shape) for piece in pieces]
            + [full(bias.shape), full(vec.shape)],
            out_specs=[rowed(width) for width, _ in shapes] + [full((4, dim, dim))],
            scratch_shapes=[pltpu.VMEM((GROUP * HDIM, GROUP * HDIM), BF)],
        ),
        out_shape=[jax.ShapeDtypeStruct((rows, width), kind) for width, kind in shapes]
        + [jax.ShapeDtypeStruct((4, dim, dim), BF)],
        compiler_params=params(),
        cost_estimate=pl.CostEstimate(
            flops=12 * rows * dim * dim, bytes_accessed=24 * rows * dim, transcendentals=rows * dim
        ),
        name="attend",
    )(lengths, tokens, *pieces, bias, vec)


def expert_kernel(first, *refs):
    if first:
        second_ref, grad_ref, up_ref, down_ref, bias_ref = refs[:5]
        refs = refs[5:]
    else:
        second_ref, grad_ref, up_ref, down_ref, bias_ref, prior_ref = refs[:6]
        refs = refs[6:]
    active_ref, total_ref, up_grad_ref, down_grad_ref, bias_grad_ref, hidden_s = refs
    step = pl.program_id(0)
    rows = pl.ds(pl.multiple_of(step * BLOCK, BLOCK), BLOCK)
    hidden = dot_nn(second_ref[rows, :], up_ref[...]) + bias_ref[0:1, :]
    lean = 0.5 + 0.5 * erf(hidden * (1.0 / math.sqrt(2.0)))
    slope = lean + hidden * (jnp.exp(-0.5 * hidden * hidden) * (1.0 / math.sqrt(2.0 * math.pi)))
    active_ref[rows, :] = (hidden * lean).astype(BF)
    back = (dot_nt(grad_ref[rows, :], down_ref[...]) * slope).astype(BF)
    hidden_s[rows, :] = back
    total = dot_nt(back, up_ref[...])
    total_ref[...] = total if first else total + prior_ref[...]

    @pl.when(step == pl.num_programs(0) - 1)
    def _():
        down_grad_ref[...] = dot_tn(active_ref[...], grad_ref[...]).astype(BF)
        up_grad_ref[...] = dot_tn(second_ref[...], hidden_s[...]).astype(BF)
        bias_grad_ref[...] = jnp.broadcast_to(
            jnp.sum(widen(hidden_s[...]), 0, keepdims=True), bias_grad_ref.shape
        )


def expert(second, grad, up, down, bias, prior):
    rows, dim = second.shape
    units = up.shape[1]
    first = prior is None
    args = [second, grad, up, down, bias] + ([] if first else [prior])
    return pl.pallas_call(
        functools.partial(expert_kernel, first),
        grid=(rows // BLOCK,),
        in_specs=[full(a.shape) for a in args[:5]] + ([] if first else [rowed(dim)]),
        out_specs=[
            full((rows, units)),
            rowed(dim),
            full((dim, units)),
            full((units, dim)),
            full((8, units)),
        ],
        out_shape=[
            jax.ShapeDtypeStruct((rows, units), BF),
            jax.ShapeDtypeStruct((rows, dim), F32),
            jax.ShapeDtypeStruct((dim, units), BF),
            jax.ShapeDtypeStruct((units, dim), BF),
            jax.ShapeDtypeStruct((8, units), F32),
        ],
        scratch_shapes=[pltpu.VMEM((rows, units), BF)],
        compiler_params=params(),
        cost_estimate=pl.CostEstimate(
            flops=10 * rows * dim * units,
            bytes_accessed=14 * rows * dim,
            transcendentals=2 * rows * units,
        ),
        name="expert",
    )(*args)


def backward_kernel(
    grad_ref,
    middle_ref,
    inner_ref,
    mixed_ref,
    q_ref,
    k_ref,
    v_ref,
    probs_ref,
    normed_ref,
    out_weight_ref,
    vec_ref,
    middle_grad_ref,
    dq_ref,
    dk_ref,
    dv_ref,
    g0,
    g1,
    g2,
    g3,
    small_ref,
    mask_ref,
    low_s,
    mixed_grad_s,
):
    step = pl.program_id(0)
    dim = grad_ref.shape[1]
    part = dim // 4

    @pl.when(step == 0)
    def _():
        mask_ref[...] = diagonal_mask(GROUP * HDIM)
        small_ref[...] = jnp.zeros_like(small_ref)

    all_rows = pl.ds(pl.multiple_of(step * BLOCK, BLOCK), BLOCK)
    vec = vec_ref[...]
    upstream = widen(grad_ref[...])
    unit, scale = normalize(middle_ref[...])
    inner = inner_ref[...]
    middle_grad = upstream + normalize_back(inner * vec[3:4], unit, scale)
    middle_grad_ref[...] = middle_grad
    middle_low = middle_grad.astype(BF)
    low_s[all_rows, :] = middle_low
    small_ref[0:1, :] += jnp.sum(middle_grad, 0, keepdims=True)
    small_ref[1:2, :] += jnp.sum(inner * unit, 0, keepdims=True)
    small_ref[2:3, :] += jnp.sum(inner, 0, keepdims=True)
    small_ref[3:4, :] += jnp.sum(upstream, 0, keepdims=True)
    mixed_grad_s[...] = dot_nt(middle_low, out_weight_ref[0]).astype(BF)
    width = GROUP * HDIM
    factor = 1.0 / math.sqrt(HDIM)
    mask = mask_ref[...]
    for c in range(BLOCK // LMAX):
        rows = pl.ds(c * LMAX, LMAX)
        into = pl.ds(pl.multiple_of(step * BLOCK + c * LMAX, LMAX), LMAX)
        for g in range(dim // width):
            cols = pl.ds(g * width, width)
            wide = spread_heads(mixed_grad_s[rows, cols], mask)
            probs = probs_ref[rows, cols]
            prob_grad = dot_nt(v_ref[rows, cols], wide)
            dv_ref[into, cols] = dot_nn(probs.astype(BF), wide).astype(BF)
            weighted = jnp.sum(probs * prob_grad, 0, keepdims=True)
            score_grad = (probs * (prob_grad - weighted)).astype(BF)
            queries = spread_heads(q_ref[rows, cols], mask)
            dk_ref[into, cols] = (dot_nn(score_grad, queries) * factor).astype(BF)
            crossed = dot_tn(score_grad, k_ref[rows, cols])
            dq_ref[into, cols] = (pick_heads(crossed) * factor).astype(BF)

    @pl.when(step == pl.num_programs(0) - 1)
    def _():
        small_ref[4:5, :] = jnp.sum(widen(dq_ref[...]), 0, keepdims=True)
        small_ref[5:6, :] = jnp.sum(widen(dv_ref[...]), 0, keepdims=True)
        for kind, (left, right) in enumerate(
            ((dq_ref, normed_ref), (dk_ref, normed_ref), (dv_ref, normed_ref), (mixed_ref, low_s))
        ):
            result = dot_tn(left[...], right[...]).astype(BF)
            for j, piece in enumerate((g0, g1, g2, g3)):
                piece[kind * part : (kind + 1) * part, :] = result[j * part : (j + 1) * part]


def backward(grad, middle, inner, mixed, q, k, v, probs, normed, weights, vec):
    rows, dim = grad.shape
    whole = full((rows, dim))
    return pl.pallas_call(
        backward_kernel,
        grid=(rows // BLOCK,),
        in_specs=[rowed(dim), rowed(dim), rowed(dim), whole]
        + [rowed(dim)] * 4
        + [whole, pl.BlockSpec((1, dim, dim), lambda i: (3, 0, 0)), full(vec.shape)],
        out_specs=[rowed(dim), whole, whole, whole] + [full((dim, dim))] * 4 + [full((8, dim))],
        out_shape=[
            jax.ShapeDtypeStruct((rows, dim), F32),
            jax.ShapeDtypeStruct((rows, dim), BF),
            jax.ShapeDtypeStruct((rows, dim), BF),
            jax.ShapeDtypeStruct((rows, dim), BF),
        ]
        + [jax.ShapeDtypeStruct((dim, dim), BF)] * 4
        + [jax.ShapeDtypeStruct((8, dim), F32)],
        scratch_shapes=[
            pltpu.VMEM((GROUP * HDIM, GROUP * HDIM), BF),
            pltpu.VMEM((rows, dim), BF),
            pltpu.VMEM((BLOCK, dim), BF),
        ],
        compiler_params=params(),
        cost_estimate=pl.CostEstimate(
            flops=14 * rows * dim * dim, bytes_accessed=40 * rows * dim, transcendentals=0
        ),
        name="attend_back",
    )(grad, middle, inner, mixed, q, k, v, probs, normed, weights, vec)


def input_kernel(
    tokens_ref, middle_grad_ref, dq_ref, dk_ref, dv_ref, weights_ref, vec_ref, out_ref, small_ref
):
    @pl.when(pl.program_id(0) == 0)
    def _():
        small_ref[...] = jnp.zeros_like(small_ref)

    unit, scale = normalize(widen(tokens_ref[...]))
    grad = (
        dot_nn(dq_ref[...], weights_ref[0])
        + dot_nn(dk_ref[...], weights_ref[1])
        + dot_nn(dv_ref[...], weights_ref[2])
    )
    small_ref[0:1, :] += jnp.sum(grad * unit, 0, keepdims=True)
    small_ref[1:2, :] += jnp.sum(grad, 0, keepdims=True)
    back = normalize_back(grad * vec_ref[0:1, :], unit, scale)
    out_ref[...] = (middle_grad_ref[...] + back).astype(BF)


def input_back(tokens, middle_grad, dq, dk, dv, weights, vec):
    rows, dim = tokens.shape
    return pl.pallas_call(
        input_kernel,
        grid=(rows // BLOCK,),
        in_specs=[rowed(dim)] * 5 + [full((3, dim, dim)), full(vec.shape)],
        out_specs=[rowed(dim), full((8, dim))],
        out_shape=[
            jax.ShapeDtypeStruct((rows, dim), BF),
            jax.ShapeDtypeStruct((8, dim), F32),
        ],
        compiler_params=params(),
        cost_estimate=pl.CostEstimate(
            flops=6 * rows * dim * dim, bytes_accessed=14 * rows * dim, transcendentals=0
        ),
        name="input_back",
    )(tokens, middle_grad, dq, dk, dv, weights, vec)


def result_kernel(middle_ref, a0, a1, a2, a3, d0, d1, d2, d3, vec_ref, out_ref):
    total = middle_ref[...] + vec_ref[5:6, :]
    for active, down in ((a0, d0), (a1, d1), (a2, d2), (a3, d3)):
        total += dot_nn(active[...], down[...])
    out_ref[...] = total.astype(BF)


def layer_result(middle, actives, downs, vec):
    rows, dim = middle.shape
    units = actives[0].shape[1]
    return pl.pallas_call(
        result_kernel,
        grid=(rows // BLOCK,),
        in_specs=[rowed(dim)]
        + [rowed(units)] * 4
        + [full(d.shape) for d in downs]
        + [full(vec.shape)],
        out_specs=rowed(dim),
        out_shape=jax.ShapeDtypeStruct((rows, dim), BF),
        compiler_params=params(),
        cost_estimate=pl.CostEstimate(
            flops=8 * rows * dim * units, bytes_accessed=22 * rows * dim, transcendentals=0
        ),
        name="layer_result",
    )(middle, *actives, *downs, vec)


def add_rows(into, base, other, other_base, rows, result=None):
    result = into if result is None else result
    size = min(rows, TILE)

    def body(i, carry):
        left = pl.ds(pl.multiple_of(base + i * size, 8), size)
        right = pl.ds(pl.multiple_of(other_base + i * size, 8), size)
        result[left, :] = (widen(into[left, :]) + widen(other[right, :])).astype(into.dtype)
        return carry

    lax.fori_loop(0, rows // size, body, 0)


def plan_levels(masks, rows):
    levels, place = [], 0
    for mask in masks:
        after = rows // 2 if (rows // 2) % 16 == 0 else rows
        levels.append((mask, rows, after, place))
        place += after
        rows = after
    return levels, place


def reduce_kernel(masks, chunk, counts, *refs):
    total = sum(counts)
    pieces, refs = refs[: 4 * len(counts)], refs[4 * len(counts) :]
    small_in, out_ref, small_out, own, cross, near_own, near_cross, far, landing = refs[:9]
    gathered, small_land, send_sem, recv_sem, local_sem = refs[9:]
    levels, place = plan_levels(masks, chunk)
    dp = lax.axis_index("dp")
    t = lax.axis_index("tensor")
    bits = {mask: (dp // mask) % 2 for mask in masks}
    peers = {mask: (dp + mask - 2 * mask * bits[mask], t) for mask in masks}
    peers["core"] = (dp, t + 1 - 2 * (t % 2))
    peers["far"] = (dp, t + 2 - 4 * ((t // 2) % 2))
    barrier = pltpu.get_barrier_semaphore()
    for peer in peers.values():
        pl.semaphore_signal(barrier, inc=1, device_id=peer, device_id_type=pl.DeviceIdType.MESH)
    pl.semaphore_wait(barrier, len(peers))

    copies = {}

    def send(key, source, target, peer):
        slot = len(copies)
        copy = pltpu.make_async_remote_copy(
            src_ref=source,
            dst_ref=target,
            send_sem=send_sem.at[slot],
            recv_sem=recv_sem.at[slot],
            device_id=peers[peer],
            device_id_type=pl.DeviceIdType.MESH,
        )
        copy.start()
        copies[key] = copy

    subs = []
    for which, count in enumerate(counts):
        quarter = pieces[4 * which : 4 * which + 4]
        for k in range(count // chunk):
            subs.append((quarter, pl.ds(k * chunk, chunk), len(subs) * chunk))
    places = [[None] * (len(levels) + 1) for _ in subs]
    locals_ = []
    small_out[...] = small_in[...]
    for i, (quarter, rows, base) in enumerate(subs):
        here = pl.ds(base, chunk)
        send((i, "near_cross"), quarter[3].at[rows, :], near_cross.at[here, :], "core")
        send((i, "near_own"), quarter[1].at[rows, :], near_own.at[here, :], "core")
        pair = []
        for j, (source, target) in enumerate(((quarter[2], cross), (quarter[0], own))):
            copy = pltpu.make_async_copy(
                source.at[rows, :], target.at[here, :], local_sem.at[2 * i + j]
            )
            copy.start()
            pair.append(copy)
        locals_.append(pair)
        places[i][0] = base

    def level_send(i, k):
        base = subs[i][2]
        mask, before, after, spot = levels[k]
        at = places[i][k]
        if after == before:
            keep = leave = at
        else:
            keep = at + bits[mask] * after
            leave = at + after - bits[mask] * after
        places[i][k + 1] = keep
        land = (base // chunk) * place + spot
        send(
            (i, "down", k),
            own.at[pl.ds(pl.multiple_of(leave, 16), after), :],
            landing.at[pl.ds(land, after), :],
            mask,
        )

    halved = [k for k, level in enumerate(levels) if level[2] != level[1]]

    def up_send(i, k):
        mask, _, after, _ = levels[k]
        rows = pl.ds(pl.multiple_of(places[i][k + 1], 16), after)
        send((i, "up", k), gathered.at[rows, :], gathered.at[rows, :], mask)

    def start_cross(i):
        base = subs[i][2]
        for copy in locals_[i]:
            copy.wait()
        copies[(i, "near_cross")].wait_recv()
        add_rows(cross, base, near_cross, base, chunk)
        here = pl.ds(base, chunk)
        send((i, "far"), cross.at[here, :], far.at[here, :], "far")
        copies[(i, "near_own")].wait_recv()
        add_rows(own, base, near_own, base, chunk)

    def take_far(i):
        base = subs[i][2]
        copies[(i, "far")].wait_recv()
        add_rows(own, base, far, base, chunk)
        level_send(i, 0)

    def take_level(i, k):
        base = subs[i][2]
        _, before, after, spot = levels[k]
        copies[(i, "down", k)].wait_recv()
        if after == before:
            copies[(i, "down", k)].wait_send()
        add_rows(
            own,
            places[i][k + 1],
            landing,
            (base // chunk) * place + spot,
            after,
            gathered if k + 1 == len(levels) else None,
        )
        if k + 1 < len(levels):
            level_send(i, k + 1)
        elif halved:
            up_send(i, halved[-1])

    def take_up(i, n):
        copies[(i, "up", halved[-1 - n])].wait_recv()
        if n + 1 < len(halved):
            up_send(i, halved[-2 - n])

    def small_step(n):
        names = ["core", "far"] + list(masks)
        spans = [(0, 24), (16, 16)] + [(16, 24)] * len(masks)
        first, count = spans[n]
        copies[("small", n)].wait()
        land = small_land.at[n]
        small_out[16:24, :] += land[16 - first : 24 - first, :]
        if n == 0:
            small_out[32:40, :] += land[0:8, :]
            small_out[24:32, :] += land[8:16, :]
        elif n == 1:
            small_out[32:40, :] += land[8:16, :]
        else:
            small_out[32:40, :] += land[16:24, :]
        if n + 1 < len(names):
            small_send(n + 1, names, spans)

    def small_send(n, names, spans):
        first, count = spans[n]
        send(
            ("small", n),
            small_out.at[pl.ds(first, count), :],
            small_land.at[n, pl.ds(0, count), :],
            names[n],
        )

    small_send(0, ["core", "far"] + list(masks), [(0, 24), (16, 16)] + [(16, 24)] * len(masks))
    tasks = []
    for i in range(len(subs)):
        tasks.append((0.5 * i, i, functools.partial(start_cross, i)))
        tasks.append((i + 1.0, i, functools.partial(take_far, i)))
        for k in range(len(levels)):
            tasks.append((i + 2.0 + k, i, functools.partial(take_level, i, k)))
        for n in range(len(halved)):
            tasks.append((i + 2.0 + len(levels) + n, i, functools.partial(take_up, i, n)))
    for n in range(2 + len(masks)):
        tasks.append((n + 1.5, -1, functools.partial(small_step, n)))
    for _, _, task in sorted(tasks, key=lambda entry: entry[:2]):
        task()
    for key, copy in copies.items():
        repeated = key[0] == "small" or (
            key[1] == "down" and levels[key[2]][1] == levels[key[2]][2]
        )
        if not repeated:
            copy.wait_send()
    out_ref[...] = gathered[...]


def reduce_all(masks, groups, small):
    dim = small.shape[1]
    counts = [group[0].shape[0] for group in groups]
    total = sum(counts)
    levels, place = plan_levels(masks, CHUNK)
    subs = total // CHUNK
    halved = sum(level[1] != level[2] for level in levels)
    copies = subs * (3 + len(levels) + halved) + 2 + len(masks)
    anywhere = pl.BlockSpec(memory_space=pl.ANY)
    local = pl.BlockSpec(memory_space=pltpu.VMEM)
    buffer = pltpu.VMEM((total, dim), BF)
    flat = [piece for group in groups for piece in group]
    return pl.pallas_call(
        functools.partial(reduce_kernel, masks, CHUNK, counts),
        in_specs=[anywhere] * len(flat) + [local],
        out_specs=[local, local],
        out_shape=[
            jax.ShapeDtypeStruct((total, dim), BF),
            jax.ShapeDtypeStruct(small.shape, F32),
        ],
        scratch_shapes=[
            buffer,
            buffer,
            buffer,
            buffer,
            buffer,
            pltpu.VMEM((subs * place, dim), BF),
            buffer,
            pltpu.VMEM((2 + len(masks), 24, dim), F32),
            pltpu.SemaphoreType.DMA((copies,)),
            pltpu.SemaphoreType.DMA((copies,)),
            pltpu.SemaphoreType.DMA((2 * subs,)),
        ],
        compiler_params=pltpu.CompilerParams(
            collective_id=0, has_side_effects=True, vmem_limit_bytes=VMEM_LIMIT
        ),
        name="reduce_all",
    )(*flat, small)


class Comm:
    def __init__(self, ndp, nt):
        self.ndp, self.nt = ndp, nt
        self.dp = lax.axis_index("dp")
        self.t = lax.axis_index("tensor")
        self.masks = []
        mask = 1
        while mask < ndp:
            self.masks.append(mask)
            mask *= 2

    def swap(self, value, dp_mask=0, t_mask=0):
        count = self.ndp * self.nt
        mask = dp_mask * self.nt + t_mask
        return lax.ppermute(value, AXES, [(i, i ^ mask) for i in range(count)])

    def gather_weight(self, shard):
        half = shard.shape[0] // 2
        bit = self.dp & 1
        mine = lax.dynamic_slice_in_dim(shard, bit * half, half, 0)
        far = self.swap(mine, t_mask=2)
        near = self.swap(shard, t_mask=1)
        other = self.swap(far, dp_mask=1)
        cross = jnp.concatenate([jnp.where(bit == 0, far, other), jnp.where(bit == 0, other, far)], 0)
        return [shard, near, cross, self.swap(cross, t_mask=1)]


def per_device(
    ndp,
    nt,
    caption_tokens,
    caption_lengths,
    output_grad,
    norm_gain,
    norm_bias,
    query_weight,
    query_bias,
    key_weight,
    value_weight,
    value_bias,
    output_weight,
    output_bias,
    second_gain,
    second_bias,
    hidden_weight,
    hidden_bias,
    down_weight,
    down_bias,
):
    comm = Comm(ndp, nt)
    t = comm.t
    rows, dim = caption_tokens.shape
    part = query_weight.shape[1]
    count = rows // LMAX
    lengths = lax.dynamic_slice_in_dim(caption_lengths, t * count, count, 0)
    biases = jnp.pad(
        jnp.stack([jnp.pad(jnp.concatenate([query_bias, value_bias]), (0, dim - 2 * part)), hidden_bias]),
        ((0, PAD - 2), (0, 0)),
    )
    shard = jnp.concatenate([query_weight.T, key_weight.T, value_weight.T, output_weight, biases], 0)
    pieces = comm.gather_weight(shard)
    ups = comm.gather_weight(hidden_weight)
    downs = comm.gather_weight(down_weight)
    rows_of = [widen(piece[4 * part : 4 * part + 2]) for piece in pieces]
    bias = jnp.stack(
        [
            jnp.concatenate([r[0, :part] for r in rows_of]),
            jnp.concatenate([r[0, part : 2 * part] for r in rows_of]),
        ]
    )
    vec = jnp.stack(
        [widen(v) for v in (norm_gain, norm_bias, output_bias, second_gain, second_bias, down_bias)]
    )
    vec = jnp.pad(vec, ((0, 2), (0, 0)))
    normed, q, k, v, probs, mixed, middle, second, weights = forward(
        lengths, caption_tokens, pieces, bias, vec
    )
    actives, up_grads, down_grads, hidden_sums = [None] * 4, [None] * 4, [None] * 4, [None] * 4
    inner = None
    for j in (3, 2, 1, 0):
        actives[j], inner, up_grads[j], down_grads[j], hidden_sums[j] = expert(
            second, output_grad, ups[j], downs[j], rows_of[j][1:2], inner
        )
    middle_grad, dq, dk, dv, g0, g1, g2, g3, small = backward(
        output_grad, middle, inner, mixed, q, k, v, probs, normed, weights, vec
    )
    token_grad, last_small = input_back(caption_tokens, middle_grad, dq, dk, dv, weights, vec)
    result = layer_result(middle, actives, downs, vec)
    shared = jnp.pad(jnp.concatenate([last_small[:2], small[:4]], 0), ((0, 2), (0, 0)))
    by_quarter = jnp.pad(
        jnp.stack(
            [
                jnp.pad(small[4:6].reshape(2, 4, part).swapaxes(0, 1).reshape(4, 2 * part), ((0, 0), (0, dim - 2 * part))),
                jnp.stack([sums[0] for sums in hidden_sums]),
            ],
            1,
        ),
        ((0, 0), (0, 6), (0, 0)),
    )
    packed = jnp.concatenate([by_quarter[1], by_quarter[3], shared, by_quarter[2], by_quarter[0]], 0)
    grads, packed = reduce_all(tuple(comm.masks), [up_grads, down_grads, [g0, g1, g2, g3]], packed)
    grads = widen(grads)
    grad_att = grads[2 * dim :]
    sums, mine = packed[16:24], packed[32:34]
    return (
        result,
        token_grad,
        sums[0],
        sums[1],
        grad_att[:part].T,
        mine[0, :part],
        grad_att[part : 2 * part].T,
        grad_att[2 * part : 3 * part].T,
        mine[0, part : 2 * part],
        grad_att[3 * part :],
        sums[2],
        sums[3],
        sums[4],
        grads[:dim],
        mine[1],
        grads[dim : 2 * dim],
        sums[5],
    )


def solution(mesh):
    ndp, nt = mesh.shape["dp"], mesh.shape["tensor"]
    both = P(("dp", "tensor"), None)
    col, row, vec = P(None, "tensor"), P("tensor", None), P("tensor")

    def body(*args):
        return per_device(ndp, nt, *args)

    return jax.shard_map(
        body,
        mesh=mesh,
        in_specs=(both, P("dp"), both, P(), P(), col, vec, col, col, vec, row, P(), P(), P(), col, vec, row, P()),
        out_specs=(both, both, P(), P(), col, vec, col, col, vec, row, P(), P(), P(), col, vec, row, P()),
        check_vma=False,
    )
```

```python
import functools
import math

import jax
import jax.numpy as jnp
from jax import lax
from jax.experimental import pallas as pl
from jax.experimental.pallas import tpu as pltpu
from jax.sharding import PartitionSpec as P


HDIM = 64
LMAX = 64
EPS = 1e-05
NEG = -1e30
GROUP = 4
BLOCK = 256
PAD = 32
CHUNK = 128
TILE = 64
AXES = ("dp", "tensor")
BF = jnp.bfloat16
F32 = jnp.float32
VMEM_LIMIT = 60 * 1024 * 1024


def widen(values):
    return values.astype(F32)


def dot_nn(left, right):
    return jnp.dot(left, right, preferred_element_type=F32)


def dot_nt(left, right):
    return lax.dot_general(left, right, (((1,), (1,)), ((), ())), preferred_element_type=F32)


def dot_tn(left, right):
    return lax.dot_general(left, right, (((0,), (0,)), ((), ())), preferred_element_type=F32)


def normalize(values):
    center = jnp.mean(values, -1, keepdims=True)
    spread = values - center
    scale = lax.rsqrt(jnp.mean(spread * spread, -1, keepdims=True) + EPS)
    return spread * scale, scale


def normalize_back(grad, unit, scale):
    return scale * (
        grad - jnp.mean(grad, -1, keepdims=True) - unit * jnp.mean(grad * unit, -1, keepdims=True)
    )


def erf(values):
    values = jnp.clip(values, -4.0, 4.0)
    square = values * values
    top = -2.72614225801306e-10
    for coef in (
        2.77068142495902e-08,
        -2.10102402082508e-06,
        -5.69250639462346e-05,
        -7.34990630326855e-04,
        -2.95459980854025e-03,
        -1.60960333262415e-02,
    ):
        top = top * square + coef
    low = -1.45660718464996e-05
    for coef in (
        -2.13374055278905e-04,
        -1.68282697438203e-03,
        -7.37332916720468e-03,
        -1.42647390514189e-02,
    ):
        low = low * square + coef
    return values * top / low


def diagonal_mask(size):
    rows = lax.shift_right_logical(lax.broadcasted_iota(jnp.int32, (size, size), 0), 6)
    cols = lax.shift_right_logical(lax.broadcasted_iota(jnp.int32, (size, size), 1), 6)
    return jnp.where(rows == cols, 1.0, 0.0).astype(BF)


def spread_heads(values, mask):
    return jnp.concatenate([values] * GROUP, 0) * mask


def pick_heads(values):
    lane = lax.shift_right_logical(
        lax.broadcasted_iota(jnp.int32, (LMAX, values.shape[1]), 1), 6
    )
    out = values[:LMAX]
    for head in range(1, GROUP):
        out = jnp.where(lane == head, values[head * LMAX : (head + 1) * LMAX], out)
    return out


def full(shape):
    return pl.BlockSpec(shape, lambda i, *_: (0,) * len(shape))


def rowed(width):
    return pl.BlockSpec((BLOCK, width), lambda i, *_: (i, 0))


def params():
    return pltpu.CompilerParams(
        dimension_semantics=("arbitrary",), vmem_limit_bytes=VMEM_LIMIT
    )


def split_rows(rows):
    count = rows // 16
    spans, start = [], 0
    for k in range(3):
        size = (count * (k + 1) // 3 - count * k // 3) * 16
        spans.append((start, size))
        start += size
    return spans


def forward_kernel(
    length_ref,
    tokens_ref,
    shard_ref,
    up_ref,
    down_ref,
    vec_ref,
    normed_ref,
    q_ref,
    k_ref,
    v_ref,
    probs_ref,
    mixed_ref,
    middle_ref,
    second_ref,
    weights_ref,
    bias_ref,
    up_near,
    up_cross,
    up_last,
    down_near,
    down_cross,
    down_last,
    mask_ref,
    land_ref,
    vector_s,
    send_sem,
    recv_sem,
    local_sem,
):
    step = pl.program_id(0)
    dim = tokens_ref.shape[1]
    part = dim // 4
    dp = lax.axis_index("dp")
    t = lax.axis_index("tensor")
    bit = dp % 2
    peers = {
        "core": (dp, t + 1 - 2 * (t % 2)),
        "far": (dp, t + 2 - 4 * ((t // 2) % 2)),
        "side": (dp + 1 - 2 * bit, t),
    }
    chunks = [
        (shard_ref, land_ref.at[1], land_ref.at[2], land_ref.at[3]),
        (up_ref, up_near, up_cross, up_last),
        (down_ref, down_near, down_cross, down_last),
    ]
    recipes = {}

    def recipe(key, source, target, peer):
        recipes[key] = (len(recipes), source, target, peer)

    for c, (shard, near, cross, last) in enumerate(chunks):
        half = shard.shape[0] // 2
        recipe((c, "near"), shard, near, "core")
        for n, (start, size) in enumerate(split_rows(half)):
            mine = pl.ds(pl.multiple_of(bit * half + start, 16), size)
            other = pl.ds(pl.multiple_of((1 - bit) * half + start, 16), size)
            recipe((c, "y", n), shard.at[mine, :], cross.at[mine, :], "far")
            recipe((c, "x", n), cross.at[mine, :], cross.at[mine, :], "side")
            recipe((c, "a", n), cross.at[mine, :], last.at[mine, :], "core")
            recipe((c, "b", n), cross.at[other, :], last.at[other, :], "core")

    def copy(key):
        slot, source, target, peer = recipes[key]
        return pltpu.make_async_remote_copy(
            src_ref=source,
            dst_ref=target,
            send_sem=send_sem.at[slot],
            recv_sem=recv_sem.at[slot],
            device_id=peers[peer],
            device_id_type=pl.DeviceIdType.MESH,
        )

    def pass_y(c, n):
        copy((c, "y", n)).wait_recv()
        copy((c, "x", n)).start()
        copy((c, "a", n)).start()

    def pass_x(c, n):
        copy((c, "x", n)).wait_recv()
        copy((c, "b", n)).start()

    @pl.when(step == 0)
    def _():
        barrier = pltpu.get_barrier_semaphore()
        for peer in peers.values():
            pl.semaphore_signal(
                barrier, inc=1, device_id=peer, device_id_type=pl.DeviceIdType.MESH
            )
        pl.semaphore_wait(barrier, 3)
        own = pltpu.make_async_copy(shard_ref, land_ref.at[0], local_sem)
        own.start()
        for c in range(3):
            for n in range(3):
                copy((c, "y", n)).start()
            copy((c, "near")).start()
        mask_ref[...] = diagonal_mask(GROUP * HDIM)
        own.wait()
        pass_y(0, 0)
        pass_y(0, 1)
        pass_x(0, 0)
        pass_y(0, 2)
        pass_x(0, 1)
        pass_x(0, 2)
        copy((0, "near")).wait_recv()
        for n in range(3):
            copy((0, "a", n)).wait_recv()
            copy((0, "b", n)).wait_recv()
        for j in range(4):
            for kind in range(4):
                weights_ref[kind, j * part : (j + 1) * part, :] = land_ref[
                    j, kind * part : (kind + 1) * part, :
                ]
        rows = [widen(land_ref[j, 4 * part : 4 * part + 16, :]) for j in range(4)]
        vector_s[0:1, :] = jnp.concatenate([r[0:1, :part] for r in rows], 1)
        vector_s[1:2, :] = jnp.concatenate([r[2:3, :part] for r in rows], 1)
        for j in range(4):
            bias_ref[8 * j : 8 * j + 8, :] = jnp.broadcast_to(rows[j][1:2], (8, dim))
        pass_y(1, 0)
        pass_y(1, 1)

    @pl.when(step == 1)
    def _():
        pass_x(1, 0)
        pass_y(1, 2)
        pass_x(1, 1)
        pass_y(2, 0)

    @pl.when(step == 2)
    def _():
        pass_x(1, 2)
        pass_y(2, 1)
        pass_x(2, 0)

    @pl.when(step == 3)
    def _():
        pass_y(2, 2)
        pass_x(2, 1)

    tokens = widen(tokens_ref[...])
    vec = vec_ref[...]
    unit, _ = normalize(tokens)
    normed = (unit * vec[0:1] + vec[1:2]).astype(BF)
    normed_ref[...] = normed
    q_ref[...] = (dot_nt(normed, weights_ref[0]) + vector_s[0:1, :]).astype(BF)
    k_ref[...] = dot_nt(normed, weights_ref[1]).astype(BF)
    v_ref[...] = (dot_nt(normed, weights_ref[2]) + vector_s[1:2, :]).astype(BF)
    width = GROUP * HDIM
    factor = 1.0 / math.sqrt(HDIM)
    mask = mask_ref[...]
    for c in range(BLOCK // LMAX):
        rows = pl.ds(c * LMAX, LMAX)
        length = length_ref[step * (BLOCK // LMAX) + c]
        live = lax.broadcasted_iota(jnp.int32, (LMAX, width), 0) < length
        for g in range(dim // width):
            cols = pl.ds(g * width, width)
            wide = spread_heads(q_ref[rows, cols], mask)
            scores = dot_nt(k_ref[rows, cols], wide) * factor
            scores = jnp.where(live, scores, NEG)
            exponent = jnp.exp(scores - jnp.max(scores, 0, keepdims=True))
            probs = exponent * (1.0 / jnp.sum(exponent, 0, keepdims=True))
            probs_ref[rows, cols] = probs
            crossed = dot_tn(probs.astype(BF), v_ref[rows, cols])
            mixed_ref[rows, cols] = pick_heads(crossed).astype(BF)
    middle = tokens + dot_nn(mixed_ref[...], weights_ref[3]) + vec[2:3]
    middle_ref[...] = middle
    unit, _ = normalize(middle)
    second_ref[...] = (unit * vec[3:4] + vec[4:5]).astype(BF)

    @pl.when(step == pl.num_programs(0) - 1)
    def _():
        pass_x(2, 2)
        for c in (1, 2):
            copy((c, "near")).wait_recv()
            for n in range(3):
                copy((c, "a", n)).wait_recv()
                copy((c, "b", n)).wait_recv()
        for key in recipes:
            copy(key).wait_send()


def forward(lengths, tokens, shard, up, down, vec):
    rows, dim = tokens.shape
    steps = rows // BLOCK
    shapes = [
        (dim, BF),
        (dim, BF),
        (dim, BF),
        (dim, BF),
        (dim, F32),
        (dim, BF),
        (dim, F32),
        (dim, BF),
    ]
    anywhere = pl.BlockSpec(memory_space=pl.ANY)
    copies = 3 * 13
    return pl.pallas_call(
        forward_kernel,
        grid_spec=pltpu.PrefetchScalarGridSpec(
            num_scalar_prefetch=1,
            grid=(steps,),
            in_specs=[rowed(dim), anywhere, anywhere, anywhere, full(vec.shape)],
            out_specs=[rowed(width) for width, _ in shapes]
            + [full((4, dim, dim)), full((32, dim))]
            + [anywhere] * 6,
            scratch_shapes=[
                pltpu.VMEM((GROUP * HDIM, GROUP * HDIM), BF),
                pltpu.VMEM((4,) + shard.shape, BF),
                pltpu.VMEM((8, dim), F32),
                pltpu.SemaphoreType.DMA((copies,)),
                pltpu.SemaphoreType.DMA((copies,)),
                pltpu.SemaphoreType.DMA,
            ],
        ),
        out_shape=[jax.ShapeDtypeStruct((rows, width), kind) for width, kind in shapes]
        + [jax.ShapeDtypeStruct((4, dim, dim), BF), jax.ShapeDtypeStruct((32, dim), F32)]
        + [jax.ShapeDtypeStruct(up.shape, BF)] * 3
        + [jax.ShapeDtypeStruct(down.shape, BF)] * 3,
        compiler_params=pltpu.CompilerParams(
            dimension_semantics=("arbitrary",),
            vmem_limit_bytes=VMEM_LIMIT,
            collective_id=1,
            has_side_effects=True,
        ),
        name="attend",
    )(lengths, tokens, shard, up, down, vec)


def expert_kernel(
    first,
    final,
    second_ref,
    grad_ref,
    up_ref,
    down_ref,
    bias_ref,
    vec_ref,
    sum_ref,
    *refs,
):
    if not first:
        prior_ref, refs = refs[0], refs[1:]
    result_ref, total_ref, up_grad_ref, down_grad_ref, bias_grad_ref, active_s, hidden_s = refs
    step = pl.program_id(0)
    rows = pl.ds(pl.multiple_of(step * BLOCK, BLOCK), BLOCK)
    hidden = dot_nn(second_ref[rows, :], up_ref[...]) + bias_ref[0:1, :]
    lean = 0.5 + 0.5 * erf(hidden * (1.0 / math.sqrt(2.0)))
    slope = lean + hidden * (jnp.exp(-0.5 * hidden * hidden) * (1.0 / math.sqrt(2.0 * math.pi)))
    active = (hidden * lean).astype(BF)
    active_s[rows, :] = active
    result = sum_ref[...] + dot_nn(active, down_ref[...])
    if final:
        result = result + vec_ref[5:6, :]
    result_ref[...] = result.astype(result_ref.dtype)
    back = (dot_nt(grad_ref[rows, :], down_ref[...]) * slope).astype(BF)
    hidden_s[rows, :] = back
    total = dot_nt(back, up_ref[...])
    total_ref[...] = total if first else total + prior_ref[...]

    @pl.when(step == pl.num_programs(0) - 1)
    def _():
        down_grad_ref[...] = dot_tn(active_s[...], grad_ref[...]).astype(BF)
        up_grad_ref[...] = dot_tn(second_ref[...], hidden_s[...]).astype(BF)
        bias_grad_ref[...] = jnp.broadcast_to(
            jnp.sum(widen(hidden_s[...]), 0, keepdims=True), bias_grad_ref.shape
        )


def expert(j, final, second, grad, up, down, bias, vec, result, prior):
    rows, dim = second.shape
    units = up.shape[1]
    first = prior is None
    args = [second, grad, up, down, bias, vec, result] + ([] if first else [prior])
    return pl.pallas_call(
        functools.partial(expert_kernel, first, final),
        grid=(rows // BLOCK,),
        in_specs=[full(a.shape) for a in args[:4]]
        + [pl.BlockSpec((8, units), lambda i: (j, 0)), full(vec.shape), rowed(dim)]
        + ([] if first else [rowed(dim)]),
        out_specs=[
            rowed(dim),
            rowed(dim),
            full((dim, units)),
            full((units, dim)),
            full((8, units)),
        ],
        out_shape=[
            jax.ShapeDtypeStruct((rows, dim), BF if final else F32),
            jax.ShapeDtypeStruct((rows, dim), F32),
            jax.ShapeDtypeStruct((dim, units), BF),
            jax.ShapeDtypeStruct((units, dim), BF),
            jax.ShapeDtypeStruct((8, units), F32),
        ],
        scratch_shapes=[pltpu.VMEM((rows, units), BF), pltpu.VMEM((rows, units), BF)],
        compiler_params=params(),
        cost_estimate=pl.CostEstimate(
            flops=12 * rows * dim * units,
            bytes_accessed=20 * rows * dim,
            transcendentals=2 * rows * units,
        ),
        name="expert",
    )(*args)


def backward_kernel(
    grad_ref,
    middle_ref,
    inner_ref,
    mixed_ref,
    q_ref,
    k_ref,
    v_ref,
    probs_ref,
    normed_ref,
    out_weight_ref,
    vec_ref,
    middle_grad_ref,
    dq_ref,
    dk_ref,
    dv_ref,
    g0,
    g1,
    g2,
    g3,
    small_ref,
    mask_ref,
    low_s,
    mixed_grad_s,
):
    step = pl.program_id(0)
    dim = grad_ref.shape[1]
    part = dim // 4

    @pl.when(step == 0)
    def _():
        mask_ref[...] = diagonal_mask(GROUP * HDIM)
        small_ref[...] = jnp.zeros_like(small_ref)

    all_rows = pl.ds(pl.multiple_of(step * BLOCK, BLOCK), BLOCK)
    vec = vec_ref[...]
    upstream = widen(grad_ref[...])
    unit, scale = normalize(middle_ref[...])
    inner = inner_ref[...]
    middle_grad = upstream + normalize_back(inner * vec[3:4], unit, scale)
    middle_grad_ref[...] = middle_grad
    middle_low = middle_grad.astype(BF)
    low_s[all_rows, :] = middle_low
    small_ref[0:1, :] += jnp.sum(middle_grad, 0, keepdims=True)
    small_ref[1:2, :] += jnp.sum(inner * unit, 0, keepdims=True)
    small_ref[2:3, :] += jnp.sum(inner, 0, keepdims=True)
    small_ref[3:4, :] += jnp.sum(upstream, 0, keepdims=True)
    mixed_grad_s[...] = dot_nt(middle_low, out_weight_ref[0]).astype(BF)
    width = GROUP * HDIM
    factor = 1.0 / math.sqrt(HDIM)
    mask = mask_ref[...]
    for c in range(BLOCK // LMAX):
        rows = pl.ds(c * LMAX, LMAX)
        into = pl.ds(pl.multiple_of(step * BLOCK + c * LMAX, LMAX), LMAX)
        for g in range(dim // width):
            cols = pl.ds(g * width, width)
            wide = spread_heads(mixed_grad_s[rows, cols], mask)
            probs = probs_ref[rows, cols]
            prob_grad = dot_nt(v_ref[rows, cols], wide)
            dv_ref[into, cols] = dot_nn(probs.astype(BF), wide).astype(BF)
            weighted = jnp.sum(probs * prob_grad, 0, keepdims=True)
            score_grad = (probs * (prob_grad - weighted)).astype(BF)
            queries = spread_heads(q_ref[rows, cols], mask)
            dk_ref[into, cols] = (dot_nn(score_grad, queries) * factor).astype(BF)
            crossed = dot_tn(score_grad, k_ref[rows, cols])
            dq_ref[into, cols] = (pick_heads(crossed) * factor).astype(BF)

    @pl.when(step == pl.num_programs(0) - 1)
    def _():
        small_ref[4:5, :] = jnp.sum(widen(dq_ref[...]), 0, keepdims=True)
        small_ref[5:6, :] = jnp.sum(widen(dv_ref[...]), 0, keepdims=True)
        for kind, (left, right) in enumerate(
            ((dq_ref, normed_ref), (dk_ref, normed_ref), (dv_ref, normed_ref), (mixed_ref, low_s))
        ):
            result = dot_tn(left[...], right[...]).astype(BF)
            for j, piece in enumerate((g0, g1, g2, g3)):
                piece[kind * part : (kind + 1) * part, :] = result[j * part : (j + 1) * part]


def backward(grad, middle, inner, mixed, q, k, v, probs, normed, weights, vec):
    rows, dim = grad.shape
    whole = full((rows, dim))
    return pl.pallas_call(
        backward_kernel,
        grid=(rows // BLOCK,),
        in_specs=[rowed(dim), rowed(dim), rowed(dim), whole]
        + [rowed(dim)] * 4
        + [whole, pl.BlockSpec((1, dim, dim), lambda i: (3, 0, 0)), full(vec.shape)],
        out_specs=[rowed(dim), whole, whole, whole] + [full((dim, dim))] * 4 + [full((8, dim))],
        out_shape=[
            jax.ShapeDtypeStruct((rows, dim), F32),
            jax.ShapeDtypeStruct((rows, dim), BF),
            jax.ShapeDtypeStruct((rows, dim), BF),
            jax.ShapeDtypeStruct((rows, dim), BF),
        ]
        + [jax.ShapeDtypeStruct((dim, dim), BF)] * 4
        + [jax.ShapeDtypeStruct((8, dim), F32)],
        scratch_shapes=[
            pltpu.VMEM((GROUP * HDIM, GROUP * HDIM), BF),
            pltpu.VMEM((rows, dim), BF),
            pltpu.VMEM((BLOCK, dim), BF),
        ],
        compiler_params=params(),
        cost_estimate=pl.CostEstimate(
            flops=14 * rows * dim * dim, bytes_accessed=40 * rows * dim, transcendentals=0
        ),
        name="attend_back",
    )(grad, middle, inner, mixed, q, k, v, probs, normed, weights, vec)


def input_kernel(
    tokens_ref, middle_grad_ref, dq_ref, dk_ref, dv_ref, weights_ref, vec_ref, out_ref, small_ref
):
    @pl.when(pl.program_id(0) == 0)
    def _():
        small_ref[...] = jnp.zeros_like(small_ref)

    unit, scale = normalize(widen(tokens_ref[...]))
    grad = (
        dot_nn(dq_ref[...], weights_ref[0])
        + dot_nn(dk_ref[...], weights_ref[1])
        + dot_nn(dv_ref[...], weights_ref[2])
    )
    small_ref[0:1, :] += jnp.sum(grad * unit, 0, keepdims=True)
    small_ref[1:2, :] += jnp.sum(grad, 0, keepdims=True)
    back = normalize_back(grad * vec_ref[0:1, :], unit, scale)
    out_ref[...] = (middle_grad_ref[...] + back).astype(BF)


def input_back(tokens, middle_grad, dq, dk, dv, weights, vec):
    rows, dim = tokens.shape
    return pl.pallas_call(
        input_kernel,
        grid=(rows // BLOCK,),
        in_specs=[rowed(dim)] * 5 + [full((3, dim, dim)), full(vec.shape)],
        out_specs=[rowed(dim), full((8, dim))],
        out_shape=[
            jax.ShapeDtypeStruct((rows, dim), BF),
            jax.ShapeDtypeStruct((8, dim), F32),
        ],
        compiler_params=params(),
        cost_estimate=pl.CostEstimate(
            flops=6 * rows * dim * dim, bytes_accessed=14 * rows * dim, transcendentals=0
        ),
        name="input_back",
    )(tokens, middle_grad, dq, dk, dv, weights, vec)


def add_rows(into, base, other, other_base, rows, result=None):
    result = into if result is None else result
    size = min(rows, TILE)

    def body(i, carry):
        left = pl.ds(pl.multiple_of(base + i * size, 8), size)
        right = pl.ds(pl.multiple_of(other_base + i * size, 8), size)
        result[left, :] = (widen(into[left, :]) + widen(other[right, :])).astype(into.dtype)
        return carry

    lax.fori_loop(0, rows // size, body, 0)


def plan_levels(masks, rows):
    levels, place = [], 0
    for mask in masks:
        after = rows // 2 if (rows // 2) % 16 == 0 else rows
        levels.append((mask, rows, after, place))
        place += after
        rows = after
    return levels, place


def reduce_kernel(masks, chunk, counts, *refs):
    pieces, refs = refs[: 4 * len(counts)], refs[4 * len(counts) :]
    small_in, refs = refs[0], refs[1:]
    out_refs, refs = refs[: len(counts)], refs[len(counts) :]
    small_out, own, cross, near_own, near_cross, far, landing = refs[:7]
    gathered, small_land, send_sem, recv_sem, local_sem = refs[7:]
    levels, place = plan_levels(masks, chunk)
    dp = lax.axis_index("dp")
    t = lax.axis_index("tensor")
    bits = {mask: (dp // mask) % 2 for mask in masks}
    peers = {mask: (dp + mask - 2 * mask * bits[mask], t) for mask in masks}
    peers["core"] = (dp, t + 1 - 2 * (t % 2))
    peers["far"] = (dp, t + 2 - 4 * ((t // 2) % 2))
    barrier = pltpu.get_barrier_semaphore()
    for peer in peers.values():
        pl.semaphore_signal(barrier, inc=1, device_id=peer, device_id_type=pl.DeviceIdType.MESH)
    pl.semaphore_wait(barrier, len(peers))

    copies = {}

    def send(key, source, target, peer):
        slot = len(copies)
        copy = pltpu.make_async_remote_copy(
            src_ref=source,
            dst_ref=target,
            send_sem=send_sem.at[slot],
            recv_sem=recv_sem.at[slot],
            device_id=peers[peer],
            device_id_type=pl.DeviceIdType.MESH,
        )
        copy.start()
        copies[key] = copy

    subs = []
    for which, count in enumerate(counts):
        quarter = pieces[4 * which : 4 * which + 4]
        for k in range(count // chunk):
            subs.append((quarter, pl.ds(k * chunk, chunk), len(subs) * chunk))
    places = [[None] * (len(levels) + 1) for _ in subs]
    locals_ = []
    small_out[...] = small_in[...]
    for i, (quarter, rows, base) in enumerate(subs):
        here = pl.ds(base, chunk)
        send((i, "near_cross"), quarter[3].at[rows, :], near_cross.at[here, :], "core")
        send((i, "near_own"), quarter[1].at[rows, :], near_own.at[here, :], "core")
        pair = []
        for j, (source, target) in enumerate(((quarter[2], cross), (quarter[0], own))):
            copy = pltpu.make_async_copy(
                source.at[rows, :], target.at[here, :], local_sem.at[2 * i + j]
            )
            copy.start()
            pair.append(copy)
        locals_.append(pair)
        places[i][0] = base

    def level_send(i, k):
        base = subs[i][2]
        mask, before, after, spot = levels[k]
        at = places[i][k]
        if after == before:
            keep = leave = at
        else:
            keep = at + bits[mask] * after
            leave = at + after - bits[mask] * after
        places[i][k + 1] = keep
        land = (base // chunk) * place + spot
        send(
            (i, "down", k),
            own.at[pl.ds(pl.multiple_of(leave, 16), after), :],
            landing.at[pl.ds(land, after), :],
            mask,
        )

    halved = [k for k, level in enumerate(levels) if level[2] != level[1]]

    def up_send(i, k):
        mask, _, after, _ = levels[k]
        rows = pl.ds(pl.multiple_of(places[i][k + 1], 16), after)
        send((i, "up", k), gathered.at[rows, :], gathered.at[rows, :], mask)

    def start_cross(i):
        base = subs[i][2]
        for copy in locals_[i]:
            copy.wait()
        copies[(i, "near_cross")].wait_recv()
        add_rows(cross, base, near_cross, base, chunk)
        here = pl.ds(base, chunk)
        send((i, "far"), cross.at[here, :], far.at[here, :], "far")
        copies[(i, "near_own")].wait_recv()
        add_rows(own, base, near_own, base, chunk)

    def take_far(i):
        base = subs[i][2]
        copies[(i, "far")].wait_recv()
        add_rows(own, base, far, base, chunk)
        level_send(i, 0)

    def take_level(i, k):
        base = subs[i][2]
        _, before, after, spot = levels[k]
        copies[(i, "down", k)].wait_recv()
        if after == before:
            copies[(i, "down", k)].wait_send()
        add_rows(
            own,
            places[i][k + 1],
            landing,
            (base // chunk) * place + spot,
            after,
            gathered if k + 1 == len(levels) else None,
        )
        if k + 1 < len(levels):
            level_send(i, k + 1)
        elif halved:
            up_send(i, halved[-1])

    def take_up(i, n):
        copies[(i, "up", halved[-1 - n])].wait_recv()
        if n + 1 < len(halved):
            up_send(i, halved[-2 - n])

    def small_step(n):
        names = ["core", "far"] + list(masks)
        spans = [(0, 24), (16, 16)] + [(16, 24)] * len(masks)
        first, count = spans[n]
        copies[("small", n)].wait()
        land = small_land.at[n]
        small_out[16:24, :] += land[16 - first : 24 - first, :]
        if n == 0:
            small_out[32:40, :] += land[0:8, :]
            small_out[24:32, :] += land[8:16, :]
        elif n == 1:
            small_out[32:40, :] += land[8:16, :]
        else:
            small_out[32:40, :] += land[16:24, :]
        if n + 1 < len(names):
            small_send(n + 1, names, spans)

    def small_send(n, names, spans):
        first, count = spans[n]
        send(
            ("small", n),
            small_out.at[pl.ds(first, count), :],
            small_land.at[n, pl.ds(0, count), :],
            names[n],
        )

    small_send(0, ["core", "far"] + list(masks), [(0, 24), (16, 16)] + [(16, 24)] * len(masks))
    tasks = []
    for i in range(len(subs)):
        tasks.append((0.5 * i, i, functools.partial(start_cross, i)))
        tasks.append((i + 1.0, i, functools.partial(take_far, i)))
        for k in range(len(levels)):
            tasks.append((i + 2.0 + k, i, functools.partial(take_level, i, k)))
        for n in range(len(halved)):
            tasks.append((i + 2.0 + len(levels) + n, i, functools.partial(take_up, i, n)))
    for n in range(2 + len(masks)):
        tasks.append((n + 1.5, -1, functools.partial(small_step, n)))
    for _, _, task in sorted(tasks, key=lambda entry: entry[:2]):
        task()
    for key, copy in copies.items():
        repeated = key[0] == "small" or (
            key[1] == "down" and levels[key[2]][1] == levels[key[2]][2]
        )
        if not repeated:
            copy.wait_send()
    start = 0
    for out_ref, count in zip(out_refs, counts):
        out_ref[...] = gathered[start : start + count, :]
        start += count


def reduce_all(masks, groups, small):
    dim = small.shape[1]
    counts = [group[0].shape[0] for group in groups]
    total = sum(counts)
    levels, place = plan_levels(masks, CHUNK)
    subs = total // CHUNK
    halved = sum(level[1] != level[2] for level in levels)
    copies = subs * (3 + len(levels) + halved) + 2 + len(masks)
    anywhere = pl.BlockSpec(memory_space=pl.ANY)
    local = pl.BlockSpec(memory_space=pltpu.VMEM)
    buffer = pltpu.VMEM((total, dim), BF)
    flat = [piece for group in groups for piece in group]
    return pl.pallas_call(
        functools.partial(reduce_kernel, masks, CHUNK, counts),
        in_specs=[anywhere] * len(flat) + [local],
        out_specs=[local] * (len(groups) + 1),
        out_shape=[jax.ShapeDtypeStruct((count, dim), BF) for count in counts]
        + [jax.ShapeDtypeStruct(small.shape, F32)],
        scratch_shapes=[
            buffer,
            buffer,
            buffer,
            buffer,
            buffer,
            pltpu.VMEM((subs * place, dim), BF),
            buffer,
            pltpu.VMEM((2 + len(masks), 24, dim), F32),
            pltpu.SemaphoreType.DMA((copies,)),
            pltpu.SemaphoreType.DMA((copies,)),
            pltpu.SemaphoreType.DMA((2 * subs,)),
        ],
        compiler_params=pltpu.CompilerParams(
            collective_id=0, has_side_effects=True, vmem_limit_bytes=VMEM_LIMIT
        ),
        name="reduce_all",
    )(*flat, small)


def per_device(
    ndp,
    nt,
    caption_tokens,
    caption_lengths,
    output_grad,
    norm_gain,
    norm_bias,
    query_weight,
    query_bias,
    key_weight,
    value_weight,
    value_bias,
    output_weight,
    output_bias,
    second_gain,
    second_bias,
    hidden_weight,
    hidden_bias,
    down_weight,
    down_bias,
):
    t = lax.axis_index("tensor")
    masks, mask = [], 1
    while mask < ndp:
        masks.append(mask)
        mask *= 2
    rows, dim = caption_tokens.shape
    part = query_weight.shape[1]
    count = rows // LMAX
    lengths = lax.dynamic_slice_in_dim(caption_lengths, t * count, count, 0)
    fill = (0, dim - part)
    biases = jnp.pad(
        jnp.stack([jnp.pad(query_bias, fill), hidden_bias, jnp.pad(value_bias, fill)]),
        ((0, PAD - 3), (0, 0)),
    )
    shard = jnp.concatenate([query_weight.T, key_weight.T, value_weight.T, output_weight, biases], 0)
    vec = jnp.stack(
        [widen(v) for v in (norm_gain, norm_bias, output_bias, second_gain, second_bias, down_bias)]
    )
    vec = jnp.pad(vec, ((0, 2), (0, 0)))
    normed, q, k, v, probs, mixed, middle, second, weights, bias, *rest = forward(
        lengths, caption_tokens, shard, hidden_weight, down_weight, vec
    )
    ups = [hidden_weight] + rest[:3]
    downs = [down_weight] + rest[3:]
    up_grads, down_grads, hidden_sums = [None] * 4, [None] * 4, [None] * 4
    result, inner = middle, None
    for j in (3, 2, 1, 0):
        result, inner, up_grads[j], down_grads[j], hidden_sums[j] = expert(
            j, j == 0, second, output_grad, ups[j], downs[j], bias, vec, result, inner
        )
    middle_grad, dq, dk, dv, g0, g1, g2, g3, small = backward(
        output_grad, middle, inner, mixed, q, k, v, probs, normed, weights, vec
    )
    token_grad, last_small = input_back(caption_tokens, middle_grad, dq, dk, dv, weights, vec)
    shared = jnp.pad(jnp.concatenate([last_small[:2], small[:4]], 0), ((0, 2), (0, 0)))
    by_quarter = jnp.pad(
        jnp.stack(
            [
                jnp.pad(small[4:6].reshape(2, 4, part).swapaxes(0, 1).reshape(4, 2 * part), ((0, 0), (0, dim - 2 * part))),
                jnp.stack([sums[0] for sums in hidden_sums]),
            ],
            1,
        ),
        ((0, 0), (0, 6), (0, 0)),
    )
    packed = jnp.concatenate([by_quarter[1], by_quarter[3], shared, by_quarter[2], by_quarter[0]], 0)
    grad_up, grad_down, grad_att, packed = reduce_all(
        tuple(masks), [up_grads, down_grads, [g0, g1, g2, g3]], packed
    )
    grad_up, grad_down, grad_att = widen(grad_up), widen(grad_down), widen(grad_att)
    sums, mine = packed[16:24], packed[32:34]
    return (
        result,
        token_grad,
        sums[0],
        sums[1],
        grad_att[:part].T,
        mine[0, :part],
        grad_att[part : 2 * part].T,
        grad_att[2 * part : 3 * part].T,
        mine[0, part : 2 * part],
        grad_att[3 * part :],
        sums[2],
        sums[3],
        sums[4],
        grad_up,
        mine[1],
        grad_down,
        sums[5],
    )


def solution(mesh):
    ndp, nt = mesh.shape["dp"], mesh.shape["tensor"]
    both = P(("dp", "tensor"), None)
    col, row, vec = P(None, "tensor"), P("tensor", None), P("tensor")

    def body(*args):
        return per_device(ndp, nt, *args)

    return jax.shard_map(
        body,
        mesh=mesh,
        in_specs=(both, P("dp"), both, P(), P(), col, vec, col, col, vec, row, P(), P(), P(), col, vec, row, P()),
        out_specs=(both, both, P(), P(), col, vec, col, col, vec, row, P(), P(), P(), col, vec, row, P()),
        check_vma=False,
    )
```

```python
import functools
import math

import jax
import jax.numpy as jnp
from jax import lax
from jax.experimental import pallas as pl
from jax.experimental.pallas import tpu as pltpu
from jax.sharding import PartitionSpec as P


HDIM = 64
LMAX = 64
EPS = 1e-05
NEG = -1e30
GROUP = 4
BLOCK = 256
PAD = 32
CHUNK = 128
TILE = 64
AXES = ("dp", "tensor")
BF = jnp.bfloat16
F32 = jnp.float32
VMEM_LIMIT = 60 * 1024 * 1024


def widen(values):
    return values.astype(F32)


def dot_nn(left, right):
    return jnp.dot(left, right, preferred_element_type=F32)


def dot_nt(left, right):
    return lax.dot_general(left, right, (((1,), (1,)), ((), ())), preferred_element_type=F32)


def dot_tn(left, right):
    return lax.dot_general(left, right, (((0,), (0,)), ((), ())), preferred_element_type=F32)


def normalize(values):
    center = jnp.mean(values, -1, keepdims=True)
    spread = values - center
    scale = lax.rsqrt(jnp.mean(spread * spread, -1, keepdims=True) + EPS)
    return spread * scale, scale


def normalize_back(grad, unit, scale):
    return scale * (
        grad - jnp.mean(grad, -1, keepdims=True) - unit * jnp.mean(grad * unit, -1, keepdims=True)
    )


def erf(values):
    values = jnp.clip(values, -4.0, 4.0)
    square = values * values
    top = -2.72614225801306e-10
    for coef in (
        2.77068142495902e-08,
        -2.10102402082508e-06,
        -5.69250639462346e-05,
        -7.34990630326855e-04,
        -2.95459980854025e-03,
        -1.60960333262415e-02,
    ):
        top = top * square + coef
    low = -1.45660718464996e-05
    for coef in (
        -2.13374055278905e-04,
        -1.68282697438203e-03,
        -7.37332916720468e-03,
        -1.42647390514189e-02,
    ):
        low = low * square + coef
    return values * top / low


def diagonal_mask(size):
    rows = lax.shift_right_logical(lax.broadcasted_iota(jnp.int32, (size, size), 0), 6)
    cols = lax.shift_right_logical(lax.broadcasted_iota(jnp.int32, (size, size), 1), 6)
    return jnp.where(rows == cols, 1.0, 0.0).astype(BF)


def spread_heads(values, mask):
    return jnp.concatenate([values] * GROUP, 0) * mask


def pick_heads(values):
    lane = lax.shift_right_logical(
        lax.broadcasted_iota(jnp.int32, (LMAX, values.shape[1]), 1), 6
    )
    out = values[:LMAX]
    for head in range(1, GROUP):
        out = jnp.where(lane == head, values[head * LMAX : (head + 1) * LMAX], out)
    return out


def full(shape):
    return pl.BlockSpec(shape, lambda i, *_: (0,) * len(shape))


def rowed(width):
    return pl.BlockSpec((BLOCK, width), lambda i, *_: (i, 0))


def params():
    return pltpu.CompilerParams(
        dimension_semantics=("arbitrary",), vmem_limit_bytes=VMEM_LIMIT
    )


def split_rows(rows):
    count = rows // 16
    spans, start = [], 0
    for k in range(3):
        size = (count * (k + 1) // 3 - count * k // 3) * 16
        spans.append((start, size))
        start += size
    return spans


def forward_kernel(
    length_ref,
    tokens_ref,
    shard_ref,
    up_ref,
    down_ref,
    vec_ref,
    normed_ref,
    q_ref,
    k_ref,
    v_ref,
    probs_ref,
    mixed_ref,
    middle_ref,
    second_ref,
    weights_ref,
    bias_ref,
    up_near,
    up_cross,
    up_last,
    down_near,
    down_cross,
    down_last,
    mask_ref,
    land_ref,
    vector_s,
    send_sem,
    recv_sem,
    local_sem,
):
    step = pl.program_id(0)
    dim = tokens_ref.shape[1]
    part = dim // 4
    dp = lax.axis_index("dp")
    t = lax.axis_index("tensor")
    bit = dp % 2
    peers = {
        "core": (dp, t + 1 - 2 * (t % 2)),
        "far": (dp, t + 2 - 4 * ((t // 2) % 2)),
        "side": (dp + 1 - 2 * bit, t),
    }
    chunks = [
        (shard_ref, land_ref.at[1], land_ref.at[2], land_ref.at[3]),
        (up_ref, up_near, up_cross, up_last),
        (down_ref, down_near, down_cross, down_last),
    ]
    recipes = {}

    def recipe(key, source, target, peer):
        recipes[key] = (len(recipes), source, target, peer)

    for c, (shard, near, cross, last) in enumerate(chunks):
        half = shard.shape[0] // 2
        recipe((c, "near"), shard, near, "core")
        for n, (start, size) in enumerate(split_rows(half)):
            mine = pl.ds(pl.multiple_of(bit * half + start, 16), size)
            other = pl.ds(pl.multiple_of((1 - bit) * half + start, 16), size)
            recipe((c, "y", n), shard.at[mine, :], cross.at[mine, :], "far")
            recipe((c, "x", n), cross.at[mine, :], cross.at[mine, :], "side")
            recipe((c, "a", n), cross.at[mine, :], last.at[mine, :], "core")
            recipe((c, "b", n), cross.at[other, :], last.at[other, :], "core")

    def copy(key):
        slot, source, target, peer = recipes[key]
        return pltpu.make_async_remote_copy(
            src_ref=source,
            dst_ref=target,
            send_sem=send_sem.at[slot],
            recv_sem=recv_sem.at[slot],
            device_id=peers[peer],
            device_id_type=pl.DeviceIdType.MESH,
        )

    def pass_y(c, n):
        copy((c, "y", n)).wait_recv()
        copy((c, "x", n)).start()
        copy((c, "a", n)).start()

    def pass_x(c, n):
        copy((c, "x", n)).wait_recv()
        copy((c, "b", n)).start()

    @pl.when(step == 0)
    def _():
        barrier = pltpu.get_barrier_semaphore()
        for peer in peers.values():
            pl.semaphore_signal(
                barrier, inc=1, device_id=peer, device_id_type=pl.DeviceIdType.MESH
            )
        pl.semaphore_wait(barrier, 3)
        own = pltpu.make_async_copy(shard_ref, land_ref.at[0], local_sem)
        own.start()
        for c in range(3):
            for n in range(3):
                copy((c, "y", n)).start()
            copy((c, "near")).start()
        mask_ref[...] = diagonal_mask(GROUP * HDIM)
        own.wait()
        pass_y(0, 0)
        pass_y(0, 1)
        pass_x(0, 0)
        pass_y(0, 2)
        pass_x(0, 1)
        pass_x(0, 2)
        copy((0, "near")).wait_recv()
        for n in range(3):
            copy((0, "a", n)).wait_recv()
            copy((0, "b", n)).wait_recv()
        for j in range(4):
            for kind in range(4):
                weights_ref[kind, j * part : (j + 1) * part, :] = land_ref[
                    j, kind * part : (kind + 1) * part, :
                ]
        rows = [widen(land_ref[j, 4 * part : 4 * part + 16, :]) for j in range(4)]
        vector_s[0:1, :] = jnp.concatenate([r[0:1, :part] for r in rows], 1)
        vector_s[1:2, :] = jnp.concatenate([r[2:3, :part] for r in rows], 1)
        for j in range(4):
            bias_ref[8 * j : 8 * j + 8, :] = jnp.broadcast_to(rows[j][1:2], (8, dim))
        pass_y(1, 0)
        pass_y(1, 1)

    @pl.when(step == 1)
    def _():
        pass_x(1, 0)
        pass_y(1, 2)
        pass_x(1, 1)
        pass_y(2, 0)

    @pl.when(step == 2)
    def _():
        pass_x(1, 2)
        pass_y(2, 1)
        pass_x(2, 0)

    @pl.when(step == 3)
    def _():
        pass_y(2, 2)
        pass_x(2, 1)

    tokens = widen(tokens_ref[...])
    vec = vec_ref[...]
    unit, _ = normalize(tokens)
    normed = (unit * vec[0:1] + vec[1:2]).astype(BF)
    normed_ref[...] = normed
    q_ref[...] = (dot_nt(normed, weights_ref[0]) + vector_s[0:1, :]).astype(BF)
    k_ref[...] = dot_nt(normed, weights_ref[1]).astype(BF)
    v_ref[...] = (dot_nt(normed, weights_ref[2]) + vector_s[1:2, :]).astype(BF)
    width = GROUP * HDIM
    factor = 1.0 / math.sqrt(HDIM)
    mask = mask_ref[...]
    for c in range(BLOCK // LMAX):
        rows = pl.ds(c * LMAX, LMAX)
        length = length_ref[
            (t * pl.num_programs(0) + step) * (BLOCK // LMAX) + c
        ]
        live = lax.broadcasted_iota(jnp.int32, (LMAX, width), 0) < length
        for g in range(dim // width):
            cols = pl.ds(g * width, width)
            wide = spread_heads(q_ref[rows, cols], mask)
            scores = dot_nt(k_ref[rows, cols], wide) * factor
            scores = jnp.where(live, scores, NEG)
            exponent = jnp.exp(scores - jnp.max(scores, 0, keepdims=True))
            probs = exponent * (1.0 / jnp.sum(exponent, 0, keepdims=True))
            probs_ref[rows, cols] = probs
            crossed = dot_tn(probs.astype(BF), v_ref[rows, cols])
            mixed_ref[rows, cols] = pick_heads(crossed).astype(BF)
    middle = tokens + dot_nn(mixed_ref[...], weights_ref[3]) + vec[2:3]
    middle_ref[...] = middle
    unit, _ = normalize(middle)
    second_ref[...] = (unit * vec[3:4] + vec[4:5]).astype(BF)

    @pl.when(step == pl.num_programs(0) - 1)
    def _():
        pass_x(2, 2)
        for c in (1, 2):
            copy((c, "near")).wait_recv()
            for n in range(3):
                copy((c, "a", n)).wait_recv()
                copy((c, "b", n)).wait_recv()
        for key in recipes:
            copy(key).wait_send()


def forward(lengths, tokens, shard, up, down, vec):
    rows, dim = tokens.shape
    steps = rows // BLOCK
    shapes = [
        (dim, BF),
        (dim, BF),
        (dim, BF),
        (dim, BF),
        (dim, F32),
        (dim, BF),
        (dim, F32),
        (dim, BF),
    ]
    anywhere = pl.BlockSpec(memory_space=pl.ANY)
    copies = 3 * 13
    return pl.pallas_call(
        forward_kernel,
        grid_spec=pltpu.PrefetchScalarGridSpec(
            num_scalar_prefetch=1,
            grid=(steps,),
            in_specs=[rowed(dim), anywhere, anywhere, anywhere, full(vec.shape)],
            out_specs=[rowed(width) for width, _ in shapes]
            + [full((4, dim, dim)), full((32, dim))]
            + [anywhere] * 6,
            scratch_shapes=[
                pltpu.VMEM((GROUP * HDIM, GROUP * HDIM), BF),
                pltpu.VMEM((4,) + shard.shape, BF),
                pltpu.VMEM((8, dim), F32),
                pltpu.SemaphoreType.DMA((copies,)),
                pltpu.SemaphoreType.DMA((copies,)),
                pltpu.SemaphoreType.DMA,
            ],
        ),
        out_shape=[jax.ShapeDtypeStruct((rows, width), kind) for width, kind in shapes]
        + [jax.ShapeDtypeStruct((4, dim, dim), BF), jax.ShapeDtypeStruct((32, dim), F32)]
        + [jax.ShapeDtypeStruct(up.shape, BF)] * 3
        + [jax.ShapeDtypeStruct(down.shape, BF)] * 3,
        compiler_params=pltpu.CompilerParams(
            dimension_semantics=("arbitrary",),
            vmem_limit_bytes=VMEM_LIMIT,
            collective_id=1,
            has_side_effects=True,
        ),
        name="attend",
    )(lengths, tokens, shard, up, down, vec)


def expert_kernel(
    first,
    final,
    second_ref,
    grad_ref,
    up_ref,
    down_ref,
    bias_ref,
    vec_ref,
    sum_ref,
    *refs,
):
    if not first:
        prior_ref, refs = refs[0], refs[1:]
    result_ref, total_ref, up_grad_ref, down_grad_ref, bias_grad_ref, active_s, hidden_s = refs
    step = pl.program_id(0)
    rows = pl.ds(pl.multiple_of(step * BLOCK, BLOCK), BLOCK)
    hidden = dot_nn(second_ref[rows, :], up_ref[...]) + bias_ref[0:1, :]
    lean = 0.5 + 0.5 * erf(hidden * (1.0 / math.sqrt(2.0)))
    slope = lean + hidden * (jnp.exp(-0.5 * hidden * hidden) * (1.0 / math.sqrt(2.0 * math.pi)))
    active = (hidden * lean).astype(BF)
    active_s[rows, :] = active
    result = sum_ref[...] + dot_nn(active, down_ref[...])
    if final:
        result = result + vec_ref[5:6, :]
    result_ref[...] = result.astype(result_ref.dtype)
    back = (dot_nt(grad_ref[rows, :], down_ref[...]) * slope).astype(BF)
    hidden_s[rows, :] = back
    total = dot_nt(back, up_ref[...])
    total_ref[...] = total if first else total + prior_ref[...]

    @pl.when(step == pl.num_programs(0) - 1)
    def _():
        down_grad_ref[...] = dot_tn(active_s[...], grad_ref[...]).astype(BF)
        up_grad_ref[...] = dot_tn(second_ref[...], hidden_s[...]).astype(BF)
        bias_grad_ref[...] = jnp.broadcast_to(
            jnp.sum(widen(hidden_s[...]), 0, keepdims=True), bias_grad_ref.shape
        )


def expert(j, final, second, grad, up, down, bias, vec, result, prior):
    rows, dim = second.shape
    units = up.shape[1]
    first = prior is None
    args = [second, grad, up, down, bias, vec, result] + ([] if first else [prior])
    return pl.pallas_call(
        functools.partial(expert_kernel, first, final),
        grid=(rows // BLOCK,),
        in_specs=[full(a.shape) for a in args[:4]]
        + [pl.BlockSpec((8, units), lambda i: (j, 0)), full(vec.shape), rowed(dim)]
        + ([] if first else [rowed(dim)]),
        out_specs=[
            rowed(dim),
            rowed(dim),
            full((dim, units)),
            full((units, dim)),
            full((8, units)),
        ],
        out_shape=[
            jax.ShapeDtypeStruct((rows, dim), BF if final else F32),
            jax.ShapeDtypeStruct((rows, dim), F32),
            jax.ShapeDtypeStruct((dim, units), BF),
            jax.ShapeDtypeStruct((units, dim), BF),
            jax.ShapeDtypeStruct((8, units), F32),
        ],
        scratch_shapes=[pltpu.VMEM((rows, units), BF), pltpu.VMEM((rows, units), BF)],
        compiler_params=params(),
        cost_estimate=pl.CostEstimate(
            flops=12 * rows * dim * units,
            bytes_accessed=20 * rows * dim,
            transcendentals=2 * rows * units,
        ),
        name="expert",
    )(*args)


def add_rows(into, base, other, other_base, rows, result=None):
    result = into if result is None else result
    size = min(rows, TILE)

    def body(i, carry):
        left = pl.ds(pl.multiple_of(base + i * size, 8), size)
        right = pl.ds(pl.multiple_of(other_base + i * size, 8), size)
        result[left, :] = (widen(into[left, :]) + widen(other[right, :])).astype(into.dtype)
        return carry

    lax.fori_loop(0, rows // size, body, 0)


def plan_levels(masks, rows):
    levels, place = [], 0
    for mask in masks:
        after = rows // 2 if (rows // 2) % 16 == 0 else rows
        levels.append((mask, rows, after, place))
        place += after
        rows = after
    return levels, place


def reduce_kernel(masks, chunk, *refs):
    (
        grad_ref,
        middle_ref,
        inner_ref,
        q_ref,
        k_ref,
        v_ref,
        probs_ref,
        mixed_ref,
        normed_ref,
        tokens_ref,
        weights_ref,
        vec_ref,
    ) = refs[:12]
    hidden_sums, refs = refs[12:16], refs[16:]
    sources, refs = (refs[:4], refs[4:8]), refs[8:]
    input_grad_ref, small_out, refs = refs[0], refs[1], refs[2:]
    out_refs, refs = refs[:3], refs[3:]
    mask_ref, low_s, mixed_grad_s, middle_grad_s, dq_ref, dk_ref, dv_ref = refs[:7]
    near_piece, last_piece, own, cross, near_own, near_cross, far, landing, gathered = refs[7:16]
    small_s, small_land, send_sem, recv_sem, local_sem, out_sem = refs[16:]

    step = pl.program_id(0)
    last = 3
    dim = grad_ref.shape[1]
    part = dim // 4
    levels, place = plan_levels(masks, chunk)
    halved = [k for k, level in enumerate(levels) if level[2] != level[1]]
    each = dim // chunk
    subs = 3 * each
    att = 2 * dim
    dp = lax.axis_index("dp")
    t = lax.axis_index("tensor")
    bits = {mask: (dp // mask) % 2 for mask in masks}
    peers = {mask: (dp + mask - 2 * mask * bits[mask], t) for mask in masks}
    peers["core"] = (dp, t + 1 - 2 * (t % 2))
    peers["far"] = (dp, t + 2 - 4 * ((t // 2) % 2))
    keeps, leaves, at = [], [], 0
    for mask, before, after, _ in levels:
        if after == before:
            keep = leave = at
        else:
            keep = at + bits[mask] * after
            leave = at + after - bits[mask] * after
        keeps.append(keep)
        leaves.append(leave)
        at = keep

    recipes = {}

    def recipe(key, source, target, peer):
        recipes[key] = (len(recipes), source, target, peer)

    def window(base, offset, size):
        return pl.ds(pl.multiple_of(base + offset, 16), size)

    for i in range(subs):
        base = i * chunk
        here = pl.ds(base, chunk)
        within = pl.ds((i % each) * chunk, chunk)
        if i < 2 * each:
            near, farthest = sources[i // each][1], sources[i // each][3]
        else:
            near, farthest = near_piece, last_piece
        recipe((i, "near_cross"), farthest.at[within, :], near_cross.at[here, :], "core")
        recipe((i, "near_own"), near.at[within, :], near_own.at[here, :], "core")
        recipe((i, "far"), cross.at[here, :], far.at[here, :], "far")
        for k, (mask, before, after, spot) in enumerate(levels):
            recipe(
                (i, "down", k),
                own.at[window(base, leaves[k], after), :],
                landing.at[pl.ds(i * place + spot, after), :],
                mask,
            )
        for k in halved:
            rows = window(base, keeps[k], levels[k][2])
            recipe((i, "up", k), gathered.at[rows, :], gathered.at[rows, :], levels[k][0])
    small_peers = ["core", "far"] + list(masks)
    spans = [(0, 24), (16, 16)] + [(16, 24)] * len(masks)
    for n, (first, count) in enumerate(spans):
        recipe(
            ("small", n),
            small_s.at[pl.ds(first, count), :],
            small_land.at[n, pl.ds(0, count), :],
            small_peers[n],
        )

    def copy(key):
        slot, source, target, peer = recipes[key]
        return pltpu.make_async_remote_copy(
            src_ref=source,
            dst_ref=target,
            send_sem=send_sem.at[slot],
            recv_sem=recv_sem.at[slot],
            device_id=peers[peer],
            device_id_type=pl.DeviceIdType.MESH,
        )

    def local_pair(i):
        within = pl.ds((i % each) * chunk, chunk)
        here = pl.ds(i * chunk, chunk)
        group = sources[i // each]
        return [
            pltpu.make_async_copy(group[2].at[within, :], cross.at[here, :], local_sem.at[2 * i]),
            pltpu.make_async_copy(group[0].at[within, :], own.at[here, :], local_sem.at[2 * i + 1]),
        ]

    def core_send(i):
        copy((i, "near_cross")).start()
        copy((i, "near_own")).start()
        if i < 2 * each:
            for piece in local_pair(i):
                piece.start()

    def start_cross(i):
        if i < 2 * each:
            for piece in local_pair(i):
                piece.wait()
        copy((i, "near_cross")).wait_recv()
        add_rows(cross, i * chunk, near_cross, i * chunk, chunk)
        copy((i, "far")).start()
        copy((i, "near_own")).wait_recv()
        add_rows(own, i * chunk, near_own, i * chunk, chunk)

    def take_far(i):
        copy((i, "far")).wait_recv()
        add_rows(own, i * chunk, far, i * chunk, chunk)
        copy((i, "down", 0)).start()

    def take_level(i, k):
        _, before, after, spot = levels[k]
        copy((i, "down", k)).wait_recv()
        if after == before:
            copy((i, "down", k)).wait_send()
        final = k + 1 == len(levels)
        add_rows(
            own,
            i * chunk + keeps[k],
            landing,
            i * place + spot,
            after,
            gathered if final else None,
        )
        if not final:
            copy((i, "down", k + 1)).start()
        elif halved:
            copy((i, "up", halved[-1])).start()

    def take_up(i, n):
        copy((i, "up", halved[-1 - n])).wait_recv()
        if n + 1 < len(halved):
            copy((i, "up", halved[-2 - n])).start()

    def small_step(n):
        first = spans[n][0]
        copy(("small", n)).wait()
        land = small_land.at[n]
        small_s[16:24, :] += land[16 - first : 24 - first, :]
        if n == 0:
            small_s[32:40, :] += land[0:8, :]
            small_s[24:32, :] += land[8:16, :]
        elif n == 1:
            small_s[32:40, :] += land[8:16, :]
        else:
            small_s[32:40, :] += land[16:24, :]
        if n + 1 < len(spans):
            copy(("small", n + 1)).start()

    def weight_grads():
        query_sum = jnp.sum(widen(dq_ref[...]), 0, keepdims=True)
        value_sum = jnp.sum(widen(dv_ref[...]), 0, keepdims=True)
        blank = jnp.zeros((1, dim - 2 * part), F32)
        for j, row in enumerate((32, 0, 24, 8)):
            cols = slice(j * part, (j + 1) * part)
            small_s[row : row + 1, :] = jnp.concatenate(
                [query_sum[:, cols], value_sum[:, cols], blank], 1
            )
            small_s[row + 1 : row + 2, :] = hidden_sums[j][0:1, :]
        for kind, (left, right) in enumerate(
            ((dq_ref, normed_ref), (dk_ref, normed_ref), (dv_ref, normed_ref), (mixed_ref, low_s))
        ):
            result = dot_tn(left[...], right[...]).astype(BF)
            low, high = kind * part, (kind + 1) * part
            own[att + low : att + high, :] = result[:part]
            near_piece[low:high, :] = result[part : 2 * part]
            cross[att + low : att + high, :] = result[2 * part : 3 * part]
            last_piece[low:high, :] = result[3 * part :]

    def input_block(block):
        rows = pl.ds(block * BLOCK, BLOCK)
        unit, scale = normalize(widen(tokens_ref[rows, :]))
        grad = (
            dot_nn(dq_ref[rows, :], weights_ref[0])
            + dot_nn(dk_ref[rows, :], weights_ref[1])
            + dot_nn(dv_ref[rows, :], weights_ref[2])
        )
        small_s[16:17, :] += jnp.sum(grad * unit, 0, keepdims=True)
        small_s[17:18, :] += jnp.sum(grad, 0, keepdims=True)
        back = normalize_back(grad * vec_ref[0:1, :], unit, scale)
        input_grad_ref[rows, :] = (middle_grad_s[rows, :] + back).astype(BF)

    span = 4.5 * chunk / 128
    tasks = []

    def add(when, task, *args):
        tasks.append((when, len(tasks), functools.partial(task, *args)))

    for i in range(subs):
        if i < 2 * each:
            add(8.0 if i < each else 16.0, start_cross, i)
            arrive = 9.0 + span * (i + 1)
        else:
            add(40.0, core_send, i)
            add(43.0 + 0.2 * span * (i - 2 * each), start_cross, i)
            arrive = 9.0 + span * (i + 1)
        add(arrive, take_far, i)
        for k in range(len(levels)):
            add(arrive + span * (1 + k), take_level, i, k)
        for n in range(len(halved)):
            add(arrive + span * (1 + len(levels) + n), take_up, i, n)
    add(32.0, weight_grads)
    blocks = tokens_ref.shape[0] // BLOCK
    for block in range(blocks):
        add(39.0 + 3.0 * block, input_block, block)
    end = 41.0 + 3.0 * blocks
    add(end, lambda: copy(("small", 0)).start())
    for n in range(len(spans)):
        add(end + 4.0 + 4.0 * n, small_step, n)
    tasks.sort(key=lambda entry: entry[:2])

    def run(low, high):
        for when, _, task in tasks:
            if low <= when < high:
                task()

    @pl.when(step == 0)
    def _():
        barrier = pltpu.get_barrier_semaphore()
        for peer in peers.values():
            pl.semaphore_signal(
                barrier, inc=1, device_id=peer, device_id_type=pl.DeviceIdType.MESH
            )
        pl.semaphore_wait(barrier, len(peers))
        for i in range(2 * each):
            core_send(i)
        mask_ref[...] = diagonal_mask(GROUP * HDIM)
        small_s[...] = jnp.zeros_like(small_s)

    for boundary in (1, 2, 3):

        @pl.when(step == boundary)
        def _():
            run(8.0 * (boundary - 1) + 0.5, 8.0 * boundary + 0.5)

    all_rows = pl.ds(pl.multiple_of(step * BLOCK, BLOCK), BLOCK)
    vec = vec_ref[...]
    upstream = widen(grad_ref[...])
    unit, scale = normalize(middle_ref[...])
    inner = inner_ref[...]
    middle_grad = upstream + normalize_back(inner * vec[3:4], unit, scale)
    middle_grad_s[all_rows, :] = middle_grad
    middle_low = middle_grad.astype(BF)
    low_s[all_rows, :] = middle_low
    small_s[18:19, :] += jnp.sum(middle_grad, 0, keepdims=True)
    small_s[19:20, :] += jnp.sum(inner * unit, 0, keepdims=True)
    small_s[20:21, :] += jnp.sum(inner, 0, keepdims=True)
    small_s[21:22, :] += jnp.sum(upstream, 0, keepdims=True)
    mixed_grad_s[...] = dot_nt(middle_low, weights_ref[3]).astype(BF)
    width = GROUP * HDIM
    factor = 1.0 / math.sqrt(HDIM)
    mask = mask_ref[...]
    for c in range(BLOCK // LMAX):
        rows = pl.ds(c * LMAX, LMAX)
        into = pl.ds(pl.multiple_of(step * BLOCK + c * LMAX, LMAX), LMAX)
        for g in range(dim // width):
            cols = pl.ds(g * width, width)
            wide = spread_heads(mixed_grad_s[rows, cols], mask)
            probs = probs_ref[rows, cols]
            prob_grad = dot_nt(v_ref[rows, cols], wide)
            dv_ref[into, cols] = dot_nn(probs.astype(BF), wide).astype(BF)
            weighted = jnp.sum(probs * prob_grad, 0, keepdims=True)
            score_grad = (probs * (prob_grad - weighted)).astype(BF)
            queries = spread_heads(q_ref[rows, cols], mask)
            dk_ref[into, cols] = (dot_nn(score_grad, queries) * factor).astype(BF)
            crossed = dot_tn(score_grad, k_ref[rows, cols])
            dq_ref[into, cols] = (pick_heads(crossed) * factor).astype(BF)

    @pl.when(step == last)
    def _():
        run(24.5, 1e9)
        outs = [
            pltpu.make_async_copy(
                gathered.at[pl.ds(n * dim, dim), :], out_refs[n], out_sem.at[n]
            )
            for n in range(3)
        ]
        for out in outs:
            out.start()
        small_out[...] = small_s[...]
        for key in recipes:
            repeated = key[0] == "small" or (
                key[1] == "down" and levels[key[2]][1] == levels[key[2]][2]
            )
            if not repeated:
                copy(key).wait_send()
        for out in outs:
            out.wait()


def backward(masks, blocked, whole, weights, vec, hidden_sums, groups):
    rows, dim = blocked[0].shape
    levels, place = plan_levels(masks, CHUNK)
    total = 3 * dim
    subs = total // CHUNK
    halved = sum(level[1] != level[2] for level in levels)
    copies = subs * (3 + len(levels) + halved) + 2 + len(masks)
    anywhere = pl.BlockSpec(memory_space=pl.ANY)
    buffer = pltpu.VMEM((total, dim), BF)
    flat = [piece for group in groups for piece in group]

    def once(shape):
        return pl.BlockSpec(
            shape, lambda i: (0,) * len(shape), pipeline_mode=pl.Buffered(1)
        )

    all_rows = pltpu.VMEM((rows, dim), BF)
    return pl.pallas_call(
        functools.partial(reduce_kernel, masks, CHUNK),
        grid=(rows // BLOCK,),
        in_specs=[rowed(dim)] * len(blocked)
        + [once((rows, dim))] * len(whole)
        + [once(weights.shape), full(vec.shape)]
        + [full(sums.shape) for sums in hidden_sums]
        + [anywhere] * len(flat),
        out_specs=[once((rows, dim)), full((40, dim))] + [anywhere] * 3,
        out_shape=[
            jax.ShapeDtypeStruct((rows, dim), BF),
            jax.ShapeDtypeStruct((40, dim), F32),
        ]
        + [jax.ShapeDtypeStruct((dim, dim), BF)] * 3,
        scratch_shapes=[
            pltpu.VMEM((GROUP * HDIM, GROUP * HDIM), BF),
            all_rows,
            pltpu.VMEM((BLOCK, dim), BF),
            pltpu.VMEM((rows, dim), F32),
            all_rows,
            all_rows,
            all_rows,
            pltpu.VMEM((dim, dim), BF),
            pltpu.VMEM((dim, dim), BF),
            buffer,
            buffer,
            buffer,
            buffer,
            buffer,
            pltpu.VMEM((subs * place, dim), BF),
            buffer,
            pltpu.VMEM((40, dim), F32),
            pltpu.VMEM((2 + len(masks), 24, dim), F32),
            pltpu.SemaphoreType.DMA((copies,)),
            pltpu.SemaphoreType.DMA((copies,)),
            pltpu.SemaphoreType.DMA((2 * subs,)),
            pltpu.SemaphoreType.DMA((3,)),
        ],
        compiler_params=pltpu.CompilerParams(
            dimension_semantics=("arbitrary",),
            collective_id=0,
            has_side_effects=True,
            vmem_limit_bytes=66 * 1024 * 1000,
        ),
        name="attend_back",
    )(*blocked, *whole, weights, vec, *hidden_sums, *flat)


def place_rows(count, rows, kind):
    row = lax.broadcasted_iota(jnp.int32, (count, rows[0].shape[0]), 0)
    out = jnp.zeros(row.shape, kind)
    for i, values in enumerate(rows):
        out = jnp.where(row == i, values.astype(kind)[None, :], out)
    return out


def per_device(
    ndp,
    nt,
    caption_tokens,
    caption_lengths,
    output_grad,
    norm_gain,
    norm_bias,
    query_weight,
    query_bias,
    key_weight,
    value_weight,
    value_bias,
    output_weight,
    output_bias,
    second_gain,
    second_bias,
    hidden_weight,
    hidden_bias,
    down_weight,
    down_bias,
):
    masks, mask = [], 1
    while mask < ndp:
        masks.append(mask)
        mask *= 2
    rows, dim = caption_tokens.shape
    part = query_weight.shape[1]
    fill = (0, dim - part)
    biases = place_rows(PAD, (jnp.pad(query_bias, fill), hidden_bias, jnp.pad(value_bias, fill)), BF)
    shard = jnp.concatenate([query_weight.T, key_weight.T, value_weight.T, output_weight, biases], 0)
    vec = place_rows(
        8, (norm_gain, norm_bias, output_bias, second_gain, second_bias, down_bias), F32
    )
    normed, q, k, v, probs, mixed, middle, second, weights, bias, *rest = forward(
        caption_lengths, caption_tokens, shard, hidden_weight, down_weight, vec
    )
    ups = [hidden_weight] + rest[:3]
    downs = [down_weight] + rest[3:]
    up_grads, down_grads, hidden_sums = [None] * 4, [None] * 4, [None] * 4
    result, inner = middle, None
    for j in (3, 2, 1, 0):
        result, inner, up_grads[j], down_grads[j], hidden_sums[j] = expert(
            j, j == 0, second, output_grad, ups[j], downs[j], bias, vec, result, inner
        )
    token_grad, packed, grad_up, grad_down, grad_att = backward(
        tuple(masks),
        [output_grad, middle, inner, q, k, v, probs],
        [mixed, normed, caption_tokens],
        weights,
        vec,
        hidden_sums,
        [up_grads, down_grads],
    )
    grad_up, grad_down, grad_att = widen(grad_up), widen(grad_down), widen(grad_att)
    sums, mine = packed[16:24], packed[32:34]
    return (
        result,
        token_grad,
        sums[0],
        sums[1],
        grad_att[:part].T,
        mine[0, :part],
        grad_att[part : 2 * part].T,
        grad_att[2 * part : 3 * part].T,
        mine[0, part : 2 * part],
        grad_att[3 * part :],
        sums[2],
        sums[3],
        sums[4],
        grad_up,
        mine[1],
        grad_down,
        sums[5],
    )


def solution(mesh):
    ndp, nt = mesh.shape["dp"], mesh.shape["tensor"]
    both = P(("dp", "tensor"), None)
    col, row, vec = P(None, "tensor"), P("tensor", None), P("tensor")

    def body(*args):
        return per_device(ndp, nt, *args)

    return jax.shard_map(
        body,
        mesh=mesh,
        in_specs=(both, P("dp"), both, P(), P(), col, vec, col, col, vec, row, P(), P(), P(), col, vec, row, P()),
        out_specs=(both, both, P(), P(), col, vec, col, col, vec, row, P(), P(), P(), col, vec, row, P()),
        check_vma=False,
    )
```

```python
import functools
import math

import jax
import jax.numpy as jnp
from jax import lax
from jax.experimental import pallas as pl
from jax.experimental.pallas import tpu as pltpu
from jax.sharding import PartitionSpec as P


HDIM = 64
LMAX = 64
EPS = 1e-05
NEG = -1e30
GROUP = 4
BLOCK = 256
PAD = 32
CHUNK = 128
TILE = 32
AXES = ("dp", "tensor")
BF = jnp.bfloat16
F32 = jnp.float32
VMEM_LIMIT = 60 * 1024 * 1024


def widen(values):
    return values.astype(F32)


def dot_nn(left, right):
    return jnp.dot(left, right, preferred_element_type=F32)


def dot_nt(left, right):
    return lax.dot_general(left, right, (((1,), (1,)), ((), ())), preferred_element_type=F32)


def dot_tn(left, right):
    return lax.dot_general(left, right, (((0,), (0,)), ((), ())), preferred_element_type=F32)


def normalize(values):
    center = jnp.mean(values, -1, keepdims=True)
    spread = values - center
    scale = lax.rsqrt(jnp.mean(spread * spread, -1, keepdims=True) + EPS)
    return spread * scale, scale


def normalize_back(grad, unit, scale):
    return scale * (
        grad - jnp.mean(grad, -1, keepdims=True) - unit * jnp.mean(grad * unit, -1, keepdims=True)
    )


def erf(values):
    values = jnp.clip(values, -4.0, 4.0)
    square = values * values
    top = -2.72614225801306e-10
    for coef in (
        2.77068142495902e-08,
        -2.10102402082508e-06,
        -5.69250639462346e-05,
        -7.34990630326855e-04,
        -2.95459980854025e-03,
        -1.60960333262415e-02,
    ):
        top = top * square + coef
    low = -1.45660718464996e-05
    for coef in (
        -2.13374055278905e-04,
        -1.68282697438203e-03,
        -7.37332916720468e-03,
        -1.42647390514189e-02,
    ):
        low = low * square + coef
    return values * top / low


def diagonal_mask(size):
    rows = lax.shift_right_logical(lax.broadcasted_iota(jnp.int32, (size, size), 0), 6)
    cols = lax.shift_right_logical(lax.broadcasted_iota(jnp.int32, (size, size), 1), 6)
    return jnp.where(rows == cols, 1.0, 0.0).astype(BF)


def spread_heads(values, mask):
    return jnp.concatenate([values] * GROUP, 0) * mask


def pick_heads(values):
    lane = lax.shift_right_logical(
        lax.broadcasted_iota(jnp.int32, (LMAX, values.shape[1]), 1), 6
    )
    out = values[:LMAX]
    for head in range(1, GROUP):
        out = jnp.where(lane == head, values[head * LMAX : (head + 1) * LMAX], out)
    return out


def full(shape):
    return pl.BlockSpec(shape, lambda i, *_: (0,) * len(shape))


def rowed(width):
    return pl.BlockSpec((BLOCK, width), lambda i, *_: (i, 0))


def params():
    return pltpu.CompilerParams(
        dimension_semantics=("arbitrary",), vmem_limit_bytes=VMEM_LIMIT
    )


def split_rows(rows):
    count = rows // 16
    spans, start = [], 0
    for k in range(3):
        size = (count * (k + 1) // 3 - count * k // 3) * 16
        spans.append((start, size))
        start += size
    return spans


def forward_kernel(
    length_ref,
    tokens_ref,
    shard_ref,
    up_ref,
    down_ref,
    vec_ref,
    normed_ref,
    q_ref,
    k_ref,
    v_ref,
    probs_ref,
    mixed_ref,
    middle_ref,
    second_ref,
    weights_ref,
    bias_ref,
    up_all,
    down_all,
    mask_ref,
    land_ref,
    stage_ref,
    vector_s,
    send_sem,
    recv_sem,
    local_sem,
):
    step = pl.program_id(0)
    dim = tokens_ref.shape[1]
    part = dim // 4
    dp = lax.axis_index("dp")
    t = lax.axis_index("tensor")
    bit = dp % 2
    peers = {
        "core": (dp, t + 1 - 2 * (t % 2)),
        "far": (dp, t + 2 - 4 * ((t // 2) % 2)),
        "side": (dp + 1 - 2 * bit, t),
    }
    chunks = [
        (shard_ref, land_ref.at[1], land_ref.at[2], land_ref.at[3]),
        (up_ref, up_all.at[1], up_all.at[2], up_all.at[3]),
        (down_ref, down_all.at[1], down_all.at[2], down_all.at[3]),
    ]
    recipes = {}

    def recipe(key, source, target, peer):
        recipes[key] = (len(recipes), source, target, peer)

    for c, (shard, near, cross, last) in enumerate(chunks):
        half = shard.shape[0] // 2
        recipe((c, "near"), shard, near, "core")
        for n, (start, size) in enumerate(split_rows(half)):
            mine = pl.ds(pl.multiple_of(bit * half + start, 16), size)
            other = pl.ds(pl.multiple_of((1 - bit) * half + start, 16), size)
            recipe((c, "y", n), shard.at[mine, :], cross.at[mine, :], "far")
            recipe((c, "x", n), cross.at[mine, :], cross.at[mine, :], "side")
            recipe((c, "a", n), cross.at[mine, :], last.at[mine, :], "core")
            recipe((c, "b", n), cross.at[other, :], last.at[other, :], "core")

    def copy(key):
        slot, source, target, peer = recipes[key]
        return pltpu.make_async_remote_copy(
            src_ref=source,
            dst_ref=target,
            send_sem=send_sem.at[slot],
            recv_sem=recv_sem.at[slot],
            device_id=peers[peer],
            device_id_type=pl.DeviceIdType.MESH,
        )

    def own_copy(n, out):
        source, target = ((up_ref, up_all), (down_ref, down_all))[n]
        if out:
            return pltpu.make_async_copy(stage_ref.at[n], target.at[0], local_sem.at[3 + n])
        return pltpu.make_async_copy(source, stage_ref.at[n], local_sem.at[1 + n])

    def pass_y(c, n):
        copy((c, "y", n)).wait_recv()
        copy((c, "x", n)).start()
        copy((c, "a", n)).start()

    def pass_x(c, n):
        copy((c, "x", n)).wait_recv()
        copy((c, "b", n)).start()

    @pl.when(step == 0)
    def _():
        barrier = pltpu.get_barrier_semaphore()
        for peer in peers.values():
            pl.semaphore_signal(
                barrier, inc=1, device_id=peer, device_id_type=pl.DeviceIdType.MESH
            )
        pl.semaphore_wait(barrier, 3)
        own = pltpu.make_async_copy(shard_ref, land_ref.at[0], local_sem.at[0])
        own.start()
        for c in range(3):
            for n in range(3):
                copy((c, "y", n)).start()
            copy((c, "near")).start()
        for n in range(2):
            own_copy(n, False).start()
        mask_ref[...] = diagonal_mask(GROUP * HDIM)
        own.wait()
        pass_y(0, 0)
        pass_y(0, 1)
        pass_x(0, 0)
        pass_y(0, 2)
        pass_x(0, 1)
        pass_x(0, 2)
        copy((0, "near")).wait_recv()
        for n in range(3):
            copy((0, "a", n)).wait_recv()
            copy((0, "b", n)).wait_recv()
        for j in range(4):
            for kind in range(4):
                weights_ref[kind, j * part : (j + 1) * part, :] = land_ref[
                    j, kind * part : (kind + 1) * part, :
                ]
        rows = [widen(land_ref[j, 4 * part : 4 * part + 16, :]) for j in range(4)]
        vector_s[0:1, :] = jnp.concatenate([r[0:1, :part] for r in rows], 1)
        vector_s[1:2, :] = jnp.concatenate([r[2:3, :part] for r in rows], 1)
        for j in range(4):
            bias_ref[8 * j : 8 * j + 8, :] = jnp.broadcast_to(rows[j][1:2], (8, dim))
        pass_y(1, 0)
        pass_y(1, 1)

    @pl.when(step == 1)
    def _():
        for n in range(2):
            own_copy(n, False).wait()
            own_copy(n, True).start()
        pass_x(1, 0)
        pass_y(1, 2)
        pass_x(1, 1)
        pass_y(2, 0)

    @pl.when(step == 2)
    def _():
        pass_x(1, 2)
        pass_y(2, 1)
        pass_x(2, 0)

    @pl.when(step == 3)
    def _():
        pass_y(2, 2)
        pass_x(2, 1)

    tokens = widen(tokens_ref[...])
    vec = vec_ref[...]
    unit, _ = normalize(tokens)
    normed = (unit * vec[0:1] + vec[1:2]).astype(BF)
    normed_ref[...] = normed
    q_ref[...] = (dot_nt(normed, weights_ref[0]) + vector_s[0:1, :]).astype(BF)
    k_ref[...] = dot_nt(normed, weights_ref[1]).astype(BF)
    v_ref[...] = (dot_nt(normed, weights_ref[2]) + vector_s[1:2, :]).astype(BF)
    width = GROUP * HDIM
    factor = 1.0 / math.sqrt(HDIM)
    mask = mask_ref[...]
    for c in range(BLOCK // LMAX):
        rows = pl.ds(c * LMAX, LMAX)
        length = length_ref[
            (t * pl.num_programs(0) + step) * (BLOCK // LMAX) + c
        ]
        live = lax.broadcasted_iota(jnp.int32, (LMAX, width), 0) < length
        for g in range(dim // width):
            cols = pl.ds(g * width, width)
            wide = spread_heads(q_ref[rows, cols], mask)
            scores = dot_nt(k_ref[rows, cols], wide) * factor
            scores = jnp.where(live, scores, NEG)
            exponent = jnp.exp(scores - jnp.max(scores, 0, keepdims=True))
            probs = exponent * (1.0 / jnp.sum(exponent, 0, keepdims=True))
            probs_ref[rows, cols] = probs
            crossed = dot_tn(probs.astype(BF), v_ref[rows, cols])
            mixed_ref[rows, cols] = pick_heads(crossed).astype(BF)
    middle = tokens + dot_nn(mixed_ref[...], weights_ref[3]) + vec[2:3]
    middle_ref[...] = middle
    unit, _ = normalize(middle)
    second_ref[...] = (unit * vec[3:4] + vec[4:5]).astype(BF)

    @pl.when(step == pl.num_programs(0) - 1)
    def _():
        pass_x(2, 2)
        for c in (1, 2):
            copy((c, "near")).wait_recv()
            for n in range(3):
                copy((c, "a", n)).wait_recv()
                copy((c, "b", n)).wait_recv()
        for key in recipes:
            copy(key).wait_send()
        for n in range(2):
            own_copy(n, True).wait()


def forward(lengths, tokens, shard, up, down, vec):
    rows, dim = tokens.shape
    steps = rows // BLOCK
    shapes = [
        (dim, BF),
        (dim, BF),
        (dim, BF),
        (dim, BF),
        (dim, F32),
        (dim, BF),
        (dim, F32),
        (dim, BF),
    ]
    anywhere = pl.BlockSpec(memory_space=pl.ANY)
    copies = 3 * 13
    return pl.pallas_call(
        forward_kernel,
        grid_spec=pltpu.PrefetchScalarGridSpec(
            num_scalar_prefetch=1,
            grid=(steps,),
            in_specs=[rowed(dim), anywhere, anywhere, anywhere, full(vec.shape)],
            out_specs=[rowed(width) for width, _ in shapes]
            + [full((4, dim, dim)), full((32, dim))]
            + [anywhere] * 2,
            scratch_shapes=[
                pltpu.VMEM((GROUP * HDIM, GROUP * HDIM), BF),
                pltpu.VMEM((4,) + shard.shape, BF),
                pltpu.VMEM((2,) + up.shape, BF),
                pltpu.VMEM((8, dim), F32),
                pltpu.SemaphoreType.DMA((copies,)),
                pltpu.SemaphoreType.DMA((copies,)),
                pltpu.SemaphoreType.DMA((5,)),
            ],
        ),
        out_shape=[jax.ShapeDtypeStruct((rows, width), kind) for width, kind in shapes]
        + [jax.ShapeDtypeStruct((4, dim, dim), BF), jax.ShapeDtypeStruct((32, dim), F32)]
        + [
            jax.ShapeDtypeStruct((4,) + up.shape, BF),
            jax.ShapeDtypeStruct((4,) + down.shape, BF),
        ],
        compiler_params=pltpu.CompilerParams(
            dimension_semantics=("arbitrary",),
            vmem_limit_bytes=VMEM_LIMIT,
            collective_id=1,
            has_side_effects=True,
        ),
        name="attend",
    )(lengths, tokens, shard, up, down, vec)


def expert_kernel(
    second_ref,
    grad_ref,
    middle_ref,
    up_ref,
    down_ref,
    bias_ref,
    vec_ref,
    result_ref,
    total_ref,
    up_grad_ref,
    down_grad_ref,
    bias_grad_ref,
    sum_s,
    active_s,
    hidden_s,
):
    piece = pl.program_id(0)
    step = pl.program_id(1)
    rows = pl.ds(pl.multiple_of(step * BLOCK, BLOCK), BLOCK)
    hidden = dot_nn(second_ref[rows, :], up_ref[...]) + bias_ref[0:1, :]
    lean = 0.5 + 0.5 * erf(hidden * (1.0 / math.sqrt(2.0)))
    slope = lean + hidden * (jnp.exp(-0.5 * hidden * hidden) * (1.0 / math.sqrt(2.0 * math.pi)))
    active = (hidden * lean).astype(BF)
    active_s[rows, :] = active
    back = (dot_nt(grad_ref[rows, :], down_ref[...]) * slope).astype(BF)
    hidden_s[rows, :] = back
    result = dot_nn(active, down_ref[...])
    total = dot_nt(back, up_ref[...])

    @pl.when(piece == 0)
    def _():
        sum_s[rows, :] = result + middle_ref[rows, :]
        total_ref[rows, :] = total

    @pl.when(piece > 0)
    def _():
        sum_s[rows, :] += result
        total_ref[rows, :] += total

    @pl.when(piece == pl.num_programs(0) - 1)
    def _():
        result_ref[rows, :] = (sum_s[rows, :] + vec_ref[5:6, :]).astype(BF)

    @pl.when(step == pl.num_programs(1) - 1)
    def _():
        down_grad_ref[...] = dot_tn(active_s[...], grad_ref[...]).astype(BF)
        up_grad_ref[...] = dot_tn(second_ref[...], hidden_s[...]).astype(BF)
        bias_grad_ref[...] = jnp.broadcast_to(
            jnp.sum(widen(hidden_s[...]), 0, keepdims=True), bias_grad_ref.shape
        )


def once(shape):
    return pl.BlockSpec(shape, lambda i, *_: (0,) * len(shape), pipeline_mode=pl.Buffered(1))


def expert(second, grad, middle, ups, downs, bias, vec):
    rows, dim = second.shape
    pieces, _, units = ups.shape

    def quarter(*shape):
        return pl.BlockSpec((None,) + shape, lambda p, i: (pieces - 1 - p, 0, 0))

    row = pl.BlockSpec((8, units), lambda p, i: (pieces - 1 - p, 0))
    return pl.pallas_call(
        expert_kernel,
        grid=(pieces, rows // BLOCK),
        in_specs=[once((rows, dim))] * 3
        + [quarter(dim, units), quarter(units, dim), row, once(vec.shape)],
        out_specs=[
            once((rows, dim)),
            once((rows, dim)),
            quarter(dim, units),
            quarter(units, dim),
            row,
        ],
        out_shape=[
            jax.ShapeDtypeStruct((rows, dim), BF),
            jax.ShapeDtypeStruct((rows, dim), F32),
            jax.ShapeDtypeStruct(ups.shape, BF),
            jax.ShapeDtypeStruct(downs.shape, BF),
            jax.ShapeDtypeStruct((8 * pieces, units), F32),
        ],
        scratch_shapes=[
            pltpu.VMEM((rows, dim), F32),
            pltpu.VMEM((rows, units), BF),
            pltpu.VMEM((rows, units), BF),
        ],
        compiler_params=pltpu.CompilerParams(
            dimension_semantics=("arbitrary", "arbitrary"), vmem_limit_bytes=VMEM_LIMIT
        ),
        cost_estimate=pl.CostEstimate(
            flops=12 * pieces * rows * dim * units,
            bytes_accessed=40 * rows * dim,
            transcendentals=2 * pieces * rows * units,
        ),
        name="expert",
    )(second, grad, middle, ups, downs, bias, vec)


def add_rows(into, base, other, other_base, rows, result=None):
    result = into if result is None else result
    size = min(rows, TILE)

    def body(i, carry):
        left = pl.ds(pl.multiple_of(base + i * size, 8), size)
        right = pl.ds(pl.multiple_of(other_base + i * size, 8), size)
        result[left, :] = (widen(into[left, :]) + widen(other[right, :])).astype(into.dtype)
        return carry

    lax.fori_loop(0, rows // size, body, 0)


def plan_levels(masks, rows):
    levels, place = [], 0
    for mask in masks:
        after = rows // 2 if (rows // 2) % 16 == 0 else rows
        levels.append((mask, rows, after, place))
        place += after
        rows = after
    return levels, place


def reduce_kernel(masks, chunk, *refs):
    (
        grad_ref,
        middle_ref,
        inner_ref,
        q_ref,
        k_ref,
        v_ref,
        probs_ref,
        mixed_ref,
        normed_ref,
        tokens_ref,
        weights_ref,
        vec_ref,
    ) = refs[:12]
    hidden_sums, sources, refs = refs[12], refs[13:15], refs[15:]
    input_grad_ref, small_out, refs = refs[0], refs[1], refs[2:]
    out_refs, refs = refs[:3], refs[3:]
    mask_ref, low_s, mixed_grad_s, middle_grad_s, dq_ref, dk_ref, dv_ref = refs[:7]
    near_piece, last_piece, own, cross, near_own, near_cross, far, landing, gathered = refs[7:16]
    small_s, small_land, send_sem, recv_sem, local_sem, out_sem = refs[16:]

    step = pl.program_id(0)
    last = 3
    dim = grad_ref.shape[1]
    part = dim // 4
    levels, place = plan_levels(masks, chunk)
    halved = [k for k, level in enumerate(levels) if level[2] != level[1]]
    each = dim // chunk
    subs = 3 * each
    att = 2 * dim
    dp = lax.axis_index("dp")
    t = lax.axis_index("tensor")
    bits = {mask: (dp // mask) % 2 for mask in masks}
    peers = {mask: (dp + mask - 2 * mask * bits[mask], t) for mask in masks}
    peers["core"] = (dp, t + 1 - 2 * (t % 2))
    peers["far"] = (dp, t + 2 - 4 * ((t // 2) % 2))
    orders = (masks, masks[1:] + masks[:1])
    geometry = []
    for order in orders:
        keeps, leaves, at = [], [], 0
        for mask, (_, before, after, _) in zip(order, levels):
            if after == before:
                keep = leave = at
            else:
                keep = at + bits[mask] * after
                leave = at + after - bits[mask] * after
            keeps.append(keep)
            leaves.append(leave)
            at = keep
        geometry.append((order, keeps, leaves))

    def shape_of(i):
        return geometry[1 if i % 4 == 2 else 0]

    recipes = {}

    def recipe(key, source, target, peer):
        recipes[key] = (len(recipes), source, target, peer)

    def window(base, offset, size):
        return pl.ds(pl.multiple_of(base + offset, 16), size)

    for i in range(subs):
        base = i * chunk
        here = pl.ds(base, chunk)
        within = pl.ds((i % each) * chunk, chunk)
        if i < 2 * each:
            near, farthest = sources[i // each].at[1], sources[i // each].at[3]
        else:
            near, farthest = near_piece, last_piece
        recipe((i, "near_cross"), farthest.at[within, :], near_cross.at[here, :], "core")
        recipe((i, "near_own"), near.at[within, :], near_own.at[here, :], "core")
        recipe((i, "far"), cross.at[here, :], far.at[here, :], "far")
        order, keeps, leaves = shape_of(i)
        for k, (_, before, after, spot) in enumerate(levels):
            recipe(
                (i, "down", k),
                own.at[window(base, leaves[k], after), :],
                landing.at[pl.ds(i * place + spot, after), :],
                order[k],
            )
        for k in halved:
            rows = window(base, keeps[k], levels[k][2])
            recipe((i, "up", k), gathered.at[rows, :], gathered.at[rows, :], order[k])
    small_peers = ["core", "far"] + list(masks)
    spans = [(0, 24), (16, 16)] + [(16, 24)] * len(masks)
    for n, (first, count) in enumerate(spans):
        recipe(
            ("small", n),
            small_s.at[pl.ds(first, count), :],
            small_land.at[n, pl.ds(0, count), :],
            small_peers[n],
        )

    def copy(key):
        slot, source, target, peer = recipes[key]
        return pltpu.make_async_remote_copy(
            src_ref=source,
            dst_ref=target,
            send_sem=send_sem.at[slot],
            recv_sem=recv_sem.at[slot],
            device_id=peers[peer],
            device_id_type=pl.DeviceIdType.MESH,
        )

    def local_pair(i):
        within = pl.ds((i % each) * chunk, chunk)
        here = pl.ds(i * chunk, chunk)
        group = sources[i // each]
        return [
            pltpu.make_async_copy(group.at[2, within, :], cross.at[here, :], local_sem.at[2 * i]),
            pltpu.make_async_copy(group.at[0, within, :], own.at[here, :], local_sem.at[2 * i + 1]),
        ]

    def core_send(i):
        copy((i, "near_cross")).start()
        copy((i, "near_own")).start()
        if i < 2 * each:
            for piece in local_pair(i):
                piece.start()

    def start_cross(i):
        if i < 2 * each:
            for piece in local_pair(i):
                piece.wait()
        copy((i, "near_cross")).wait_recv()
        add_rows(cross, i * chunk, near_cross, i * chunk, chunk)
        copy((i, "far")).start()
        copy((i, "near_own")).wait_recv()
        add_rows(own, i * chunk, near_own, i * chunk, chunk)

    def take_far(i):
        copy((i, "far")).wait_recv()
        add_rows(own, i * chunk, far, i * chunk, chunk)
        copy((i, "down", 0)).start()

    def take_level(i, k):
        _, before, after, spot = levels[k]
        copy((i, "down", k)).wait_recv()
        if after == before:
            copy((i, "down", k)).wait_send()
        final = k + 1 == len(levels)
        add_rows(
            own,
            i * chunk + shape_of(i)[1][k],
            landing,
            i * place + spot,
            after,
            gathered if final else None,
        )
        if not final:
            copy((i, "down", k + 1)).start()
        elif halved:
            copy((i, "up", halved[-1])).start()

    def take_up(i, n):
        copy((i, "up", halved[-1 - n])).wait_recv()
        if n + 1 < len(halved):
            copy((i, "up", halved[-2 - n])).start()

    def small_step(n):
        first = spans[n][0]
        copy(("small", n)).wait()
        land = small_land.at[n]
        small_s[16:24, :] += land[16 - first : 24 - first, :]
        if n == 0:
            small_s[32:40, :] += land[0:8, :]
            small_s[24:32, :] += land[8:16, :]
        elif n == 1:
            small_s[32:40, :] += land[8:16, :]
        else:
            small_s[32:40, :] += land[16:24, :]
        if n + 1 < len(spans):
            copy(("small", n + 1)).start()

    def weight_grads():
        query_sum = jnp.sum(widen(dq_ref[...]), 0, keepdims=True)
        value_sum = jnp.sum(widen(dv_ref[...]), 0, keepdims=True)
        blank = jnp.zeros((1, dim - 2 * part), F32)
        for j, row in enumerate((32, 0, 24, 8)):
            cols = slice(j * part, (j + 1) * part)
            small_s[row : row + 1, :] = jnp.concatenate(
                [query_sum[:, cols], value_sum[:, cols], blank], 1
            )
            small_s[row + 1 : row + 2, :] = hidden_sums[8 * j : 8 * j + 1, :]
        for kind, (left, right) in enumerate(
            ((dq_ref, normed_ref), (dk_ref, normed_ref), (dv_ref, normed_ref), (mixed_ref, low_s))
        ):
            result = dot_tn(left[...], right[...]).astype(BF)
            low, high = kind * part, (kind + 1) * part
            own[att + low : att + high, :] = result[:part]
            near_piece[low:high, :] = result[part : 2 * part]
            cross[att + low : att + high, :] = result[2 * part : 3 * part]
            last_piece[low:high, :] = result[3 * part :]

    def input_pair(pair):
        lax.fori_loop(2 * pair, 2 * pair + 2, input_block, 0)

    def input_block(block, carry):
        rows = pl.ds(pl.multiple_of(block * BLOCK, BLOCK), BLOCK)
        unit, scale = normalize(widen(tokens_ref[rows, :]))
        grad = (
            dot_nn(dq_ref[rows, :], weights_ref[0])
            + dot_nn(dk_ref[rows, :], weights_ref[1])
            + dot_nn(dv_ref[rows, :], weights_ref[2])
        )
        small_s[16:17, :] += jnp.sum(grad * unit, 0, keepdims=True)
        small_s[17:18, :] += jnp.sum(grad, 0, keepdims=True)
        back = normalize_back(grad * vec_ref[0:1, :], unit, scale)
        input_grad_ref[rows, :] = (middle_grad_s[rows, :] + back).astype(BF)
        return carry

    span = 4.9 * chunk / 128
    tasks = []

    def add(when, task, *args):
        tasks.append((when, len(tasks), functools.partial(task, *args)))

    for i in range(subs):
        arrive = 2.0 + span * (i + 1)
        if i < 2 * each:
            add(1.0 + 0.2 * span * i, start_cross, i)
        else:
            add(36.0, core_send, i)
            add(39.0 + 0.2 * span * (i - 2 * each), start_cross, i)
        add(arrive, take_far, i)
        for k in range(len(levels)):
            add(arrive + span * (1 + k), take_level, i, k)
        for n in range(len(halved)):
            add(arrive + span * (1 + len(levels) + n), take_up, i, n)
    blocks = tokens_ref.shape[0] // BLOCK
    add(27.0, weight_grads)
    for pair in range(blocks // 2):
        add(35.0 + 5.0 * pair, input_pair, pair)
    end = 37.0 + 2.5 * blocks
    add(end, lambda: copy(("small", 0)).start())
    for n in range(len(spans)):
        add(end + 4.0 + 4.0 * n, small_step, n)
    tasks.sort(key=lambda entry: entry[:2])

    def run(low, high):
        for when, _, task in tasks:
            if low <= when < high:
                task()

    @pl.when(step == 0)
    def _():
        barrier = pltpu.get_barrier_semaphore()
        for peer in peers.values():
            pl.semaphore_signal(
                barrier, inc=1, device_id=peer, device_id_type=pl.DeviceIdType.MESH
            )
        pl.semaphore_wait(barrier, len(peers))
        for i in range(2 * each):
            core_send(i)
        mask_ref[...] = diagonal_mask(GROUP * HDIM)
        small_s[...] = jnp.zeros_like(small_s)

    all_rows = pl.ds(pl.multiple_of(step * BLOCK, BLOCK), BLOCK)
    vec = vec_ref[...]
    upstream = widen(grad_ref[...])
    unit, scale = normalize(middle_ref[...])
    inner = inner_ref[...]
    middle_grad = upstream + normalize_back(inner * vec[3:4], unit, scale)
    middle_grad_s[all_rows, :] = middle_grad
    middle_low = middle_grad.astype(BF)
    low_s[all_rows, :] = middle_low
    small_s[18:19, :] += jnp.sum(middle_grad, 0, keepdims=True)
    small_s[19:20, :] += jnp.sum(inner * unit, 0, keepdims=True)
    small_s[20:21, :] += jnp.sum(inner, 0, keepdims=True)
    small_s[21:22, :] += jnp.sum(upstream, 0, keepdims=True)
    mixed_grad_s[...] = dot_nt(middle_low, weights_ref[3]).astype(BF)
    width = GROUP * HDIM
    factor = 1.0 / math.sqrt(HDIM)
    mask = mask_ref[...]
    for c in range(BLOCK // LMAX):
        rows = pl.ds(c * LMAX, LMAX)
        into = pl.ds(pl.multiple_of(step * BLOCK + c * LMAX, LMAX), LMAX)
        for block in range(blocks):
            slot = block * (BLOCK // LMAX) + c

            @pl.when(step == block)
            def _():
                run(0.5 + 1.5 * slot, 2.0 + 1.5 * slot)

        for g in range(dim // width):
            cols = pl.ds(g * width, width)
            wide = spread_heads(mixed_grad_s[rows, cols], mask)
            probs = probs_ref[rows, cols]
            prob_grad = dot_nt(v_ref[rows, cols], wide)
            dv_ref[into, cols] = dot_nn(probs.astype(BF), wide).astype(BF)
            weighted = jnp.sum(probs * prob_grad, 0, keepdims=True)
            score_grad = (probs * (prob_grad - weighted)).astype(BF)
            queries = spread_heads(q_ref[rows, cols], mask)
            dk_ref[into, cols] = (dot_nn(score_grad, queries) * factor).astype(BF)
            crossed = dot_tn(score_grad, k_ref[rows, cols])
            dq_ref[into, cols] = (pick_heads(crossed) * factor).astype(BF)

    @pl.when(step == last)
    def _():
        run(0.5 + 1.5 * blocks * (BLOCK // LMAX), 1e9)
        outs = [
            pltpu.make_async_copy(
                gathered.at[pl.ds(n * dim, dim), :], out_refs[n], out_sem.at[n]
            )
            for n in range(3)
        ]
        for out in outs:
            out.start()
        small_out[...] = small_s[...]
        for key in recipes:
            repeated = key[0] == "small" or (
                key[1] == "down" and levels[key[2]][1] == levels[key[2]][2]
            )
            if not repeated:
                copy(key).wait_send()
        for out in outs:
            out.wait()


def backward(masks, blocked, whole, weights, vec, hidden_sums, groups):
    rows, dim = blocked[0].shape
    levels, place = plan_levels(masks, CHUNK)
    total = 3 * dim
    subs = total // CHUNK
    halved = sum(level[1] != level[2] for level in levels)
    copies = subs * (3 + len(levels) + halved) + 2 + len(masks)
    anywhere = pl.BlockSpec(memory_space=pl.ANY)
    buffer = pltpu.VMEM((total, dim), BF)
    all_rows = pltpu.VMEM((rows, dim), BF)
    return pl.pallas_call(
        functools.partial(reduce_kernel, masks, CHUNK),
        grid=(rows // BLOCK,),
        in_specs=[rowed(dim)] * len(blocked)
        + [once((rows, dim))] * len(whole)
        + [once(weights.shape), full(vec.shape)]
        + [once(hidden_sums.shape)]
        + [anywhere] * len(groups),
        out_specs=[once((rows, dim)), full((40, dim))] + [anywhere] * 3,
        out_shape=[
            jax.ShapeDtypeStruct((rows, dim), BF),
            jax.ShapeDtypeStruct((40, dim), F32),
        ]
        + [jax.ShapeDtypeStruct((dim, dim), BF)] * 3,
        scratch_shapes=[
            pltpu.VMEM((GROUP * HDIM, GROUP * HDIM), BF),
            all_rows,
            pltpu.VMEM((BLOCK, dim), BF),
            pltpu.VMEM((rows, dim), F32),
            all_rows,
            all_rows,
            all_rows,
            pltpu.VMEM((dim, dim), BF),
            pltpu.VMEM((dim, dim), BF),
            buffer,
            buffer,
            buffer,
            buffer,
            buffer,
            pltpu.VMEM((subs * place, dim), BF),
            buffer,
            pltpu.VMEM((40, dim), F32),
            pltpu.VMEM((2 + len(masks), 24, dim), F32),
            pltpu.SemaphoreType.DMA((copies,)),
            pltpu.SemaphoreType.DMA((copies,)),
            pltpu.SemaphoreType.DMA((2 * subs,)),
            pltpu.SemaphoreType.DMA((3,)),
        ],
        compiler_params=pltpu.CompilerParams(
            dimension_semantics=("arbitrary",),
            collective_id=0,
            has_side_effects=True,
            vmem_limit_bytes=66 * 1024 * 1000,
        ),
        name="attend_back",
    )(*blocked, *whole, weights, vec, hidden_sums, *groups)


def lay_out(size, vectors, pitch, kind):
    out = None
    for i, values in enumerate(vectors):
        start = i * pitch
        piece = lax.pad(
            values.astype(kind), jnp.zeros((), kind), [(start, size - start - values.shape[0], 0)]
        )
        out = piece if out is None else out + piece
    return out


def per_device(
    ndp,
    nt,
    caption_tokens,
    caption_lengths,
    output_grad,
    norm_gain,
    norm_bias,
    query_weight,
    query_bias,
    key_weight,
    value_weight,
    value_bias,
    output_weight,
    output_bias,
    second_gain,
    second_bias,
    hidden_weight,
    hidden_bias,
    down_weight,
    down_bias,
):
    masks, mask = [], 1
    while mask < ndp:
        masks.append(mask)
        mask *= 2
    rows, dim = caption_tokens.shape
    part = query_weight.shape[1]
    biases = lay_out(PAD * dim, (query_bias, hidden_bias, value_bias), dim, BF).reshape(PAD, dim)
    shard = jnp.concatenate([query_weight.T, key_weight.T, value_weight.T, output_weight, biases], 0)
    vec = lay_out(
        8 * dim, (norm_gain, norm_bias, output_bias, second_gain, second_bias, down_bias), dim, F32
    ).reshape(8, dim)
    normed, q, k, v, probs, mixed, middle, second, weights, bias, ups, downs = forward(
        caption_lengths, caption_tokens, shard, hidden_weight, down_weight, vec
    )
    result, inner, up_grads, down_grads, hidden_sums = expert(
        second, output_grad, middle, ups, downs, bias, vec
    )
    token_grad, packed, grad_up, grad_down, grad_att = backward(
        tuple(masks),
        [output_grad, middle, inner, q, k, v, probs],
        [mixed, normed, caption_tokens],
        weights,
        vec,
        hidden_sums,
        [up_grads, down_grads],
    )
    grad_up, grad_down, grad_att = widen(grad_up), widen(grad_down), widen(grad_att)
    sums, mine = packed[16:24], packed[32:34]
    return (
        result,
        token_grad,
        sums[0],
        sums[1],
        grad_att[:part].T,
        mine[0, :part],
        grad_att[part : 2 * part].T,
        grad_att[2 * part : 3 * part].T,
        mine[0, part : 2 * part],
        grad_att[3 * part :],
        sums[2],
        sums[3],
        sums[4],
        grad_up,
        mine[1],
        grad_down,
        sums[5],
    )


def solution(mesh):
    ndp, nt = mesh.shape["dp"], mesh.shape["tensor"]
    both = P(("dp", "tensor"), None)
    col, row, vec = P(None, "tensor"), P("tensor", None), P("tensor")

    def body(*args):
        return per_device(ndp, nt, *args)

    return jax.shard_map(
        body,
        mesh=mesh,
        in_specs=(both, P("dp"), both, P(), P(), col, vec, col, col, vec, row, P(), P(), P(), col, vec, row, P()),
        out_specs=(both, both, P(), P(), col, vec, col, col, vec, row, P(), P(), P(), col, vec, row, P()),
        check_vma=False,
    )
```

```python
import functools
import math

import jax
import jax.numpy as jnp
from jax import lax
from jax.experimental import pallas as pl
from jax.experimental.pallas import tpu as pltpu
from jax.sharding import PartitionSpec as P


HDIM = 64
LMAX = 64
EPS = 1e-05
NEG = -1e30
GROUP = 4
BLOCK = 256
PAD = 32
CHUNK = 128
TILE = 128
AXES = ("dp", "tensor")
BF = jnp.bfloat16
F32 = jnp.float32
VMEM_LIMIT = 60 * 1024 * 1024


def widen(values):
    return values.astype(F32)


def dot_nn(left, right):
    return jnp.dot(left, right, preferred_element_type=F32)


def dot_nt(left, right):
    return lax.dot_general(left, right, (((1,), (1,)), ((), ())), preferred_element_type=F32)


def dot_tn(left, right):
    return lax.dot_general(left, right, (((0,), (0,)), ((), ())), preferred_element_type=F32)


def normalize(values):
    center = jnp.mean(values, -1, keepdims=True)
    spread = values - center
    scale = lax.rsqrt(jnp.mean(spread * spread, -1, keepdims=True) + EPS)
    return spread * scale, scale


def normalize_back(grad, unit, scale):
    return scale * (
        grad - jnp.mean(grad, -1, keepdims=True) - unit * jnp.mean(grad * unit, -1, keepdims=True)
    )


def erf(values):
    values = jnp.clip(values, -4.0, 4.0)
    square = values * values
    top = -2.72614225801306e-10
    for coef in (
        2.77068142495902e-08,
        -2.10102402082508e-06,
        -5.69250639462346e-05,
        -7.34990630326855e-04,
        -2.95459980854025e-03,
        -1.60960333262415e-02,
    ):
        top = top * square + coef
    low = -1.45660718464996e-05
    for coef in (
        -2.13374055278905e-04,
        -1.68282697438203e-03,
        -7.37332916720468e-03,
        -1.42647390514189e-02,
    ):
        low = low * square + coef
    return values * top / low


def diagonal_mask(size):
    rows = lax.shift_right_logical(lax.broadcasted_iota(jnp.int32, (size, size), 0), 6)
    cols = lax.shift_right_logical(lax.broadcasted_iota(jnp.int32, (size, size), 1), 6)
    return jnp.where(rows == cols, 1.0, 0.0).astype(BF)


def spread_heads(values, mask):
    return jnp.concatenate([values] * GROUP, 0) * mask


def pick_heads(values):
    lane = lax.shift_right_logical(
        lax.broadcasted_iota(jnp.int32, (LMAX, values.shape[1]), 1), 6
    )
    out = values[:LMAX]
    for head in range(1, GROUP):
        out = jnp.where(lane == head, values[head * LMAX : (head + 1) * LMAX], out)
    return out


def full(shape):
    return pl.BlockSpec(shape, lambda i, *_: (0,) * len(shape))


def rowed(width):
    return pl.BlockSpec((BLOCK, width), lambda i, *_: (i, 0))


def params():
    return pltpu.CompilerParams(
        dimension_semantics=("arbitrary",), vmem_limit_bytes=VMEM_LIMIT
    )


def split_rows(rows):
    count = rows // 16
    spans, start = [], 0
    for k in range(3):
        size = (count * (k + 1) // 3 - count * k // 3) * 16
        spans.append((start, size))
        start += size
    return spans


def forward_kernel(
    length_ref,
    tokens_ref,
    shard_ref,
    up_ref,
    down_ref,
    vec_ref,
    normed_ref,
    q_ref,
    k_ref,
    v_ref,
    probs_ref,
    mixed_ref,
    middle_ref,
    second_ref,
    weights_ref,
    bias_ref,
    up_all,
    down_all,
    mask_ref,
    land_ref,
    stage_ref,
    vector_s,
    send_sem,
    recv_sem,
    local_sem,
):
    step = pl.program_id(0)
    dim = tokens_ref.shape[1]
    part = dim // 4
    dp = lax.axis_index("dp")
    t = lax.axis_index("tensor")
    bit = dp % 2
    peers = {
        "core": (dp, t + 1 - 2 * (t % 2)),
        "far": (dp, t + 2 - 4 * ((t // 2) % 2)),
        "side": (dp + 1 - 2 * bit, t),
    }
    chunks = [
        (shard_ref, land_ref.at[1], land_ref.at[2], land_ref.at[3]),
        (up_ref, up_all.at[1], up_all.at[2], up_all.at[3]),
        (down_ref, down_all.at[1], down_all.at[2], down_all.at[3]),
    ]
    recipes = {}

    def recipe(key, source, target, peer):
        recipes[key] = (len(recipes), source, target, peer)

    for c, (shard, near, cross, last) in enumerate(chunks):
        half = shard.shape[0] // 2
        recipe((c, "near"), shard, near, "core")
        for n, (start, size) in enumerate(split_rows(half)):
            mine = pl.ds(pl.multiple_of(bit * half + start, 16), size)
            other = pl.ds(pl.multiple_of((1 - bit) * half + start, 16), size)
            recipe((c, "y", n), shard.at[mine, :], cross.at[mine, :], "far")
            recipe((c, "x", n), cross.at[mine, :], cross.at[mine, :], "side")
            recipe((c, "a", n), cross.at[mine, :], last.at[mine, :], "core")
            recipe((c, "b", n), cross.at[other, :], last.at[other, :], "core")

    def copy(key):
        slot, source, target, peer = recipes[key]
        return pltpu.make_async_remote_copy(
            src_ref=source,
            dst_ref=target,
            send_sem=send_sem.at[slot],
            recv_sem=recv_sem.at[slot],
            device_id=peers[peer],
            device_id_type=pl.DeviceIdType.MESH,
        )

    def own_copy(n, out):
        source, target = ((up_ref, up_all), (down_ref, down_all))[n]
        if out:
            return pltpu.make_async_copy(stage_ref.at[n], target.at[0], local_sem.at[3 + n])
        return pltpu.make_async_copy(source, stage_ref.at[n], local_sem.at[1 + n])

    def pass_y(c, n):
        copy((c, "y", n)).wait_recv()
        copy((c, "x", n)).start()
        copy((c, "a", n)).start()

    def pass_x(c, n):
        copy((c, "x", n)).wait_recv()
        copy((c, "b", n)).start()

    @pl.when(step == 0)
    def _():
        barrier = pltpu.get_barrier_semaphore()
        for peer in peers.values():
            pl.semaphore_signal(
                barrier, inc=1, device_id=peer, device_id_type=pl.DeviceIdType.MESH
            )
        pl.semaphore_wait(barrier, 3)
        own = pltpu.make_async_copy(shard_ref, land_ref.at[0], local_sem.at[0])
        own.start()
        for c in range(3):
            for n in range(3):
                copy((c, "y", n)).start()
            copy((c, "near")).start()
        for n in range(2):
            own_copy(n, False).start()
        mask_ref[...] = diagonal_mask(GROUP * HDIM)
        own.wait()
        pass_y(0, 0)
        pass_y(0, 1)
        pass_x(0, 0)
        pass_y(0, 2)
        pass_x(0, 1)
        pass_x(0, 2)
        copy((0, "near")).wait_recv()
        for n in range(3):
            copy((0, "a", n)).wait_recv()
            copy((0, "b", n)).wait_recv()
        for j in range(4):
            for kind in range(4):
                weights_ref[kind, j * part : (j + 1) * part, :] = land_ref[
                    j, kind * part : (kind + 1) * part, :
                ]
        rows = [widen(land_ref[j, 4 * part : 4 * part + 16, :]) for j in range(4)]
        vector_s[0:1, :] = jnp.concatenate([r[0:1, :part] for r in rows], 1)
        vector_s[1:2, :] = jnp.concatenate([r[2:3, :part] for r in rows], 1)
        for j in range(4):
            bias_ref[8 * j : 8 * j + 8, :] = jnp.broadcast_to(rows[j][1:2], (8, dim))
        pass_y(1, 0)
        pass_y(1, 1)

    @pl.when(step == 1)
    def _():
        for n in range(2):
            own_copy(n, False).wait()
            own_copy(n, True).start()
        pass_x(1, 0)
        pass_y(1, 2)
        pass_x(1, 1)
        pass_y(2, 0)

    @pl.when(step == 2)
    def _():
        pass_x(1, 2)
        pass_y(2, 1)
        pass_x(2, 0)

    @pl.when(step == 3)
    def _():
        pass_y(2, 2)
        pass_x(2, 1)

    tokens = widen(tokens_ref[...])
    vec = vec_ref[...]
    unit, _ = normalize(tokens)
    normed = (unit * vec[0:1] + vec[1:2]).astype(BF)
    normed_ref[...] = normed
    q_ref[...] = (dot_nt(normed, weights_ref[0]) + vector_s[0:1, :]).astype(BF)
    k_ref[...] = dot_nt(normed, weights_ref[1]).astype(BF)
    v_ref[...] = (dot_nt(normed, weights_ref[2]) + vector_s[1:2, :]).astype(BF)
    width = GROUP * HDIM
    factor = 1.0 / math.sqrt(HDIM)
    mask = mask_ref[...]
    for c in range(BLOCK // LMAX):
        rows = pl.ds(c * LMAX, LMAX)
        length = length_ref[
            (t * pl.num_programs(0) + step) * (BLOCK // LMAX) + c
        ]
        live = lax.broadcasted_iota(jnp.int32, (LMAX, width), 0) < length
        for g in range(dim // width):
            cols = pl.ds(g * width, width)
            wide = spread_heads(q_ref[rows, cols], mask)
            scores = dot_nt(k_ref[rows, cols], wide) * factor
            scores = jnp.where(live, scores, NEG)
            exponent = jnp.exp(scores - jnp.max(scores, 0, keepdims=True))
            probs = exponent * (1.0 / jnp.sum(exponent, 0, keepdims=True))
            probs_ref[rows, cols] = probs
            crossed = dot_tn(probs.astype(BF), v_ref[rows, cols])
            mixed_ref[rows, cols] = pick_heads(crossed).astype(BF)
    middle = tokens + dot_nn(mixed_ref[...], weights_ref[3]) + vec[2:3]
    middle_ref[...] = middle
    unit, _ = normalize(middle)
    second_ref[...] = (unit * vec[3:4] + vec[4:5]).astype(BF)

    @pl.when(step == pl.num_programs(0) - 1)
    def _():
        pass_x(2, 2)
        for c in (1, 2):
            copy((c, "near")).wait_recv()
            for n in range(3):
                copy((c, "a", n)).wait_recv()
                copy((c, "b", n)).wait_recv()
        for key in recipes:
            copy(key).wait_send()
        for n in range(2):
            own_copy(n, True).wait()


def forward(lengths, tokens, shard, up, down, vec):
    rows, dim = tokens.shape
    steps = rows // BLOCK
    shapes = [
        (dim, BF),
        (dim, BF),
        (dim, BF),
        (dim, BF),
        (dim, F32),
        (dim, BF),
        (dim, F32),
        (dim, BF),
    ]
    anywhere = pl.BlockSpec(memory_space=pl.ANY)
    copies = 3 * 13
    return pl.pallas_call(
        forward_kernel,
        grid_spec=pltpu.PrefetchScalarGridSpec(
            num_scalar_prefetch=1,
            grid=(steps,),
            in_specs=[rowed(dim), anywhere, anywhere, anywhere, full(vec.shape)],
            out_specs=[rowed(width) for width, _ in shapes]
            + [full((4, dim, dim)), full((32, dim))]
            + [anywhere] * 2,
            scratch_shapes=[
                pltpu.VMEM((GROUP * HDIM, GROUP * HDIM), BF),
                pltpu.VMEM((4,) + shard.shape, BF),
                pltpu.VMEM((2,) + up.shape, BF),
                pltpu.VMEM((8, dim), F32),
                pltpu.SemaphoreType.DMA((copies,)),
                pltpu.SemaphoreType.DMA((copies,)),
                pltpu.SemaphoreType.DMA((5,)),
            ],
        ),
        out_shape=[jax.ShapeDtypeStruct((rows, width), kind) for width, kind in shapes]
        + [jax.ShapeDtypeStruct((4, dim, dim), BF), jax.ShapeDtypeStruct((32, dim), F32)]
        + [
            jax.ShapeDtypeStruct((4,) + up.shape, BF),
            jax.ShapeDtypeStruct((4,) + down.shape, BF),
        ],
        compiler_params=pltpu.CompilerParams(
            dimension_semantics=("arbitrary",),
            vmem_limit_bytes=VMEM_LIMIT,
            collective_id=1,
            has_side_effects=True,
        ),
        name="attend",
    )(lengths, tokens, shard, up, down, vec)


def expert_kernel(
    second_ref,
    grad_ref,
    middle_ref,
    up_ref,
    down_ref,
    bias_ref,
    vec_ref,
    result_ref,
    total_ref,
    up_grad_ref,
    down_grad_ref,
    bias_grad_ref,
    sum_s,
    active_s,
    hidden_s,
):
    piece = pl.program_id(0)
    step = pl.program_id(1)
    rows = pl.ds(pl.multiple_of(step * BLOCK, BLOCK), BLOCK)
    hidden = dot_nn(second_ref[rows, :], up_ref[...]) + bias_ref[0:1, :]
    lean = 0.5 + 0.5 * erf(hidden * (1.0 / math.sqrt(2.0)))
    slope = lean + hidden * (jnp.exp(-0.5 * hidden * hidden) * (1.0 / math.sqrt(2.0 * math.pi)))
    active = (hidden * lean).astype(BF)
    active_s[rows, :] = active
    back = (dot_nt(grad_ref[rows, :], down_ref[...]) * slope).astype(BF)
    hidden_s[rows, :] = back
    result = dot_nn(active, down_ref[...])
    total = dot_nt(back, up_ref[...])

    @pl.when(piece == 0)
    def _():
        sum_s[rows, :] = result + middle_ref[rows, :]
        total_ref[rows, :] = total

    @pl.when(piece > 0)
    def _():
        sum_s[rows, :] += result
        total_ref[rows, :] += total

    @pl.when(piece == pl.num_programs(0) - 1)
    def _():
        result_ref[rows, :] = (sum_s[rows, :] + vec_ref[5:6, :]).astype(BF)

    @pl.when(step == pl.num_programs(1) - 1)
    def _():
        down_grad_ref[...] = dot_tn(active_s[...], grad_ref[...]).astype(BF)
        up_grad_ref[...] = dot_tn(second_ref[...], hidden_s[...]).astype(BF)
        bias_grad_ref[...] = jnp.broadcast_to(
            jnp.sum(widen(hidden_s[...]), 0, keepdims=True), bias_grad_ref.shape
        )


def once(shape):
    return pl.BlockSpec(shape, lambda i, *_: (0,) * len(shape), pipeline_mode=pl.Buffered(1))


def expert(second, grad, middle, ups, downs, bias, vec):
    rows, dim = second.shape
    pieces, _, units = ups.shape

    def quarter(*shape):
        return pl.BlockSpec((None,) + shape, lambda p, i: (pieces - 1 - p, 0, 0))

    row = pl.BlockSpec((8, units), lambda p, i: (pieces - 1 - p, 0))
    return pl.pallas_call(
        expert_kernel,
        grid=(pieces, rows // BLOCK),
        in_specs=[once((rows, dim))] * 3
        + [quarter(dim, units), quarter(units, dim), row, once(vec.shape)],
        out_specs=[
            once((rows, dim)),
            once((rows, dim)),
            quarter(dim, units),
            quarter(units, dim),
            row,
        ],
        out_shape=[
            jax.ShapeDtypeStruct((rows, dim), BF),
            jax.ShapeDtypeStruct((rows, dim), F32),
            jax.ShapeDtypeStruct(ups.shape, BF),
            jax.ShapeDtypeStruct(downs.shape, BF),
            jax.ShapeDtypeStruct((8 * pieces, units), F32),
        ],
        scratch_shapes=[
            pltpu.VMEM((rows, dim), F32),
            pltpu.VMEM((rows, units), BF),
            pltpu.VMEM((rows, units), BF),
        ],
        compiler_params=pltpu.CompilerParams(
            dimension_semantics=("arbitrary", "arbitrary"), vmem_limit_bytes=VMEM_LIMIT
        ),
        cost_estimate=pl.CostEstimate(
            flops=12 * pieces * rows * dim * units,
            bytes_accessed=40 * rows * dim,
            transcendentals=2 * pieces * rows * units,
        ),
        name="expert",
    )(second, grad, middle, ups, downs, bias, vec)


def add_rows(into, base, other, other_base, rows, result=None):
    result = into if result is None else result
    size = min(rows, TILE)

    def body(i, carry):
        left = pl.ds(pl.multiple_of(base + i * size, 8), size)
        right = pl.ds(pl.multiple_of(other_base + i * size, 8), size)
        result[left, :] = (widen(into[left, :]) + widen(other[right, :])).astype(into.dtype)
        return carry

    lax.fori_loop(0, rows // size, body, 0)


def plan_levels(masks, rows):
    levels, place = [], 0
    for mask in masks:
        after = rows // 2 if (rows // 2) % 16 == 0 else rows
        levels.append((mask, rows, after, place))
        place += after
        rows = after
    return levels, place


def reduce_kernel(masks, chunk, *refs):
    (
        grad_ref,
        middle_ref,
        inner_ref,
        q_ref,
        k_ref,
        v_ref,
        probs_ref,
        mixed_ref,
        normed_ref,
        tokens_ref,
        weights_ref,
        vec_ref,
    ) = refs[:12]
    hidden_sums, sources, refs = refs[12], refs[13:15], refs[15:]
    input_grad_ref, small_out, refs = refs[0], refs[1], refs[2:]
    out_refs, refs = refs[:3], refs[3:]
    mask_ref, low_s, mixed_grad_s, middle_grad_s, dq_ref, dk_ref, dv_ref = refs[:7]
    near_piece, last_piece, own, cross, near_own, near_cross, far, landing, gathered = refs[7:16]
    small_s, small_land, send_sem, recv_sem, local_sem, out_sem = refs[16:]

    step = pl.program_id(0)
    last = 3
    dim = grad_ref.shape[1]
    part = dim // 4
    levels, place = plan_levels(masks, chunk)
    halved = [k for k, level in enumerate(levels) if level[2] != level[1]]
    each = dim // chunk
    subs = 3 * each
    att = 2 * dim
    dp = lax.axis_index("dp")
    t = lax.axis_index("tensor")
    bits = {mask: (dp // mask) % 2 for mask in masks}
    peers = {mask: (dp + mask - 2 * mask * bits[mask], t) for mask in masks}
    peers["core"] = (dp, t + 1 - 2 * (t % 2))
    peers["far"] = (dp, t + 2 - 4 * ((t // 2) % 2))
    keeps, leaves, at = [], [], 0
    for mask, before, after, _ in levels:
        if after == before:
            keep = leave = at
        else:
            keep = at + bits[mask] * after
            leave = at + after - bits[mask] * after
        keeps.append(keep)
        leaves.append(leave)
        at = keep

    recipes = {}

    def recipe(key, source, target, peer):
        recipes[key] = (len(recipes), source, target, peer)

    def window(base, offset, size):
        return pl.ds(pl.multiple_of(base + offset, 16), size)

    for i in range(subs):
        base = i * chunk
        here = pl.ds(base, chunk)
        within = pl.ds((i % each) * chunk, chunk)
        if i < 2 * each:
            near, farthest = sources[i // each].at[1], sources[i // each].at[3]
        else:
            near, farthest = near_piece, last_piece
        recipe((i, "near_cross"), farthest.at[within, :], near_cross.at[here, :], "core")
        recipe((i, "near_own"), near.at[within, :], near_own.at[here, :], "core")
        recipe((i, "far"), cross.at[here, :], far.at[here, :], "far")
        for k, (mask, before, after, spot) in enumerate(levels):
            recipe(
                (i, "down", k),
                own.at[window(base, leaves[k], after), :],
                landing.at[pl.ds(i * place + spot, after), :],
                mask,
            )
        for k in halved:
            rows = window(base, keeps[k], levels[k][2])
            recipe((i, "up", k), gathered.at[rows, :], gathered.at[rows, :], levels[k][0])
    small_peers = ["core", "far"] + list(masks)
    spans = [(0, 24), (16, 16)] + [(16, 24)] * len(masks)
    for n, (first, count) in enumerate(spans):
        recipe(
            ("small", n),
            small_s.at[pl.ds(first, count), :],
            small_land.at[n, pl.ds(0, count), :],
            small_peers[n],
        )

    def copy(key):
        slot, source, target, peer = recipes[key]
        return pltpu.make_async_remote_copy(
            src_ref=source,
            dst_ref=target,
            send_sem=send_sem.at[slot],
            recv_sem=recv_sem.at[slot],
            device_id=peers[peer],
            device_id_type=pl.DeviceIdType.MESH,
        )

    def local_pair(i):
        within = pl.ds((i % each) * chunk, chunk)
        here = pl.ds(i * chunk, chunk)
        group = sources[i // each]
        return [
            pltpu.make_async_copy(group.at[2, within, :], cross.at[here, :], local_sem.at[2 * i]),
            pltpu.make_async_copy(group.at[0, within, :], own.at[here, :], local_sem.at[2 * i + 1]),
        ]

    def core_send(i):
        copy((i, "near_cross")).start()
        copy((i, "near_own")).start()
        if i < 2 * each:
            for piece in local_pair(i):
                piece.start()

    def start_cross(i):
        if i < 2 * each:
            for piece in local_pair(i):
                piece.wait()
        copy((i, "near_cross")).wait_recv()
        add_rows(cross, i * chunk, near_cross, i * chunk, chunk)
        copy((i, "far")).start()
        copy((i, "near_own")).wait_recv()
        add_rows(own, i * chunk, near_own, i * chunk, chunk)

    def take_far(i):
        copy((i, "far")).wait_recv()
        add_rows(own, i * chunk, far, i * chunk, chunk)
        copy((i, "down", 0)).start()

    def take_level(i, k):
        _, before, after, spot = levels[k]
        copy((i, "down", k)).wait_recv()
        if after == before:
            copy((i, "down", k)).wait_send()
        final = k + 1 == len(levels)
        add_rows(
            own,
            i * chunk + keeps[k],
            landing,
            i * place + spot,
            after,
            gathered if final else None,
        )
        if not final:
            copy((i, "down", k + 1)).start()
        elif halved:
            copy((i, "up", halved[-1])).start()

    def take_up(i, n):
        copy((i, "up", halved[-1 - n])).wait_recv()
        if n + 1 < len(halved):
            copy((i, "up", halved[-2 - n])).start()

    def small_step(n):
        first = spans[n][0]
        copy(("small", n)).wait()
        land = small_land.at[n]
        small_s[16:24, :] += land[16 - first : 24 - first, :]
        if n == 0:
            small_s[32:40, :] += land[0:8, :]
            small_s[24:32, :] += land[8:16, :]
        elif n == 1:
            small_s[32:40, :] += land[8:16, :]
        else:
            small_s[32:40, :] += land[16:24, :]
        if n + 1 < len(spans):
            copy(("small", n + 1)).start()

    def weight_grads():
        query_sum = jnp.sum(widen(dq_ref[...]), 0, keepdims=True)
        value_sum = jnp.sum(widen(dv_ref[...]), 0, keepdims=True)
        blank = jnp.zeros((1, dim - 2 * part), F32)
        for j, row in enumerate((32, 0, 24, 8)):
            cols = slice(j * part, (j + 1) * part)
            small_s[row : row + 1, :] = jnp.concatenate(
                [query_sum[:, cols], value_sum[:, cols], blank], 1
            )
            small_s[row + 1 : row + 2, :] = hidden_sums[8 * j : 8 * j + 1, :]
        for kind, (left, right) in enumerate(
            ((dq_ref, normed_ref), (dk_ref, normed_ref), (dv_ref, normed_ref), (mixed_ref, low_s))
        ):
            result = dot_tn(left[...], right[...]).astype(BF)
            low, high = kind * part, (kind + 1) * part
            own[att + low : att + high, :] = result[:part]
            near_piece[low:high, :] = result[part : 2 * part]
            cross[att + low : att + high, :] = result[2 * part : 3 * part]
            last_piece[low:high, :] = result[3 * part :]

    def input_pair(pair):
        lax.fori_loop(2 * pair, 2 * pair + 2, input_block, 0)

    def input_block(block, carry):
        rows = pl.ds(pl.multiple_of(block * BLOCK, BLOCK), BLOCK)
        unit, scale = normalize(widen(tokens_ref[rows, :]))
        grad = (
            dot_nn(dq_ref[rows, :], weights_ref[0])
            + dot_nn(dk_ref[rows, :], weights_ref[1])
            + dot_nn(dv_ref[rows, :], weights_ref[2])
        )
        small_s[16:17, :] += jnp.sum(grad * unit, 0, keepdims=True)
        small_s[17:18, :] += jnp.sum(grad, 0, keepdims=True)
        back = normalize_back(grad * vec_ref[0:1, :], unit, scale)
        input_grad_ref[rows, :] = (middle_grad_s[rows, :] + back).astype(BF)
        return carry

    span = 3.0 * chunk / 128
    tasks = []

    def add(when, task, *args):
        tasks.append((when, len(tasks), functools.partial(task, *args)))

    for i in range(subs):
        arrive = 2.0 + span * (i + 1)
        if i < 2 * each:
            add(1.0 + 0.2 * span * i, start_cross, i)
        else:
            add(36.0, core_send, i)
            add(39.0 + 0.2 * span * (i - 2 * each), start_cross, i)
        add(arrive, take_far, i)
        for k in range(len(levels)):
            add(arrive + span * (1 + k), take_level, i, k)
        for n in range(len(halved)):
            add(arrive + span * (1 + len(levels) + n), take_up, i, n)
    blocks = tokens_ref.shape[0] // BLOCK
    add(27.0, weight_grads)
    for pair in range(blocks // 2):
        add(35.0 + 5.0 * pair, input_pair, pair)
    end = 37.0 + 2.5 * blocks
    add(end, lambda: copy(("small", 0)).start())
    for n in range(len(spans)):
        add(end + 4.0 + 4.0 * n, small_step, n)
    tasks.sort(key=lambda entry: entry[:2])

    def run(low, high):
        for when, _, task in tasks:
            if low <= when < high:
                task()

    @pl.when(step == 0)
    def _():
        barrier = pltpu.get_barrier_semaphore()
        for peer in peers.values():
            pl.semaphore_signal(
                barrier, inc=1, device_id=peer, device_id_type=pl.DeviceIdType.MESH
            )
        pl.semaphore_wait(barrier, len(peers))
        for i in range(2 * each):
            core_send(i)
        mask_ref[...] = diagonal_mask(GROUP * HDIM)
        small_s[...] = jnp.zeros_like(small_s)

    all_rows = pl.ds(pl.multiple_of(step * BLOCK, BLOCK), BLOCK)
    vec = vec_ref[...]
    upstream = widen(grad_ref[...])
    unit, scale = normalize(middle_ref[...])
    inner = inner_ref[...]
    middle_grad = upstream + normalize_back(inner * vec[3:4], unit, scale)
    middle_grad_s[all_rows, :] = middle_grad
    middle_low = middle_grad.astype(BF)
    low_s[all_rows, :] = middle_low
    small_s[18:19, :] += jnp.sum(middle_grad, 0, keepdims=True)
    small_s[19:20, :] += jnp.sum(inner * unit, 0, keepdims=True)
    small_s[20:21, :] += jnp.sum(inner, 0, keepdims=True)
    small_s[21:22, :] += jnp.sum(upstream, 0, keepdims=True)
    mixed_grad_s[...] = dot_nt(middle_low, weights_ref[3]).astype(BF)
    width = GROUP * HDIM
    factor = 1.0 / math.sqrt(HDIM)
    mask = mask_ref[...]
    for c in range(BLOCK // LMAX):
        rows = pl.ds(c * LMAX, LMAX)
        into = pl.ds(pl.multiple_of(step * BLOCK + c * LMAX, LMAX), LMAX)
        for block in range(blocks):
            slot = block * (BLOCK // LMAX) + c

            @pl.when(step == block)
            def _():
                run(0.5 + 1.5 * slot, 2.0 + 1.5 * slot)

        for g in range(dim // width):
            cols = pl.ds(g * width, width)
            wide = spread_heads(mixed_grad_s[rows, cols], mask)
            probs = probs_ref[rows, cols]
            prob_grad = dot_nt(v_ref[rows, cols], wide)
            dv_ref[into, cols] = dot_nn(probs.astype(BF), wide).astype(BF)
            weighted = jnp.sum(probs * prob_grad, 0, keepdims=True)
            score_grad = (probs * (prob_grad - weighted)).astype(BF)
            queries = spread_heads(q_ref[rows, cols], mask)
            dk_ref[into, cols] = (dot_nn(score_grad, queries) * factor).astype(BF)
            crossed = dot_tn(score_grad, k_ref[rows, cols])
            dq_ref[into, cols] = (pick_heads(crossed) * factor).astype(BF)

    @pl.when(step == last)
    def _():
        run(0.5 + 1.5 * blocks * (BLOCK // LMAX), 1e9)
        outs = [
            pltpu.make_async_copy(
                gathered.at[pl.ds(n * dim, dim), :], out_refs[n], out_sem.at[n]
            )
            for n in range(3)
        ]
        for out in outs:
            out.start()
        small_out[...] = small_s[...]
        for key in recipes:
            repeated = key[0] == "small" or (
                key[1] == "down" and levels[key[2]][1] == levels[key[2]][2]
            )
            if not repeated:
                copy(key).wait_send()
        for out in outs:
            out.wait()


def backward(masks, blocked, whole, weights, vec, hidden_sums, groups):
    rows, dim = blocked[0].shape
    levels, place = plan_levels(masks, CHUNK)
    total = 3 * dim
    subs = total // CHUNK
    halved = sum(level[1] != level[2] for level in levels)
    copies = subs * (3 + len(levels) + halved) + 2 + len(masks)
    anywhere = pl.BlockSpec(memory_space=pl.ANY)
    buffer = pltpu.VMEM((total, dim), BF)
    all_rows = pltpu.VMEM((rows, dim), BF)
    return pl.pallas_call(
        functools.partial(reduce_kernel, masks, CHUNK),
        grid=(rows // BLOCK,),
        in_specs=[rowed(dim)] * len(blocked)
        + [once((rows, dim))] * len(whole)
        + [once(weights.shape), full(vec.shape)]
        + [once(hidden_sums.shape)]
        + [anywhere] * len(groups),
        out_specs=[once((rows, dim)), full((40, dim))] + [anywhere] * 3,
        out_shape=[
            jax.ShapeDtypeStruct((rows, dim), BF),
            jax.ShapeDtypeStruct((40, dim), F32),
        ]
        + [jax.ShapeDtypeStruct((dim, dim), BF)] * 3,
        scratch_shapes=[
            pltpu.VMEM((GROUP * HDIM, GROUP * HDIM), BF),
            all_rows,
            pltpu.VMEM((BLOCK, dim), BF),
            pltpu.VMEM((rows, dim), F32),
            all_rows,
            all_rows,
            all_rows,
            pltpu.VMEM((dim, dim), BF),
            pltpu.VMEM((dim, dim), BF),
            buffer,
            buffer,
            buffer,
            buffer,
            buffer,
            pltpu.VMEM((subs * place, dim), BF),
            buffer,
            pltpu.VMEM((40, dim), F32),
            pltpu.VMEM((2 + len(masks), 24, dim), F32),
            pltpu.SemaphoreType.DMA((copies,)),
            pltpu.SemaphoreType.DMA((copies,)),
            pltpu.SemaphoreType.DMA((2 * subs,)),
            pltpu.SemaphoreType.DMA((3,)),
        ],
        compiler_params=pltpu.CompilerParams(
            dimension_semantics=("arbitrary",),
            collective_id=0,
            has_side_effects=True,
            vmem_limit_bytes=66 * 1024 * 1000,
        ),
        name="attend_back",
    )(*blocked, *whole, weights, vec, hidden_sums, *groups)


def lay_out(size, vectors, pitch, kind):
    out = None
    for i, values in enumerate(vectors):
        start = i * pitch
        piece = lax.pad(
            values.astype(kind), jnp.zeros((), kind), [(start, size - start - values.shape[0], 0)]
        )
        out = piece if out is None else out + piece
    return out


def per_device(
    ndp,
    nt,
    caption_tokens,
    caption_lengths,
    output_grad,
    norm_gain,
    norm_bias,
    query_weight,
    query_bias,
    key_weight,
    value_weight,
    value_bias,
    output_weight,
    output_bias,
    second_gain,
    second_bias,
    hidden_weight,
    hidden_bias,
    down_weight,
    down_bias,
):
    masks, mask = [], 1
    while mask < ndp:
        masks.append(mask)
        mask *= 2
    rows, dim = caption_tokens.shape
    part = query_weight.shape[1]
    biases = lay_out(PAD * dim, (query_bias, hidden_bias, value_bias), dim, BF).reshape(PAD, dim)
    shard = jnp.concatenate([query_weight.T, key_weight.T, value_weight.T, output_weight, biases], 0)
    vec = lay_out(
        8 * dim, (norm_gain, norm_bias, output_bias, second_gain, second_bias, down_bias), dim, F32
    ).reshape(8, dim)
    normed, q, k, v, probs, mixed, middle, second, weights, bias, ups, downs = forward(
        caption_lengths, caption_tokens, shard, hidden_weight, down_weight, vec
    )
    result, inner, up_grads, down_grads, hidden_sums = expert(
        second, output_grad, middle, ups, downs, bias, vec
    )
    token_grad, packed, grad_up, grad_down, grad_att = backward(
        tuple(masks),
        [output_grad, middle, inner, q, k, v, probs],
        [mixed, normed, caption_tokens],
        weights,
        vec,
        hidden_sums,
        [up_grads, down_grads],
    )
    grad_up, grad_down, grad_att = widen(grad_up), widen(grad_down), widen(grad_att)
    sums, mine = packed[16:24], packed[32:34]
    return (
        result,
        token_grad,
        sums[0],
        sums[1],
        grad_att[:part].T,
        mine[0, :part],
        grad_att[part : 2 * part].T,
        grad_att[2 * part : 3 * part].T,
        mine[0, part : 2 * part],
        grad_att[3 * part :],
        sums[2],
        sums[3],
        sums[4],
        grad_up,
        mine[1],
        grad_down,
        sums[5],
    )


def solution(mesh):
    ndp, nt = mesh.shape["dp"], mesh.shape["tensor"]
    both = P(("dp", "tensor"), None)
    col, row, vec = P(None, "tensor"), P("tensor", None), P("tensor")

    def body(*args):
        return per_device(ndp, nt, *args)

    return jax.shard_map(
        body,
        mesh=mesh,
        in_specs=(both, P("dp"), both, P(), P(), col, vec, col, col, vec, row, P(), P(), P(), col, vec, row, P()),
        out_specs=(both, both, P(), P(), col, vec, col, col, vec, row, P(), P(), P(), col, vec, row, P()),
        check_vma=False,
    )
```

```python
import functools
import math

import jax
import jax.numpy as jnp
from jax import lax
from jax.experimental import pallas as pl
from jax.experimental.pallas import tpu as pltpu
from jax.sharding import PartitionSpec as P


HDIM = 64
LMAX = 64
EPS = 1e-05
NEG = -1e30
GROUP = 4
BLOCK = 256
PAD = 32
CHUNK = 128
TILE = 128
AXES = ("dp", "tensor")
BF = jnp.bfloat16
F32 = jnp.float32
VMEM_LIMIT = 60 * 1024 * 1024


def widen(values):
    return values.astype(F32)


def dot_nn(left, right):
    return jnp.dot(left, right, preferred_element_type=F32)


def dot_nt(left, right):
    return lax.dot_general(left, right, (((1,), (1,)), ((), ())), preferred_element_type=F32)


def dot_tn(left, right):
    return lax.dot_general(left, right, (((0,), (0,)), ((), ())), preferred_element_type=F32)


def normalize(values):
    center = jnp.mean(values, -1, keepdims=True)
    spread = values - center
    scale = lax.rsqrt(jnp.mean(spread * spread, -1, keepdims=True) + EPS)
    return spread * scale, scale


def normalize_back(grad, unit, scale):
    return scale * (
        grad - jnp.mean(grad, -1, keepdims=True) - unit * jnp.mean(grad * unit, -1, keepdims=True)
    )


def erf(values):
    values = jnp.clip(values, -4.0, 4.0)
    square = values * values
    top = -2.72614225801306e-10
    for coef in (
        2.77068142495902e-08,
        -2.10102402082508e-06,
        -5.69250639462346e-05,
        -7.34990630326855e-04,
        -2.95459980854025e-03,
        -1.60960333262415e-02,
    ):
        top = top * square + coef
    low = -1.45660718464996e-05
    for coef in (
        -2.13374055278905e-04,
        -1.68282697438203e-03,
        -7.37332916720468e-03,
        -1.42647390514189e-02,
    ):
        low = low * square + coef
    return values * top / low


def diagonal_mask(size):
    rows = lax.shift_right_logical(lax.broadcasted_iota(jnp.int32, (size, size), 0), 6)
    cols = lax.shift_right_logical(lax.broadcasted_iota(jnp.int32, (size, size), 1), 6)
    return jnp.where(rows == cols, 1.0, 0.0).astype(BF)


def spread_heads(values, mask):
    return jnp.concatenate([values] * GROUP, 0) * mask


def pick_heads(values):
    lane = lax.shift_right_logical(
        lax.broadcasted_iota(jnp.int32, (LMAX, values.shape[1]), 1), 6
    )
    out = values[:LMAX]
    for head in range(1, GROUP):
        out = jnp.where(lane == head, values[head * LMAX : (head + 1) * LMAX], out)
    return out


def full(shape):
    return pl.BlockSpec(shape, lambda i, *_: (0,) * len(shape))


def rowed(width):
    return pl.BlockSpec((BLOCK, width), lambda i, *_: (i, 0))


def params():
    return pltpu.CompilerParams(
        dimension_semantics=("arbitrary",), vmem_limit_bytes=VMEM_LIMIT
    )


def split_rows(rows):
    count = rows // 16
    spans, start = [], 0
    for k in range(3):
        size = (count * (k + 1) // 3 - count * k // 3) * 16
        spans.append((start, size))
        start += size
    return spans


def forward_kernel(
    length_ref,
    tokens_ref,
    shard_ref,
    up_ref,
    down_ref,
    vec_ref,
    normed_ref,
    q_ref,
    k_ref,
    v_ref,
    probs_ref,
    mixed_ref,
    middle_ref,
    second_ref,
    weights_ref,
    bias_ref,
    up_all,
    down_all,
    mask_ref,
    land_ref,
    stage_ref,
    vector_s,
    send_sem,
    recv_sem,
    local_sem,
):
    step = pl.program_id(0)
    dim = tokens_ref.shape[1]
    part = dim // 4
    dp = lax.axis_index("dp")
    t = lax.axis_index("tensor")
    bit = dp % 2
    peers = {
        "core": (dp, t + 1 - 2 * (t % 2)),
        "far": (dp, t + 2 - 4 * ((t // 2) % 2)),
        "side": (dp + 1 - 2 * bit, t),
    }
    chunks = [
        (shard_ref, land_ref.at[1], land_ref.at[2], land_ref.at[3]),
        (up_ref, up_all.at[1], up_all.at[2], up_all.at[3]),
        (down_ref, down_all.at[1], down_all.at[2], down_all.at[3]),
    ]
    recipes = {}

    def recipe(key, source, target, peer):
        recipes[key] = (len(recipes), source, target, peer)

    for c, (shard, near, cross, last) in enumerate(chunks):
        half = shard.shape[0] // 2
        recipe((c, "near"), shard, near, "core")
        for n, (start, size) in enumerate(split_rows(half)):
            mine = pl.ds(pl.multiple_of(bit * half + start, 16), size)
            other = pl.ds(pl.multiple_of((1 - bit) * half + start, 16), size)
            recipe((c, "y", n), shard.at[mine, :], cross.at[mine, :], "far")
            recipe((c, "x", n), cross.at[mine, :], cross.at[mine, :], "side")
            recipe((c, "a", n), cross.at[mine, :], last.at[mine, :], "core")
            recipe((c, "b", n), cross.at[other, :], last.at[other, :], "core")

    def copy(key):
        slot, source, target, peer = recipes[key]
        return pltpu.make_async_remote_copy(
            src_ref=source,
            dst_ref=target,
            send_sem=send_sem.at[slot],
            recv_sem=recv_sem.at[slot],
            device_id=peers[peer],
            device_id_type=pl.DeviceIdType.MESH,
        )

    def own_copy(n, out):
        source, target = ((up_ref, up_all), (down_ref, down_all))[n]
        if out:
            return pltpu.make_async_copy(stage_ref.at[n], target.at[0], local_sem.at[3 + n])
        return pltpu.make_async_copy(source, stage_ref.at[n], local_sem.at[1 + n])

    def pass_y(c, n):
        copy((c, "y", n)).wait_recv()
        copy((c, "x", n)).start()
        copy((c, "a", n)).start()

    def pass_x(c, n):
        copy((c, "x", n)).wait_recv()
        copy((c, "b", n)).start()

    @pl.when(step == 0)
    def _():
        barrier = pltpu.get_barrier_semaphore()
        for peer in peers.values():
            pl.semaphore_signal(
                barrier, inc=1, device_id=peer, device_id_type=pl.DeviceIdType.MESH
            )
        pl.semaphore_wait(barrier, 3)
        own = pltpu.make_async_copy(shard_ref, land_ref.at[0], local_sem.at[0])
        own.start()
        for c in range(3):
            for n in range(3):
                copy((c, "y", n)).start()
            copy((c, "near")).start()
        for n in range(2):
            own_copy(n, False).start()
        mask_ref[...] = diagonal_mask(GROUP * HDIM)
        own.wait()
        pass_y(0, 0)
        pass_y(0, 1)
        pass_x(0, 0)
        pass_y(0, 2)
        pass_x(0, 1)
        pass_x(0, 2)
        copy((0, "near")).wait_recv()
        for n in range(3):
            copy((0, "a", n)).wait_recv()
            copy((0, "b", n)).wait_recv()
        for j in range(4):
            for kind in range(4):
                weights_ref[kind, j * part : (j + 1) * part, :] = land_ref[
                    j, kind * part : (kind + 1) * part, :
                ]
        rows = [widen(land_ref[j, 4 * part : 4 * part + 16, :]) for j in range(4)]
        vector_s[0:1, :] = jnp.concatenate([r[0:1, :part] for r in rows], 1)
        vector_s[1:2, :] = jnp.concatenate([r[2:3, :part] for r in rows], 1)
        for j in range(4):
            bias_ref[8 * j : 8 * j + 8, :] = jnp.broadcast_to(rows[j][1:2], (8, dim))
        pass_y(1, 0)
        pass_y(1, 1)

    @pl.when(step == 1)
    def _():
        for n in range(2):
            own_copy(n, False).wait()
            own_copy(n, True).start()
        pass_x(1, 0)
        pass_y(1, 2)
        pass_x(1, 1)
        pass_y(2, 0)

    @pl.when(step == 2)
    def _():
        pass_x(1, 2)
        pass_y(2, 1)
        pass_x(2, 0)

    @pl.when(step == 3)
    def _():
        pass_y(2, 2)
        pass_x(2, 1)

    tokens = widen(tokens_ref[...])
    vec = vec_ref[...]
    unit, _ = normalize(tokens)
    normed = (unit * vec[0:1] + vec[1:2]).astype(BF)
    normed_ref[...] = normed
    q_ref[...] = (dot_nt(normed, weights_ref[0]) + vector_s[0:1, :]).astype(BF)
    k_ref[...] = dot_nt(normed, weights_ref[1]).astype(BF)
    v_ref[...] = (dot_nt(normed, weights_ref[2]) + vector_s[1:2, :]).astype(BF)
    width = GROUP * HDIM
    factor = 1.0 / math.sqrt(HDIM)
    mask = mask_ref[...]
    for c in range(BLOCK // LMAX):
        rows = pl.ds(c * LMAX, LMAX)
        length = length_ref[
            (t * pl.num_programs(0) + step) * (BLOCK // LMAX) + c
        ]
        live = lax.broadcasted_iota(jnp.int32, (LMAX, width), 0) < length
        for g in range(dim // width):
            cols = pl.ds(g * width, width)
            wide = spread_heads(q_ref[rows, cols], mask)
            scores = dot_nt(k_ref[rows, cols], wide) * factor
            scores = jnp.where(live, scores, NEG)
            exponent = jnp.exp(scores - jnp.max(scores, 0, keepdims=True))
            probs = exponent * (1.0 / jnp.sum(exponent, 0, keepdims=True))
            probs_ref[rows, cols] = probs
            crossed = dot_tn(probs.astype(BF), v_ref[rows, cols])
            mixed_ref[rows, cols] = pick_heads(crossed).astype(BF)
    middle = tokens + dot_nn(mixed_ref[...], weights_ref[3]) + vec[2:3]
    middle_ref[...] = middle
    unit, _ = normalize(middle)
    second_ref[...] = (unit * vec[3:4] + vec[4:5]).astype(BF)

    @pl.when(step == pl.num_programs(0) - 1)
    def _():
        pass_x(2, 2)
        for c in (1, 2):
            copy((c, "near")).wait_recv()
            for n in range(3):
                copy((c, "a", n)).wait_recv()
                copy((c, "b", n)).wait_recv()
        for key in recipes:
            copy(key).wait_send()
        for n in range(2):
            own_copy(n, True).wait()


def forward(lengths, tokens, shard, up, down, vec):
    rows, dim = tokens.shape
    steps = rows // BLOCK
    shapes = [
        (dim, BF),
        (dim, BF),
        (dim, BF),
        (dim, BF),
        (dim, F32),
        (dim, BF),
        (dim, F32),
        (dim, BF),
    ]
    anywhere = pl.BlockSpec(memory_space=pl.ANY)
    copies = 3 * 13
    return pl.pallas_call(
        forward_kernel,
        grid_spec=pltpu.PrefetchScalarGridSpec(
            num_scalar_prefetch=1,
            grid=(steps,),
            in_specs=[rowed(dim), anywhere, anywhere, anywhere, full(vec.shape)],
            out_specs=[rowed(width) for width, _ in shapes]
            + [full((4, dim, dim)), full((32, dim))]
            + [anywhere] * 2,
            scratch_shapes=[
                pltpu.VMEM((GROUP * HDIM, GROUP * HDIM), BF),
                pltpu.VMEM((4,) + shard.shape, BF),
                pltpu.VMEM((2,) + up.shape, BF),
                pltpu.VMEM((8, dim), F32),
                pltpu.SemaphoreType.DMA((copies,)),
                pltpu.SemaphoreType.DMA((copies,)),
                pltpu.SemaphoreType.DMA((5,)),
            ],
        ),
        out_shape=[jax.ShapeDtypeStruct((rows, width), kind) for width, kind in shapes]
        + [jax.ShapeDtypeStruct((4, dim, dim), BF), jax.ShapeDtypeStruct((32, dim), F32)]
        + [
            jax.ShapeDtypeStruct((4,) + up.shape, BF),
            jax.ShapeDtypeStruct((4,) + down.shape, BF),
        ],
        compiler_params=pltpu.CompilerParams(
            dimension_semantics=("arbitrary",),
            vmem_limit_bytes=VMEM_LIMIT,
            collective_id=1,
            has_side_effects=True,
        ),
        name="attend",
    )(lengths, tokens, shard, up, down, vec)


def expert_kernel(
    second_ref,
    grad_ref,
    middle_ref,
    up_ref,
    down_ref,
    bias_ref,
    vec_ref,
    result_ref,
    total_ref,
    up_grad_ref,
    down_grad_ref,
    bias_grad_ref,
    sum_s,
    active_s,
    hidden_s,
):
    piece = pl.program_id(0)
    step = pl.program_id(1)
    rows = pl.ds(pl.multiple_of(step * BLOCK, BLOCK), BLOCK)
    hidden = dot_nn(second_ref[rows, :], up_ref[...]) + bias_ref[0:1, :]
    lean = 0.5 + 0.5 * erf(hidden * (1.0 / math.sqrt(2.0)))
    slope = lean + hidden * (jnp.exp(-0.5 * hidden * hidden) * (1.0 / math.sqrt(2.0 * math.pi)))
    active = (hidden * lean).astype(BF)
    active_s[rows, :] = active
    back = (dot_nt(grad_ref[rows, :], down_ref[...]) * slope).astype(BF)
    hidden_s[rows, :] = back
    result = dot_nn(active, down_ref[...])
    total = dot_nt(back, up_ref[...])

    @pl.when(piece == 0)
    def _():
        sum_s[rows, :] = result + middle_ref[rows, :]
        total_ref[rows, :] = total

    @pl.when(piece > 0)
    def _():
        sum_s[rows, :] += result
        total_ref[rows, :] += total

    @pl.when(piece == pl.num_programs(0) - 1)
    def _():
        result_ref[rows, :] = (sum_s[rows, :] + vec_ref[5:6, :]).astype(BF)

    @pl.when(step == pl.num_programs(1) - 1)
    def _():
        down_grad_ref[...] = dot_tn(active_s[...], grad_ref[...]).astype(BF)
        up_grad_ref[...] = dot_tn(second_ref[...], hidden_s[...]).astype(BF)
        bias_grad_ref[...] = jnp.broadcast_to(
            jnp.sum(widen(hidden_s[...]), 0, keepdims=True), bias_grad_ref.shape
        )


def once(shape):
    return pl.BlockSpec(shape, lambda i, *_: (0,) * len(shape), pipeline_mode=pl.Buffered(1))


def expert(second, grad, middle, ups, downs, bias, vec):
    rows, dim = second.shape
    pieces, _, units = ups.shape

    def quarter(*shape):
        return pl.BlockSpec((None,) + shape, lambda p, i: (pieces - 1 - p, 0, 0))

    row = pl.BlockSpec((8, units), lambda p, i: (pieces - 1 - p, 0))
    return pl.pallas_call(
        expert_kernel,
        grid=(pieces, rows // BLOCK),
        in_specs=[once((rows, dim))] * 3
        + [quarter(dim, units), quarter(units, dim), row, once(vec.shape)],
        out_specs=[
            once((rows, dim)),
            once((rows, dim)),
            quarter(dim, units),
            quarter(units, dim),
            row,
        ],
        out_shape=[
            jax.ShapeDtypeStruct((rows, dim), BF),
            jax.ShapeDtypeStruct((rows, dim), F32),
            jax.ShapeDtypeStruct(ups.shape, BF),
            jax.ShapeDtypeStruct(downs.shape, BF),
            jax.ShapeDtypeStruct((8 * pieces, units), F32),
        ],
        scratch_shapes=[
            pltpu.VMEM((rows, dim), F32),
            pltpu.VMEM((rows, units), BF),
            pltpu.VMEM((rows, units), BF),
        ],
        compiler_params=pltpu.CompilerParams(
            dimension_semantics=("arbitrary", "arbitrary"), vmem_limit_bytes=VMEM_LIMIT
        ),
        cost_estimate=pl.CostEstimate(
            flops=12 * pieces * rows * dim * units,
            bytes_accessed=40 * rows * dim,
            transcendentals=2 * pieces * rows * units,
        ),
        name="expert",
    )(second, grad, middle, ups, downs, bias, vec)


def add_rows(into, base, other, other_base, rows, result=None):
    result = into if result is None else result
    size = min(rows, TILE)

    def body(i, carry):
        left = pl.ds(pl.multiple_of(base + i * size, 8), size)
        right = pl.ds(pl.multiple_of(other_base + i * size, 8), size)
        result[left, :] = (widen(into[left, :]) + widen(other[right, :])).astype(into.dtype)
        return carry

    lax.fori_loop(0, rows // size, body, 0)


def plan_levels(masks, rows):
    levels, place = [], 0
    for mask in masks:
        after = rows // 2 if (rows // 2) % 16 == 0 else rows
        levels.append((mask, rows, after, place))
        place += after
        rows = after
    return levels, place


def reduce_kernel(masks, chunk, *refs):
    (
        grad_ref,
        middle_ref,
        inner_ref,
        q_ref,
        k_ref,
        v_ref,
        probs_ref,
        mixed_ref,
        normed_ref,
        tokens_ref,
        weights_ref,
        vec_ref,
    ) = refs[:12]
    hidden_sums, sources, refs = refs[12], refs[13:15], refs[15:]
    input_grad_ref, small_out, refs = refs[0], refs[1], refs[2:]
    out_refs, refs = refs[:3], refs[3:]
    mask_ref, low_s, mixed_grad_s, middle_grad_s, dq_ref, dk_ref, dv_ref = refs[:7]
    near_piece, last_piece, own, cross, near_own, near_cross, far, landing, gathered = refs[7:16]
    small_s, small_land, send_sem, recv_sem, local_sem, out_sem = refs[16:]

    step = pl.program_id(0)
    last = 3
    dim = grad_ref.shape[1]
    part = dim // 4
    levels, place = plan_levels(masks, chunk)
    halved = [k for k, level in enumerate(levels) if level[2] != level[1]]
    each = dim // chunk
    subs = 3 * each
    att = 2 * dim
    dp = lax.axis_index("dp")
    t = lax.axis_index("tensor")
    bits = {mask: (dp // mask) % 2 for mask in masks}
    peers = {mask: (dp + mask - 2 * mask * bits[mask], t) for mask in masks}
    peers["core"] = (dp, t + 1 - 2 * (t % 2))
    peers["far"] = (dp, t + 2 - 4 * ((t // 2) % 2))
    keeps, leaves, at = [], [], 0
    for mask, before, after, _ in levels:
        if after == before:
            keep = leave = at
        else:
            keep = at + bits[mask] * after
            leave = at + after - bits[mask] * after
        keeps.append(keep)
        leaves.append(leave)
        at = keep

    recipes = {}

    def recipe(key, source, target, peer):
        recipes[key] = (len(recipes), source, target, peer)

    def window(base, offset, size):
        return pl.ds(pl.multiple_of(base + offset, 16), size)

    for i in range(subs):
        base = i * chunk
        here = pl.ds(base, chunk)
        within = pl.ds((i % each) * chunk, chunk)
        if i < 2 * each:
            near, farthest = sources[i // each].at[1], sources[i // each].at[3]
        else:
            near, farthest = near_piece, last_piece
        recipe((i, "near_cross"), farthest.at[within, :], near_cross.at[here, :], "core")
        recipe((i, "near_own"), near.at[within, :], near_own.at[here, :], "core")
        recipe((i, "far"), cross.at[here, :], far.at[here, :], "far")
        for k, (mask, before, after, spot) in enumerate(levels):
            recipe(
                (i, "down", k),
                own.at[window(base, leaves[k], after), :],
                landing.at[pl.ds(i * place + spot, after), :],
                mask,
            )
        for k in halved:
            rows = window(base, keeps[k], levels[k][2])
            recipe((i, "up", k), gathered.at[rows, :], gathered.at[rows, :], levels[k][0])
    small_peers = ["core", "far"] + list(masks)
    spans = [(0, 24), (16, 16)] + [(16, 24)] * len(masks)
    for n, (first, count) in enumerate(spans):
        recipe(
            ("small", n),
            small_s.at[pl.ds(first, count), :],
            small_land.at[n, pl.ds(0, count), :],
            small_peers[n],
        )

    def copy(key):
        slot, source, target, peer = recipes[key]
        return pltpu.make_async_remote_copy(
            src_ref=source,
            dst_ref=target,
            send_sem=send_sem.at[slot],
            recv_sem=recv_sem.at[slot],
            device_id=peers[peer],
            device_id_type=pl.DeviceIdType.MESH,
        )

    def local_pair(i):
        within = pl.ds((i % each) * chunk, chunk)
        here = pl.ds(i * chunk, chunk)
        group = sources[i // each]
        return [
            pltpu.make_async_copy(group.at[2, within, :], cross.at[here, :], local_sem.at[2 * i]),
            pltpu.make_async_copy(group.at[0, within, :], own.at[here, :], local_sem.at[2 * i + 1]),
        ]

    def core_send(i):
        copy((i, "near_cross")).start()
        copy((i, "near_own")).start()
        if i < 2 * each:
            for piece in local_pair(i):
                piece.start()

    def start_cross(i):
        if i < 2 * each:
            for piece in local_pair(i):
                piece.wait()
        copy((i, "near_cross")).wait_recv()
        add_rows(cross, i * chunk, near_cross, i * chunk, chunk)
        copy((i, "far")).start()
        copy((i, "near_own")).wait_recv()
        add_rows(own, i * chunk, near_own, i * chunk, chunk)

    def take_far(i):
        copy((i, "far")).wait_recv()
        add_rows(own, i * chunk, far, i * chunk, chunk)
        copy((i, "down", 0)).start()

    def take_level(i, k):
        _, before, after, spot = levels[k]
        copy((i, "down", k)).wait_recv()
        if after == before:
            copy((i, "down", k)).wait_send()
        final = k + 1 == len(levels)
        add_rows(
            own,
            i * chunk + keeps[k],
            landing,
            i * place + spot,
            after,
            gathered if final else None,
        )
        if not final:
            copy((i, "down", k + 1)).start()
        elif halved:
            copy((i, "up", halved[-1])).start()

    def take_up(i, n):
        copy((i, "up", halved[-1 - n])).wait_recv()
        if n + 1 < len(halved):
            copy((i, "up", halved[-2 - n])).start()

    def small_step(n):
        first = spans[n][0]
        copy(("small", n)).wait()
        land = small_land.at[n]
        small_s[16:24, :] += land[16 - first : 24 - first, :]
        if n == 0:
            small_s[32:40, :] += land[0:8, :]
            small_s[24:32, :] += land[8:16, :]
        elif n == 1:
            small_s[32:40, :] += land[8:16, :]
        else:
            small_s[32:40, :] += land[16:24, :]
        if n + 1 < len(spans):
            copy(("small", n + 1)).start()

    def weight_grads():
        query_sum = jnp.sum(widen(dq_ref[...]), 0, keepdims=True)
        value_sum = jnp.sum(widen(dv_ref[...]), 0, keepdims=True)
        blank = jnp.zeros((1, dim - 2 * part), F32)
        for j, row in enumerate((32, 0, 24, 8)):
            cols = slice(j * part, (j + 1) * part)
            small_s[row : row + 1, :] = jnp.concatenate(
                [query_sum[:, cols], value_sum[:, cols], blank], 1
            )
            small_s[row + 1 : row + 2, :] = hidden_sums[8 * j : 8 * j + 1, :]
        for kind, (left, right) in enumerate(
            ((dq_ref, normed_ref), (dk_ref, normed_ref), (dv_ref, normed_ref), (mixed_ref, low_s))
        ):
            result = dot_tn(left[...], right[...]).astype(BF)
            low, high = kind * part, (kind + 1) * part
            own[att + low : att + high, :] = result[:part]
            near_piece[low:high, :] = result[part : 2 * part]
            cross[att + low : att + high, :] = result[2 * part : 3 * part]
            last_piece[low:high, :] = result[3 * part :]

    def input_pair(pair):
        lax.fori_loop(2 * pair, 2 * pair + 2, input_block, 0)

    def input_block(block, carry):
        rows = pl.ds(pl.multiple_of(block * BLOCK, BLOCK), BLOCK)
        unit, scale = normalize(widen(tokens_ref[rows, :]))
        grad = (
            dot_nn(dq_ref[rows, :], weights_ref[0])
            + dot_nn(dk_ref[rows, :], weights_ref[1])
            + dot_nn(dv_ref[rows, :], weights_ref[2])
        )
        small_s[16:17, :] += jnp.sum(grad * unit, 0, keepdims=True)
        small_s[17:18, :] += jnp.sum(grad, 0, keepdims=True)
        back = normalize_back(grad * vec_ref[0:1, :], unit, scale)
        input_grad_ref[rows, :] = (middle_grad_s[rows, :] + back).astype(BF)
        return carry

    span = 3.0 * chunk / 128
    tasks = []

    def add(when, task, *args):
        tasks.append((when, len(tasks), functools.partial(task, *args)))

    for i in range(subs):
        arrive = 2.0 + span * (i + 1)
        if i < 2 * each:
            add(1.0 + 0.2 * span * i, start_cross, i)
        else:
            add(36.0, core_send, i)
            add(39.0 + 0.2 * span * (i - 2 * each), start_cross, i)
        add(arrive, take_far, i)
        for k in range(len(levels)):
            add(arrive + span * (1 + k), take_level, i, k)
        for n in range(len(halved)):
            add(arrive + span * (1 + len(levels) + n), take_up, i, n)
    blocks = tokens_ref.shape[0] // BLOCK
    add(27.0, weight_grads)
    for pair in range(blocks // 2):
        add(45.0 + 6.0 * pair, input_pair, pair)
    end = 43.0 + 3.0 * blocks
    add(end, lambda: copy(("small", 0)).start())
    for n in range(len(spans)):
        add(end + 3.0 + 3.0 * n, small_step, n)
    tasks.sort(key=lambda entry: entry[:2])

    def run(low, high):
        for when, _, task in tasks:
            if low <= when < high:
                task()

    @pl.when(step == 0)
    def _():
        barrier = pltpu.get_barrier_semaphore()
        for peer in peers.values():
            pl.semaphore_signal(
                barrier, inc=1, device_id=peer, device_id_type=pl.DeviceIdType.MESH
            )
        pl.semaphore_wait(barrier, len(peers))
        for i in range(2 * each):
            core_send(i)
        mask_ref[...] = diagonal_mask(GROUP * HDIM)
        small_s[...] = jnp.zeros_like(small_s)

    all_rows = pl.ds(pl.multiple_of(step * BLOCK, BLOCK), BLOCK)
    vec = vec_ref[...]
    upstream = widen(grad_ref[...])
    unit, scale = normalize(middle_ref[...])
    inner = inner_ref[...]
    middle_grad = upstream + normalize_back(inner * vec[3:4], unit, scale)
    middle_grad_s[all_rows, :] = middle_grad
    middle_low = middle_grad.astype(BF)
    low_s[all_rows, :] = middle_low
    small_s[18:19, :] += jnp.sum(middle_grad, 0, keepdims=True)
    small_s[19:20, :] += jnp.sum(inner * unit, 0, keepdims=True)
    small_s[20:21, :] += jnp.sum(inner, 0, keepdims=True)
    small_s[21:22, :] += jnp.sum(upstream, 0, keepdims=True)
    mixed_grad_s[...] = dot_nt(middle_low, weights_ref[3]).astype(BF)
    width = GROUP * HDIM
    factor = 1.0 / math.sqrt(HDIM)
    mask = mask_ref[...]
    for c in range(BLOCK // LMAX):
        rows = pl.ds(c * LMAX, LMAX)
        into = pl.ds(pl.multiple_of(step * BLOCK + c * LMAX, LMAX), LMAX)
        for block in range(blocks):
            slot = block * (BLOCK // LMAX) + c

            @pl.when(step == block)
            def _():
                run(0.5 + 1.5 * slot, 2.0 + 1.5 * slot)

        for g in range(dim // width):
            cols = pl.ds(g * width, width)
            wide = spread_heads(mixed_grad_s[rows, cols], mask)
            probs = probs_ref[rows, cols]
            prob_grad = dot_nt(v_ref[rows, cols], wide)
            dv_ref[into, cols] = dot_nn(probs.astype(BF), wide).astype(BF)
            weighted = jnp.sum(probs * prob_grad, 0, keepdims=True)
            score_grad = (probs * (prob_grad - weighted)).astype(BF)
            queries = spread_heads(q_ref[rows, cols], mask)
            dk_ref[into, cols] = (dot_nn(score_grad, queries) * factor).astype(BF)
            crossed = dot_tn(score_grad, k_ref[rows, cols])
            dq_ref[into, cols] = (pick_heads(crossed) * factor).astype(BF)

    @pl.when(step == last)
    def _():
        run(0.5 + 1.5 * blocks * (BLOCK // LMAX), 1e9)
        outs = [
            pltpu.make_async_copy(
                gathered.at[pl.ds(n * dim, dim), :], out_refs[n], out_sem.at[n]
            )
            for n in range(3)
        ]
        for out in outs:
            out.start()
        small_out[...] = small_s[...]
        for key in recipes:
            repeated = key[0] == "small" or (
                key[1] == "down" and levels[key[2]][1] == levels[key[2]][2]
            )
            if not repeated:
                copy(key).wait_send()
        for out in outs:
            out.wait()


def backward(masks, blocked, whole, weights, vec, hidden_sums, groups):
    rows, dim = blocked[0].shape
    levels, place = plan_levels(masks, CHUNK)
    total = 3 * dim
    subs = total // CHUNK
    halved = sum(level[1] != level[2] for level in levels)
    copies = subs * (3 + len(levels) + halved) + 2 + len(masks)
    anywhere = pl.BlockSpec(memory_space=pl.ANY)
    buffer = pltpu.VMEM((total, dim), BF)
    all_rows = pltpu.VMEM((rows, dim), BF)
    return pl.pallas_call(
        functools.partial(reduce_kernel, masks, CHUNK),
        grid=(rows // BLOCK,),
        in_specs=[rowed(dim)] * len(blocked)
        + [once((rows, dim))] * len(whole)
        + [once(weights.shape), full(vec.shape)]
        + [once(hidden_sums.shape)]
        + [anywhere] * len(groups),
        out_specs=[once((rows, dim)), full((40, dim))] + [anywhere] * 3,
        out_shape=[
            jax.ShapeDtypeStruct((rows, dim), BF),
            jax.ShapeDtypeStruct((40, dim), F32),
        ]
        + [jax.ShapeDtypeStruct((dim, dim), BF)] * 3,
        scratch_shapes=[
            pltpu.VMEM((GROUP * HDIM, GROUP * HDIM), BF),
            all_rows,
            pltpu.VMEM((BLOCK, dim), BF),
            pltpu.VMEM((rows, dim), F32),
            all_rows,
            all_rows,
            all_rows,
            pltpu.VMEM((dim, dim), BF),
            pltpu.VMEM((dim, dim), BF),
            buffer,
            buffer,
            buffer,
            buffer,
            buffer,
            pltpu.VMEM((subs * place, dim), BF),
            buffer,
            pltpu.VMEM((40, dim), F32),
            pltpu.VMEM((2 + len(masks), 24, dim), F32),
            pltpu.SemaphoreType.DMA((copies,)),
            pltpu.SemaphoreType.DMA((copies,)),
            pltpu.SemaphoreType.DMA((2 * subs,)),
            pltpu.SemaphoreType.DMA((3,)),
        ],
        compiler_params=pltpu.CompilerParams(
            dimension_semantics=("arbitrary",),
            collective_id=0,
            has_side_effects=True,
            vmem_limit_bytes=66 * 1024 * 1000,
        ),
        name="attend_back",
    )(*blocked, *whole, weights, vec, hidden_sums, *groups)


def lay_out(size, vectors, pitch, kind):
    out = None
    for i, values in enumerate(vectors):
        start = i * pitch
        piece = lax.pad(
            values.astype(kind), jnp.zeros((), kind), [(start, size - start - values.shape[0], 0)]
        )
        out = piece if out is None else out + piece
    return out


def per_device(
    ndp,
    nt,
    caption_tokens,
    caption_lengths,
    output_grad,
    norm_gain,
    norm_bias,
    query_weight,
    query_bias,
    key_weight,
    value_weight,
    value_bias,
    output_weight,
    output_bias,
    second_gain,
    second_bias,
    hidden_weight,
    hidden_bias,
    down_weight,
    down_bias,
):
    masks, mask = [], 1
    while mask < ndp:
        masks.append(mask)
        mask *= 2
    rows, dim = caption_tokens.shape
    part = query_weight.shape[1]
    biases = lay_out(PAD * dim, (query_bias, hidden_bias, value_bias), dim, BF).reshape(PAD, dim)
    shard = jnp.concatenate([query_weight.T, key_weight.T, value_weight.T, output_weight, biases], 0)
    vec = lay_out(
        8 * dim, (norm_gain, norm_bias, output_bias, second_gain, second_bias, down_bias), dim, F32
    ).reshape(8, dim)
    normed, q, k, v, probs, mixed, middle, second, weights, bias, ups, downs = forward(
        caption_lengths, caption_tokens, shard, hidden_weight, down_weight, vec
    )
    result, inner, up_grads, down_grads, hidden_sums = expert(
        second, output_grad, middle, ups, downs, bias, vec
    )
    token_grad, packed, grad_up, grad_down, grad_att = backward(
        tuple(masks),
        [output_grad, middle, inner, q, k, v, probs],
        [mixed, normed, caption_tokens],
        weights,
        vec,
        hidden_sums,
        [up_grads, down_grads],
    )
    grad_up, grad_down, grad_att = widen(grad_up), widen(grad_down), widen(grad_att)
    sums, mine = packed[16:24], packed[32:34]
    return (
        result,
        token_grad,
        sums[0],
        sums[1],
        grad_att[:part].T,
        mine[0, :part],
        grad_att[part : 2 * part].T,
        grad_att[2 * part : 3 * part].T,
        mine[0, part : 2 * part],
        grad_att[3 * part :],
        sums[2],
        sums[3],
        sums[4],
        grad_up,
        mine[1],
        grad_down,
        sums[5],
    )


def solution(mesh):
    ndp, nt = mesh.shape["dp"], mesh.shape["tensor"]
    both = P(("dp", "tensor"), None)
    col, row, vec = P(None, "tensor"), P("tensor", None), P("tensor")

    def body(*args):
        return per_device(ndp, nt, *args)

    return jax.shard_map(
        body,
        mesh=mesh,
        in_specs=(both, P("dp"), both, P(), P(), col, vec, col, col, vec, row, P(), P(), P(), col, vec, row, P()),
        out_specs=(both, both, P(), P(), col, vec, col, col, vec, row, P(), P(), P(), col, vec, row, P()),
        check_vma=False,
    )
```
